16 devices in a mesh: dp: 2 (over y, z), tp: 8 (over x, core).
Axes of the slice: x: 4, y: 2, z: 1, core: 2. Of those that a mesh axis runs over, the one named last changes fastest.
The devices are a block of a 4x4x8 slice.
Arguments:
- x_steps: bfloat16 [3, 256, 4096], P(None, 'dp'), parts along dimension 1
- seq_lens: int32 [256], P(('dp', 'tp')), parts along dimension 0
- k_cache: bfloat16 [256, 3072, 128], P(('dp', 'tp')), parts along dimension 0
- v_cache: bfloat16 [256, 3072, 128], P(('dp', 'tp')), parts along dimension 0
- ln_gain: bfloat16 [4096], replicated
- ln_bias: bfloat16 [4096], replicated
- w_q: bfloat16 [4096, 4096], P(None, 'tp')
- b_q: bfloat16 [4096], P('tp')
- w_kv: bfloat16 [4096, 256], replicated
- b_kv: bfloat16 [256], replicated
- w_out: bfloat16 [4096, 4096], P('tp')
- b_out: bfloat16 [4096], replicated
Outputs:
- output 1: bfloat16 [3, 256, 4096], P(None, 'dp'), parts along dimension 1
- output 2: bfloat16 [256, 3072, 128], P(('dp', 'tp')), parts along dimension 0
- output 3: bfloat16 [256, 3072, 128], P(('dp', 'tp')), parts along dimension 0
There are 2 independent parts. The reference program is written for one: setup_inputs(seed, part) draws one part's arguments, and reference() takes and returns one part's arrays. A program takes and returns all parts, laid end to end along the dimension named above; an argument that names none is the same for every part.
All inputs are finite; a program needn't handle non-finite values.
Results may differ from the reference program's by a relative error of at most 0.00996645.
Values are sent between devices in bfloat16 or wider.
A program may use at most 768 MiB of HBM per device.

```python
import jax
import jax.numpy as jnp
from jax import lax

BATCH_ROWS = 128
CACHE_LEN = 3072
D_MODEL = 4096
N_HEADS = 32
HEAD_DIM = 128
N_STEPS = 3
LN_EPS = 1e-5


def draw_lens(len_keys):
    seq_lens = jax.random.randint(len_keys[0], (BATCH_ROWS,), 64, CACHE_LEN - 3, dtype=jnp.int32)
    top_idx = jax.random.randint(len_keys[1], (), 0, BATCH_ROWS, dtype=jnp.int32)
    low_idx = (top_idx + 1 + jax.random.randint(len_keys[2], (), 0, BATCH_ROWS - 1, dtype=jnp.int32)) % BATCH_ROWS
    seq_lens = seq_lens.at[top_idx].set(CACHE_LEN - 4)
    return seq_lens.at[low_idx].set(64)


def setup_inputs(seed: int = 0, part: int = 0) -> dict:
    part_keys = jax.random.split(jax.random.fold_in(jax.random.key(seed), part), 4)
    shared_keys = jax.random.split(jax.random.key(seed + 1), 10)
    len_keys = jax.random.split(part_keys[0], 3)
    q_width = N_HEADS * HEAD_DIM
    cache_shape = (BATCH_ROWS, CACHE_LEN, HEAD_DIM)
    x_steps = jax.random.normal(part_keys[1], (N_STEPS, BATCH_ROWS, D_MODEL), jnp.float32)
    k_cache = 2.0 * jax.random.normal(part_keys[2], cache_shape, jnp.float32)
    v_cache = jax.random.normal(part_keys[3], cache_shape, jnp.float32)
    shared_dir = jax.random.normal(shared_keys[0], (HEAD_DIM,), jnp.float32)
    ln_gain = 1.0 + 0.3 * jax.random.normal(shared_keys[1], (D_MODEL,), jnp.float32)
    ln_bias = 0.3 * jax.random.normal(shared_keys[2], (D_MODEL,), jnp.float32)
    w_q = jax.random.normal(shared_keys[3], (D_MODEL, q_width), jnp.float32) * D_MODEL ** -0.5
    b_q = jnp.tile(shared_dir, N_HEADS) + 0.2 * jax.random.normal(shared_keys[4], (q_width,), jnp.float32)
    w_kv = jax.random.normal(shared_keys[5], (D_MODEL, 2 * HEAD_DIM), jnp.float32) * D_MODEL ** -0.5
    b_key = shared_dir + 0.2 * jax.random.normal(shared_keys[6], (HEAD_DIM,), jnp.float32)
    b_value = 0.3 * jax.random.normal(shared_keys[7], (HEAD_DIM,), jnp.float32)
    w_out = jax.random.normal(shared_keys[8], (q_width, D_MODEL), jnp.float32) * q_width ** -0.5
    b_out = 0.3 * jax.random.normal(shared_keys[9], (D_MODEL,), jnp.float32)
    return {
        'x_steps': x_steps.astype(jnp.bfloat16),
        'seq_lens': draw_lens(len_keys),
        'k_cache': k_cache.astype(jnp.bfloat16),
        'v_cache': v_cache.astype(jnp.bfloat16),
        'ln_gain': ln_gain.astype(jnp.bfloat16),
        'ln_bias': ln_bias.astype(jnp.bfloat16),
        'w_q': w_q.astype(jnp.bfloat16),
        'b_q': b_q.astype(jnp.bfloat16),
        'w_kv': w_kv.astype(jnp.bfloat16),
        'b_kv': jnp.concatenate([b_key, b_value]).astype(jnp.bfloat16),
        'w_out': w_out.astype(jnp.bfloat16),
        'b_out': b_out.astype(jnp.bfloat16),
    }


def layer_norm(x_rows, ln_gain, ln_bias):
    x_float = x_rows.astype(jnp.float32)
    row_mean = jnp.mean(x_float, axis=-1, keepdims=True)
    centered = x_float - row_mean
    row_var = jnp.mean(centered * centered, axis=-1, keepdims=True)
    scaled = centered * lax.rsqrt(row_var + LN_EPS)
    return (scaled * ln_gain.astype(jnp.float32) + ln_bias.astype(jnp.float32)).astype(jnp.bfloat16)


def attend_row(row_in):
    q_row, k_row, v_row, last_pos = row_in
    positions = jnp.arange(CACHE_LEN, dtype=jnp.int32)
    scores = jnp.einsum('hd,td->ht', q_row.astype(jnp.float32), k_row.astype(jnp.float32)) * HEAD_DIM ** -0.5
    scores = jnp.where(positions[None, :] <= last_pos, scores, -jnp.inf)
    weights = jnp.exp(scores - jnp.max(scores, axis=-1, keepdims=True))
    numerator = jnp.einsum('ht,td->hd', weights.astype(jnp.bfloat16).astype(jnp.float32), v_row.astype(jnp.float32))
    return (numerator / jnp.sum(weights, axis=-1, keepdims=True)).astype(jnp.bfloat16)


def reference(x_steps, seq_lens, k_cache, v_cache, ln_gain, ln_bias, w_q, b_q, w_kv, b_kv, w_out, b_out):
    positions = jnp.arange(CACHE_LEN, dtype=jnp.int32)

    def one_step(cache_pair, step_in):
        key_rows, value_rows = cache_pair
        x_rows, step_idx = step_in
        normed = layer_norm(x_rows, ln_gain, ln_bias)
        q_rows = (jnp.dot(normed, w_q, preferred_element_type=jnp.float32) + b_q.astype(jnp.float32)).astype(jnp.bfloat16)
        kv_rows = (jnp.dot(normed, w_kv, preferred_element_type=jnp.float32) + b_kv.astype(jnp.float32)).astype(jnp.bfloat16)
        write_pos = seq_lens + step_idx
        written = (positions[None, :] == write_pos[:, None])[:, :, None]
        key_rows = jnp.where(written, kv_rows[:, None, :HEAD_DIM], key_rows)
        value_rows = jnp.where(written, kv_rows[:, None, HEAD_DIM:], value_rows)
        attn_rows = lax.map(attend_row, (q_rows.reshape(BATCH_ROWS, N_HEADS, HEAD_DIM), key_rows, value_rows, write_pos))
        proj_sum = jnp.dot(attn_rows.reshape(BATCH_ROWS, N_HEADS * HEAD_DIM), w_out, preferred_element_type=jnp.float32)
        out_rows = (x_rows.astype(jnp.float32) + proj_sum + b_out.astype(jnp.float32)).astype(jnp.bfloat16)
        return (key_rows, value_rows), out_rows

    step_ids = jnp.arange(N_STEPS, dtype=jnp.int32)
    final_pair, y_steps = lax.scan(one_step, (k_cache, v_cache), (x_steps, step_ids))
    return y_steps, final_pair[0], final_pair[1]
```

```python
import functools
import math

import jax
import jax.numpy as jnp
from jax import lax
from jax.experimental import pallas as pl
from jax.experimental.pallas import tpu as pltpu
from jax.sharding import PartitionSpec as P

LN_EPS = 1e-5
KEY_TILE = 256
FRESH_ROWS = 16
VMEM_LIMIT = 60 * 1024 * 1024


def layer_norm(x_rows, ln_gain, ln_bias):
    x_float = x_rows.astype(jnp.float32)
    row_mean = jnp.mean(x_float, axis=-1, keepdims=True)
    centered = x_float - row_mean
    row_var = jnp.mean(centered * centered, axis=-1, keepdims=True)
    scaled = centered * lax.rsqrt(row_var + LN_EPS)
    return (scaled * ln_gain.astype(jnp.float32) + ln_bias.astype(jnp.float32)).astype(jnp.bfloat16)


def attend_one(q_rows, k_ref, v_ref, score_ref, seq_len, fresh_k, fresh_v, fresh_mask):
    rows, depth = q_rows.shape
    length = k_ref.shape[0]
    to_log2 = depth ** -0.5 * math.log2(math.e)
    contract_last = (((1,), (1,)), ((), ()))
    new_scores = lax.dot_general(q_rows, fresh_k, contract_last, preferred_element_type=jnp.float32)
    new_scores = jnp.where(fresh_mask, new_scores, -jnp.inf)
    best = None
    lane = lax.broadcasted_iota(jnp.int32, (rows, KEY_TILE), 1)
    for start in range(0, length, KEY_TILE):
        tile = lax.dot_general(q_rows, k_ref[start:start + KEY_TILE, :], contract_last, preferred_element_type=jnp.float32)
        tile = jnp.where(lane < seq_len - start, tile, -jnp.inf)
        score_ref[:, start:start + KEY_TILE] = tile
        best = tile if best is None else jnp.maximum(best, tile)
    top = jnp.maximum(jnp.max(best, axis=-1, keepdims=True), jnp.max(new_scores, axis=-1, keepdims=True))
    new_weights = jnp.exp2((new_scores - top) * to_log2)
    numerator = jnp.dot(new_weights.astype(jnp.bfloat16), fresh_v, preferred_element_type=jnp.float32)
    total = None
    for start in range(0, length, KEY_TILE):
        weights = jnp.exp2((score_ref[:, start:start + KEY_TILE] - top) * to_log2)
        total = weights if total is None else total + weights
        numerator = numerator + jnp.dot(weights.astype(jnp.bfloat16), v_ref[start:start + KEY_TILE, :], preferred_element_type=jnp.float32)
    denominator = jnp.sum(total, axis=-1, keepdims=True) + jnp.sum(new_weights, axis=-1, keepdims=True)
    return numerator / denominator


def attention_kernel(n_steps, len_ref, q_ref, fk_ref, fv_ref, k_hbm, v_hbm, out_ref, k_buf, v_buf, score_buf, sems):
    n_seqs, rows, _ = q_ref.shape

    def fetch(b):
        return (pltpu.make_async_copy(k_hbm.at[b], k_buf.at[b], sems.at[0, b]),
                pltpu.make_async_copy(v_hbm.at[b], v_buf.at[b], sems.at[1, b]))

    for b in range(n_seqs):
        for copy in fetch(b):
            copy.start()
    shape = (rows, FRESH_ROWS)
    step_of_row = lax.broadcasted_iota(jnp.int32, shape, 0) // (rows // n_steps)
    fresh_mask = lax.broadcasted_iota(jnp.int32, shape, 1) <= step_of_row

    def body(i, carry):
        for j in range(2):
            for copy in fetch(2 * i + j):
                copy.wait()
        for j in range(2):
            b = 2 * i + j
            out = attend_one(q_ref[b], k_buf.at[b], v_buf.at[b], score_buf.at[j], len_ref[b], fk_ref[b], fv_ref[b], fresh_mask)
            out_ref[b] = out.astype(out_ref.dtype)
        return carry

    lax.fori_loop(0, n_seqs // 2, body, 0)


def attention(q_rows, seq_lens, k_cache, v_cache, fresh_k, fresh_v, n_steps):
    n_seqs, rows, depth = q_rows.shape
    length = k_cache.shape[1]
    pad = ((0, 0), (0, FRESH_ROWS - n_steps), (0, 0))
    vmem = pl.BlockSpec(memory_space=pltpu.VMEM)
    return pl.pallas_call(
        functools.partial(attention_kernel, n_steps),
        out_shape=jax.ShapeDtypeStruct(q_rows.shape, jnp.bfloat16),
        in_specs=[pl.BlockSpec(memory_space=pltpu.SMEM), vmem, vmem, vmem, pl.BlockSpec(memory_space=pl.ANY), pl.BlockSpec(memory_space=pl.ANY)],
        out_specs=vmem,
        scratch_shapes=[
            pltpu.VMEM((n_seqs, length, depth), jnp.bfloat16),
            pltpu.VMEM((n_seqs, length, depth), jnp.bfloat16),
            pltpu.VMEM((2, rows, length), jnp.float32),
            pltpu.SemaphoreType.DMA((2, n_seqs)),
        ],
        compiler_params=pltpu.CompilerParams(vmem_limit_bytes=VMEM_LIMIT),
        cost_estimate=pl.CostEstimate(flops=4 * n_seqs * rows * length * depth, bytes_accessed=4 * n_seqs * length * depth, transcendentals=n_seqs * rows * length),
    )(seq_lens, q_rows, jnp.pad(fresh_k, pad), jnp.pad(fresh_v, pad), k_cache, v_cache)


WINDOW = 16


def patch_kernel(n_steps, len_ref, fk_ref, fv_ref, k_in, v_in, k_out, v_out, k_win, v_win, sems):
    n_seqs, length = k_out.shape[0], k_out.shape[1]

    def first_row(b):
        return pl.multiple_of(jnp.minimum(len_ref[b] // 8 * 8, length - WINDOW), 8)

    def moves(b, back):
        rows = pl.ds(first_row(b), WINDOW)
        pairs = ((k_out.at[b, rows, :], k_win.at[b]), (v_out.at[b, rows, :], v_win.at[b]))
        return [pltpu.make_async_copy(win, hbm, sems.at[i, b]) if back else pltpu.make_async_copy(hbm, win, sems.at[i, b])
                for i, (hbm, win) in enumerate(pairs)]

    for b in range(n_seqs):
        for copy in moves(b, False):
            copy.start()
    for b in range(n_seqs):
        for copy in moves(b, False):
            copy.wait()
        offset = len_ref[b] - first_row(b)
        row = lax.broadcasted_iota(jnp.int32, (WINDOW, k_win.shape[2]), 0)
        for win, fresh in ((k_win, fk_ref), (v_win, fv_ref)):
            rows = win[b].astype(jnp.float32)
            for s in range(n_steps):
                rows = jnp.where(row == offset + s, fresh[b, s:s + 1, :].astype(jnp.float32), rows)
            win[b] = rows.astype(win.dtype)
    for b in range(n_seqs):
        for copy in moves(b, True):
            copy.start()
    for b in range(n_seqs):
        for copy in moves(b, True):
            copy.wait()


def patch_caches(k_copy, v_copy, seq_lens, fresh_k, fresh_v):
    n_seqs, _, depth = k_copy.shape
    n_steps = fresh_k.shape[1]
    vmem = pl.BlockSpec(memory_space=pltpu.VMEM)
    hbm = pl.BlockSpec(memory_space=pl.ANY)
    return pl.pallas_call(
        functools.partial(patch_kernel, n_steps),
        out_shape=[jax.ShapeDtypeStruct(k_copy.shape, k_copy.dtype)] * 2,
        in_specs=[pl.BlockSpec(memory_space=pltpu.SMEM), vmem, vmem, hbm, hbm],
        out_specs=[hbm, hbm],
        scratch_shapes=[
            pltpu.VMEM((n_seqs, WINDOW, depth), jnp.bfloat16),
            pltpu.VMEM((n_seqs, WINDOW, depth), jnp.bfloat16),
            pltpu.SemaphoreType.DMA((2, n_seqs)),
        ],
        input_output_aliases={3: 0, 4: 1},
    )(seq_lens, fresh_k, fresh_v, k_copy, v_copy)


def solution(mesh):
    tp_size = mesh.shape['tp']

    def local_block(x_steps, seq_lens, k_cache, v_cache, ln_gain, ln_bias, w_q, b_q, w_kv, b_kv, w_out, b_out):
        n_steps, group_rows, width = x_steps.shape
        local_rows, _, head_dim = k_cache.shape
        q_part_width = w_q.shape[1]
        n_heads = q_part_width * tp_size // head_dim
        perm = [(i, i) for i in range(tp_size)]
        k_copy = lax.ppermute(k_cache, 'tp', perm)
        v_copy = lax.ppermute(v_cache, 'tp', perm)
        row_start = lax.axis_index('tp') * local_rows
        normed = layer_norm(x_steps, ln_gain, ln_bias)
        q_part = (jnp.einsum('sbk,kn->sbn', normed, w_q, preferred_element_type=jnp.float32) + b_q.astype(jnp.float32)).astype(jnp.bfloat16)
        q_local = lax.all_to_all(q_part, 'tp', 1, 2, tiled=True)
        own_normed = lax.dynamic_slice_in_dim(normed, row_start, local_rows, axis=1)
        kv_rows = (jnp.einsum('sbk,kn->bsn', own_normed, w_kv, preferred_element_type=jnp.float32) + b_kv.astype(jnp.float32)).astype(jnp.bfloat16)
        fresh_k, fresh_v = kv_rows[:, :, :head_dim], kv_rows[:, :, head_dim:]
        q_rows = q_local.reshape(n_steps, local_rows, n_heads, head_dim).transpose(1, 0, 2, 3).reshape(local_rows, n_steps * n_heads, head_dim)
        attn = attention(q_rows, seq_lens, k_cache, v_cache, fresh_k, fresh_v, n_steps)
        attn = attn.reshape(local_rows, n_steps, n_heads * head_dim).transpose(1, 0, 2)
        attn_heads = lax.all_to_all(attn, 'tp', 2, 1, tiled=True)
        proj_part = jnp.einsum('sbk,kn->sbn', attn_heads, w_out, preferred_element_type=jnp.float32).astype(jnp.bfloat16)
        proj_sum = lax.psum(proj_part, 'tp')
        y_steps = (x_steps.astype(jnp.float32) + proj_sum.astype(jnp.float32) + b_out.astype(jnp.float32)).astype(jnp.bfloat16)
        k_out, v_out = patch_caches(k_copy, v_copy, seq_lens, fresh_k, fresh_v)
        return y_steps, k_out, v_out

    row_spec = P(('dp', 'tp'), None, None)
    return jax.shard_map(
        local_block,
        mesh=mesh,
        in_specs=(P(None, 'dp', None), P(('dp', 'tp')), row_spec, row_spec, P(None), P(None), P(None, 'tp'), P('tp'), P(None, None), P(None), P('tp', None), P(None)),
        out_specs=(P(None, 'dp', None), row_spec, row_spec),
        check_vma=False,
    )
```

```python
import functools
import math

import jax
import jax.numpy as jnp
from jax import lax
from jax.experimental import pallas as pl
from jax.experimental.pallas import tpu as pltpu
from jax.sharding import PartitionSpec as P

LN_EPS = 1e-5
KEY_TILE = 256
FRESH_ROWS = 16
VMEM_LIMIT = 60 * 1024 * 1024


def layer_norm(x_rows, ln_gain, ln_bias):
    x_float = x_rows.astype(jnp.float32)
    row_mean = jnp.mean(x_float, axis=-1, keepdims=True)
    centered = x_float - row_mean
    row_var = jnp.mean(centered * centered, axis=-1, keepdims=True)
    scaled = centered * lax.rsqrt(row_var + LN_EPS)
    return (scaled * ln_gain.astype(jnp.float32) + ln_bias.astype(jnp.float32)).astype(jnp.bfloat16)


def attend_one(q_rows, k_ref, v_ref, score_ref, seq_len, fresh_k, fresh_v, fresh_mask):
    rows, depth = q_rows.shape
    length = k_ref.shape[0]
    to_log2 = depth ** -0.5 * math.log2(math.e)
    contract_last = (((1,), (1,)), ((), ()))
    new_scores = lax.dot_general(q_rows, fresh_k, contract_last, preferred_element_type=jnp.float32)
    new_scores = jnp.where(fresh_mask, new_scores, -jnp.inf)
    best = None
    lane = lax.broadcasted_iota(jnp.int32, (rows, KEY_TILE), 1)
    for start in range(0, length, KEY_TILE):
        tile = lax.dot_general(q_rows, k_ref[start:start + KEY_TILE, :], contract_last, preferred_element_type=jnp.float32)
        tile = jnp.where(lane < seq_len - start, tile, -jnp.inf)
        score_ref[:, start:start + KEY_TILE] = tile
        best = tile if best is None else jnp.maximum(best, tile)
    top = jnp.maximum(jnp.max(best, axis=-1, keepdims=True), jnp.max(new_scores, axis=-1, keepdims=True))
    new_weights = jnp.exp2((new_scores - top) * to_log2)
    numerator = jnp.dot(new_weights.astype(jnp.bfloat16), fresh_v, preferred_element_type=jnp.float32)
    total = None
    for start in range(0, length, KEY_TILE):
        weights = jnp.exp2((score_ref[:, start:start + KEY_TILE] - top) * to_log2)
        total = weights if total is None else total + weights
        numerator = numerator + jnp.dot(weights.astype(jnp.bfloat16), v_ref[start:start + KEY_TILE, :], preferred_element_type=jnp.float32)
    denominator = jnp.sum(total, axis=-1, keepdims=True) + jnp.sum(new_weights, axis=-1, keepdims=True)
    return numerator / denominator


def attention_kernel(n_steps, len_ref, q_ref, fk_ref, fv_ref, k_hbm, v_hbm, out_ref, k_out, v_out, k_buf, v_buf, score_buf, sems, out_sems):
    n_seqs, rows, depth = q_ref.shape
    length = k_buf.shape[1]

    def fetch(b):
        return (pltpu.make_async_copy(k_hbm.at[b], k_buf.at[b], sems.at[0, b]),
                pltpu.make_async_copy(v_hbm.at[b], v_buf.at[b], sems.at[1, b]))

    def store(b):
        return (pltpu.make_async_copy(k_buf.at[b], k_out.at[b], out_sems.at[0, b]),
                pltpu.make_async_copy(v_buf.at[b], v_out.at[b], out_sems.at[1, b]))

    def patch(b, buf, fresh):
        start = pl.multiple_of(jnp.minimum(len_ref[b] // 8 * 8, length - WINDOW), 8)
        offset = len_ref[b] - start
        row = lax.broadcasted_iota(jnp.int32, (WINDOW, depth), 0)
        window = buf[b, pl.ds(start, WINDOW), :].astype(jnp.float32)
        for s in range(n_steps):
            window = jnp.where(row == offset + s, fresh[b, s:s + 1, :].astype(jnp.float32), window)
        buf[b, pl.ds(start, WINDOW), :] = window.astype(buf.dtype)

    for b in range(n_seqs):
        for copy in fetch(b):
            copy.start()
    shape = (rows, FRESH_ROWS)
    step_of_row = lax.broadcasted_iota(jnp.int32, shape, 0) // (rows // n_steps)
    fresh_mask = lax.broadcasted_iota(jnp.int32, shape, 1) <= step_of_row

    def body(i, carry):
        for j in range(2):
            b = 2 * i + j
            for copy in fetch(b):
                copy.wait()
            patch(b, k_buf, fk_ref)
            patch(b, v_buf, fv_ref)
            for copy in store(b):
                copy.start()
        for j in range(2):
            b = 2 * i + j
            out = attend_one(q_ref[b], k_buf.at[b], v_buf.at[b], score_buf.at[j], len_ref[b], fk_ref[b], fv_ref[b], fresh_mask)
            out_ref[b] = out.astype(out_ref.dtype)
        return carry

    lax.fori_loop(0, n_seqs // 2, body, 0)
    for b in range(n_seqs):
        for copy in store(b):
            copy.wait()


WINDOW = 16


def attention(q_rows, seq_lens, k_cache, v_cache, fresh_k, fresh_v, n_steps):
    n_seqs, rows, depth = q_rows.shape
    length = k_cache.shape[1]
    pad = ((0, 0), (0, FRESH_ROWS - n_steps), (0, 0))
    vmem = pl.BlockSpec(memory_space=pltpu.VMEM)
    hbm = pl.BlockSpec(memory_space=pl.ANY)
    return pl.pallas_call(
        functools.partial(attention_kernel, n_steps),
        out_shape=[jax.ShapeDtypeStruct(q_rows.shape, jnp.bfloat16), jax.ShapeDtypeStruct(k_cache.shape, k_cache.dtype), jax.ShapeDtypeStruct(v_cache.shape, v_cache.dtype)],
        in_specs=[pl.BlockSpec(memory_space=pltpu.SMEM), vmem, vmem, vmem, hbm, hbm],
        out_specs=[vmem, hbm, hbm],
        scratch_shapes=[
            pltpu.VMEM((n_seqs, length, depth), jnp.bfloat16),
            pltpu.VMEM((n_seqs, length, depth), jnp.bfloat16),
            pltpu.VMEM((2, rows, length), jnp.float32),
            pltpu.SemaphoreType.DMA((2, n_seqs)),
            pltpu.SemaphoreType.DMA((2, n_seqs)),
        ],
        compiler_params=pltpu.CompilerParams(vmem_limit_bytes=VMEM_LIMIT),
        cost_estimate=pl.CostEstimate(flops=4 * n_seqs * rows * length * depth, bytes_accessed=8 * n_seqs * length * depth, transcendentals=n_seqs * rows * length),
    )(seq_lens, q_rows, jnp.pad(fresh_k, pad), jnp.pad(fresh_v, pad), k_cache, v_cache)


def solution(mesh):
    tp_size = mesh.shape['tp']

    def local_block(x_steps, seq_lens, k_cache, v_cache, ln_gain, ln_bias, w_q, b_q, w_kv, b_kv, w_out, b_out):
        n_steps, group_rows, width = x_steps.shape
        local_rows, _, head_dim = k_cache.shape
        q_part_width = w_q.shape[1]
        n_heads = q_part_width * tp_size // head_dim
        row_start = lax.axis_index('tp') * local_rows
        normed = layer_norm(x_steps, ln_gain, ln_bias)
        q_part = (jnp.einsum('sbk,kn->sbn', normed, w_q, preferred_element_type=jnp.float32) + b_q.astype(jnp.float32)).astype(jnp.bfloat16)
        q_local = lax.all_to_all(q_part, 'tp', 1, 2, tiled=True)
        own_normed = lax.dynamic_slice_in_dim(normed, row_start, local_rows, axis=1)
        kv_rows = (jnp.einsum('sbk,kn->bsn', own_normed, w_kv, preferred_element_type=jnp.float32) + b_kv.astype(jnp.float32)).astype(jnp.bfloat16)
        fresh_k, fresh_v = kv_rows[:, :, :head_dim], kv_rows[:, :, head_dim:]
        q_rows = q_local.reshape(n_steps, local_rows, n_heads, head_dim).transpose(1, 0, 2, 3).reshape(local_rows, n_steps * n_heads, head_dim)
        attn, k_out, v_out = attention(q_rows, seq_lens, k_cache, v_cache, fresh_k, fresh_v, n_steps)
        attn = attn.reshape(local_rows, n_steps, n_heads * head_dim).transpose(1, 0, 2)
        attn_heads = lax.all_to_all(attn, 'tp', 2, 1, tiled=True)
        proj_part = jnp.einsum('sbk,kn->sbn', attn_heads, w_out, preferred_element_type=jnp.float32).astype(jnp.bfloat16)
        proj_sum = lax.psum(proj_part, 'tp')
        y_steps = (x_steps.astype(jnp.float32) + proj_sum.astype(jnp.float32) + b_out.astype(jnp.float32)).astype(jnp.bfloat16)
        return y_steps, k_out, v_out

    row_spec = P(('dp', 'tp'), None, None)
    return jax.shard_map(
        local_block,
        mesh=mesh,
        in_specs=(P(None, 'dp', None), P(('dp', 'tp')), row_spec, row_spec, P(None), P(None), P(None, 'tp'), P('tp'), P(None, None), P(None), P('tp', None), P(None)),
        out_specs=(P(None, 'dp', None), row_spec, row_spec),
        check_vma=False,
    )
```

```python
import functools
import math

import jax
import jax.numpy as jnp
from jax import lax
from jax.experimental import pallas as pl
from jax.experimental.pallas import tpu as pltpu
from jax.sharding import PartitionSpec as P

LN_EPS = 1e-5
KEY_TILE = 256
FRESH_ROWS = 16
VMEM_LIMIT = 60 * 1024 * 1024


def layer_norm(x_rows, ln_gain, ln_bias):
    x_float = x_rows.astype(jnp.float32)
    row_mean = jnp.mean(x_float, axis=-1, keepdims=True)
    centered = x_float - row_mean
    row_var = jnp.mean(centered * centered, axis=-1, keepdims=True)
    scaled = centered * lax.rsqrt(row_var + LN_EPS)
    return (scaled * ln_gain.astype(jnp.float32) + ln_bias.astype(jnp.float32)).astype(jnp.bfloat16)


def attend_one(q_rows, k_ref, v_ref, score_ref, seq_len, fresh_k, fresh_v, fresh_mask):
    rows, depth = q_rows.shape
    length = k_ref.shape[0]
    to_log2 = depth ** -0.5 * math.log2(math.e)
    contract_last = (((1,), (1,)), ((), ()))
    new_scores = lax.dot_general(q_rows, fresh_k, contract_last, preferred_element_type=jnp.float32)
    new_scores = jnp.where(fresh_mask, new_scores, -jnp.inf)
    best = None
    lane = lax.broadcasted_iota(jnp.int32, (rows, KEY_TILE), 1)
    for start in range(0, length, KEY_TILE):
        tile = lax.dot_general(q_rows, k_ref[start:start + KEY_TILE, :], contract_last, preferred_element_type=jnp.float32)
        tile = jnp.where(lane < seq_len - start, tile, -jnp.inf)
        score_ref[:, start:start + KEY_TILE] = tile
        best = tile if best is None else jnp.maximum(best, tile)
    top = jnp.maximum(jnp.max(best, axis=-1, keepdims=True), jnp.max(new_scores, axis=-1, keepdims=True))
    new_weights = jnp.exp2((new_scores - top) * to_log2)
    numerator = jnp.dot(new_weights.astype(jnp.bfloat16), fresh_v, preferred_element_type=jnp.float32)
    total = None
    for start in range(0, length, KEY_TILE):
        weights = jnp.exp2((score_ref[:, start:start + KEY_TILE] - top) * to_log2)
        total = weights if total is None else total + weights
        numerator = numerator + jnp.dot(weights.astype(jnp.bfloat16), v_ref[start:start + KEY_TILE, :], preferred_element_type=jnp.float32)
    denominator = jnp.sum(total, axis=-1, keepdims=True) + jnp.sum(new_weights, axis=-1, keepdims=True)
    return numerator / denominator


def attention_kernel(n_steps, len_ref, q_ref, fk_ref, fv_ref, k_hbm, v_hbm, out_ref, k_out, v_out, k_buf, v_buf, score_buf, head_buf, sems, out_sems):
    n_seqs, rows, depth = q_ref.shape
    length = k_buf.shape[1]

    def fetch(b):
        return (pltpu.make_async_copy(k_hbm.at[b], k_buf.at[b], sems.at[0, b]),
                pltpu.make_async_copy(v_hbm.at[b], v_buf.at[b], sems.at[1, b]))

    def store(b):
        return (pltpu.make_async_copy(k_buf.at[b], k_out.at[b], out_sems.at[0, b]),
                pltpu.make_async_copy(v_buf.at[b], v_out.at[b], out_sems.at[1, b]))

    def patch(b, buf, fresh):
        start = pl.multiple_of(jnp.minimum(len_ref[b] // 8 * 8, length - WINDOW), 8)
        offset = len_ref[b] - start
        row = lax.broadcasted_iota(jnp.int32, (WINDOW, depth), 0)
        window = buf[b, pl.ds(start, WINDOW), :].astype(jnp.float32)
        for s in range(n_steps):
            window = jnp.where(row == offset + s, fresh[b, s:s + 1, :].astype(jnp.float32), window)
        buf[b, pl.ds(start, WINDOW), :] = window.astype(buf.dtype)

    for b in range(n_seqs):
        for copy in fetch(b):
            copy.start()
    shape = (rows, FRESH_ROWS)
    step_of_row = lax.broadcasted_iota(jnp.int32, shape, 0) // (rows // n_steps)
    fresh_mask = lax.broadcasted_iota(jnp.int32, shape, 1) <= step_of_row

    def body(i, carry):
        for j in range(2):
            b = 2 * i + j
            for copy in fetch(b):
                copy.wait()
            patch(b, k_buf, fk_ref)
            patch(b, v_buf, fv_ref)
            for copy in store(b):
                copy.start()
        for j in range(2):
            b = 2 * i + j
            out = attend_one(q_ref[b], k_buf.at[b], v_buf.at[b], score_buf.at[j], len_ref[b], fk_ref[b], fv_ref[b], fresh_mask)
            head_buf[pl.ds(b, rows, stride=n_seqs), :] = out
        return carry

    lax.fori_loop(0, n_seqs // 2, body, 0)
    n_chips, _, _, chip_width = out_ref.shape
    chip_heads = chip_width // depth
    for chip in range(n_chips):
        for s in range(n_steps):
            for h in range(chip_heads):
                first = ((s * n_chips + chip) * chip_heads + h) * n_seqs
                out_ref[chip, s, :, h * depth:(h + 1) * depth] = head_buf[first:first + n_seqs, :].astype(out_ref.dtype)
    for b in range(n_seqs):
        for copy in store(b):
            copy.wait()


WINDOW = 16


def attention(q_rows, seq_lens, k_cache, v_cache, fresh_k, fresh_v, n_steps, n_chips):
    n_seqs, rows, depth = q_rows.shape
    length = k_cache.shape[1]
    pad = ((0, 0), (0, FRESH_ROWS - n_steps), (0, 0))
    vmem = pl.BlockSpec(memory_space=pltpu.VMEM)
    hbm = pl.BlockSpec(memory_space=pl.ANY)
    return pl.pallas_call(
        functools.partial(attention_kernel, n_steps),
        out_shape=[jax.ShapeDtypeStruct((n_chips, n_steps, n_seqs, rows // n_steps // n_chips * depth), jnp.bfloat16), jax.ShapeDtypeStruct(k_cache.shape, k_cache.dtype), jax.ShapeDtypeStruct(v_cache.shape, v_cache.dtype)],
        in_specs=[pl.BlockSpec(memory_space=pltpu.SMEM), vmem, vmem, vmem, hbm, hbm],
        out_specs=[vmem, hbm, hbm],
        scratch_shapes=[
            pltpu.VMEM((n_seqs, length, depth), jnp.bfloat16),
            pltpu.VMEM((n_seqs, length, depth), jnp.bfloat16),
            pltpu.VMEM((2, rows, length), jnp.float32),
            pltpu.VMEM((rows * n_seqs, depth), jnp.float32),
            pltpu.SemaphoreType.DMA((2, n_seqs)),
            pltpu.SemaphoreType.DMA((2, n_seqs)),
        ],
        compiler_params=pltpu.CompilerParams(vmem_limit_bytes=VMEM_LIMIT),
        cost_estimate=pl.CostEstimate(flops=4 * n_seqs * rows * length * depth, bytes_accessed=8 * n_seqs * length * depth, transcendentals=n_seqs * rows * length),
    )(seq_lens, q_rows, jnp.pad(fresh_k, pad), jnp.pad(fresh_v, pad), k_cache, v_cache)


MESH = pl.DeviceIdType.MESH
N_CHIPS = 4


def project_kernel(n_steps, a_ref, w_ref, x_ref, b_ref, y_ref, w_buf, x_buf, a_buf, p_buf, mid_buf, fin_buf,
                   load_sems, w_sems, a_send, a_recv, f_send, f_recv, rs_send, rs_recv, ag_send, ag_recv):
    me = lax.axis_index('tp')
    chip, core = me // 2, me % 2
    n_seqs = a_ref.shape[2]
    block = 2 * n_seqs
    own_rows, width = w_ref.shape
    half = width // 2
    quarter = half // 2

    def chip_at(k):
        return (chip + k) % N_CHIPS

    def device(k):
        return {'tp': chip_at(k) * 2 + core}

    right, left, far, partner = device(1), device(3), device(2), {'tp': chip * 2 + 1 - core}

    barrier = pltpu.get_barrier_semaphore()
    for peer in (right, left, far, partner):
        pl.semaphore_signal(barrier, inc=1, device_id=peer, device_id_type=MESH)

    def cols(which, begin, size):
        return pl.ds(pl.multiple_of(which * half + begin, quarter), size)

    def rows_of(k):
        return pl.ds(pl.multiple_of(chip_at(k) * block, block), block)

    own_w_rows = pl.ds(pl.multiple_of(core * own_rows, own_rows), own_rows)
    w_load = pltpu.make_async_copy(w_ref.at[:, cols(core, 0, half)], w_buf.at[own_w_rows, :], load_sems.at[0])
    x_load = pltpu.make_async_copy(x_ref.at[:, rows_of(0), cols(core, 0, half)], x_buf, load_sems.at[1])
    w_load.start()
    x_load.start()
    pl.semaphore_wait(barrier, 4)

    def remote(src, dst, send, recv, to):
        return pltpu.make_async_remote_copy(src_ref=src, dst_ref=dst, send_sem=send, recv_sem=recv, device_id=to, device_id_type=MESH)

    def a_copy(s, d):
        return remote(a_ref.at[chip_at(d), s], a_buf.at[core, chip, s], a_send.at[s, d - 1], a_recv.at[s, d - 1], device(d))

    def a_forward(s, d):
        src = a_ref.at[chip, s] if d == 0 else a_buf.at[core, chip_at(N_CHIPS - d), s]
        return remote(src, a_buf.at[core, chip_at(N_CHIPS - d), s], f_send.at[s, d], f_recv.at[s, d], partner)

    for s in range(n_steps):
        for d in (2, 1, 3):
            a_copy(s, d).start()
        if s == 0:
            w_swap = remote(w_ref.at[:, cols(1 - core, 0, half)], w_buf.at[own_w_rows, :], w_sems.at[0], w_sems.at[1], partner)
            w_swap.start()
    for s in range(n_steps):
        a_forward(s, 0).start()
        a_buf[core, chip, s] = a_ref[chip, s]

    low, high = pl.ds(0, quarter), pl.ds(quarter, quarter)

    def rs(s, i):
        part = p_buf.at[s]
        src, dst, to = (
            (part.at[rows_of(2), low], mid_buf.at[s, 0], right),
            (part.at[rows_of(2), high], mid_buf.at[s, 1], left),
            (part.at[rows_of(1), high], fin_buf.at[s, 0], right),
            (part.at[rows_of(3), low], fin_buf.at[s, 1], left),
            (part.at[rows_of(1), low], fin_buf.at[s, 2], right),
            (part.at[rows_of(3), high], fin_buf.at[s, 3], left),
        )[i]
        return remote(src, dst, rs_send.at[s, i], rs_recv.at[s, i], to)

    def ag(s, i):
        k, begin, size, to = (
            (0, 0, half, right),
            (0, 0, half, left),
            (3, 0, quarter, right),
            (1, quarter, quarter, left),
            (0, 0, half, partner),
            (3, 0, half, partner),
            (1, 0, half, partner),
            (2, 0, quarter, partner),
            (2, quarter, quarter, partner),
        )[i]
        where = y_ref.at[s, rows_of(k), cols(core, begin, size)]
        return remote(where, where, ag_send.at[s, i], ag_recv.at[s, i], to)

    def partial(s):
        for d in (1, 3, 2):
            a_copy(s, d).wait_recv()
            a_forward(s, d).start()
        for d in range(N_CHIPS):
            a_forward(s, d).wait_recv()
        if s == 0:
            w_load.wait()
            w_swap.wait_recv()
        lhs = jnp.concatenate([a_buf[c, t, s] for t in range(N_CHIPS) for c in range(2)], axis=0)
        for n in range(0, half, 512):
            p_buf[s, :, n:n + 512] = jnp.dot(lhs, w_buf[:, n:n + 512], preferred_element_type=jnp.float32).astype(p_buf.dtype)
        for i in range(4):
            rs(s, i).start()

    def add_into(target, other):
        target[...] = (target[...].astype(jnp.float32) + other[...].astype(jnp.float32)).astype(target.dtype)

    def middle(s):
        rs(s, 0).wait_recv()
        add_into(p_buf.at[s, rows_of(1), low], mid_buf.at[s, 0])
        rs(s, 4).start()
        rs(s, 1).wait_recv()
        add_into(p_buf.at[s, rows_of(3), high], mid_buf.at[s, 1])
        rs(s, 5).start()

    def finish(s):
        for i in (2, 3, 4, 5):
            rs(s, i).wait_recv()
        if s == 0:
            x_load.wait()
        for begin, one, two in ((0, 1, 2), (quarter, 0, 3)):
            total = p_buf[s, rows_of(0), begin:begin + quarter].astype(jnp.float32)
            total = total + fin_buf[s, one].astype(jnp.float32)
            total = total + fin_buf[s, two].astype(jnp.float32)
            total = total + x_buf[s, :, begin:begin + quarter].astype(jnp.float32)
            total = total + b_ref[:, cols(core, begin, quarter)].astype(jnp.float32)
            y_ref[s, rows_of(0), cols(core, begin, quarter)] = total.astype(y_ref.dtype)
        for i in (0, 1, 4):
            ag(s, i).start()

    def relay(s):
        ag(s, 0).wait_recv()
        ag(s, 2).start()
        ag(s, 5).start()
        ag(s, 1).wait_recv()
        ag(s, 3).start()
        ag(s, 6).start()

    def last(s):
        ag(s, 2).wait_recv()
        ag(s, 7).start()
        ag(s, 3).wait_recv()
        ag(s, 8).start()

    stages = (partial, middle, finish, relay, last)
    for t in range(n_steps + len(stages) - 1):
        for i, stage in enumerate(stages):
            if 0 <= t - i < n_steps:
                stage(t - i)
    w_swap.wait_send()
    for s in range(n_steps):
        for i in range(4, 9):
            ag(s, i).wait_recv()
        for i in range(9):
            ag(s, i).wait_send()
        for i in range(6):
            rs(s, i).wait_send()
        for d in (1, 2, 3):
            a_copy(s, d).wait_send()
        for d in range(N_CHIPS):
            a_forward(s, d).wait_send()


def project(attn, w_out, x_steps, b_out):
    n_chips, n_steps, n_seqs, chip_width = attn.shape
    width = w_out.shape[1]
    half, block = width // 2, 2 * n_seqs
    vmem = pl.BlockSpec(memory_space=pltpu.VMEM)
    hbm = pl.BlockSpec(memory_space=pl.ANY)
    dma = pltpu.SemaphoreType.DMA
    return pl.pallas_call(
        functools.partial(project_kernel, n_steps),
        out_shape=jax.ShapeDtypeStruct(x_steps.shape, jnp.bfloat16),
        in_specs=[vmem, hbm, hbm, vmem],
        out_specs=vmem,
        scratch_shapes=[
            pltpu.VMEM((chip_width, half), jnp.bfloat16),
            pltpu.VMEM((n_steps, block, half), jnp.bfloat16),
            pltpu.VMEM((2, n_chips, n_steps, n_seqs, chip_width), jnp.bfloat16),
            pltpu.VMEM((n_steps, n_chips * block, half), jnp.bfloat16),
            pltpu.VMEM((n_steps, 2, block, half // 2), jnp.bfloat16),
            pltpu.VMEM((n_steps, 4, block, half // 2), jnp.bfloat16),
            dma((2,)), dma((2,)),
            dma((n_steps, 3)), dma((n_steps, 3)),
            dma((n_steps, 4)), dma((n_steps, 4)),
            dma((n_steps, 6)), dma((n_steps, 6)),
            dma((n_steps, 9)), dma((n_steps, 9)),
        ],
        compiler_params=pltpu.CompilerParams(vmem_limit_bytes=40 * 1024 * 1024, collective_id=1, has_side_effects=True),
        cost_estimate=pl.CostEstimate(flops=2 * n_steps * n_chips * block * chip_width * half, bytes_accessed=4 * width * chip_width, transcendentals=0),
    )(attn, w_out, x_steps, b_out.reshape(1, width))


def solution(mesh):
    tp_size = mesh.shape['tp']

    def local_block(x_steps, seq_lens, k_cache, v_cache, ln_gain, ln_bias, w_q, b_q, w_kv, b_kv, w_out, b_out):
        n_steps, group_rows, width = x_steps.shape
        local_rows, _, head_dim = k_cache.shape
        q_part_width = w_q.shape[1]
        n_heads = q_part_width * tp_size // head_dim
        row_start = lax.axis_index('tp') * local_rows
        normed = layer_norm(x_steps, ln_gain, ln_bias)
        q_part = (jnp.einsum('sbk,kn->sbn', normed, w_q, preferred_element_type=jnp.float32) + b_q.astype(jnp.float32)).astype(jnp.bfloat16)
        q_local = lax.all_to_all(q_part, 'tp', 1, 2, tiled=True)
        own_normed = lax.dynamic_slice_in_dim(normed, row_start, local_rows, axis=1)
        kv_rows = (jnp.einsum('sbk,kn->bsn', own_normed, w_kv, preferred_element_type=jnp.float32) + b_kv.astype(jnp.float32)).astype(jnp.bfloat16)
        fresh_k, fresh_v = kv_rows[:, :, :head_dim], kv_rows[:, :, head_dim:]
        q_rows = q_local.reshape(n_steps, local_rows, n_heads, head_dim).transpose(1, 0, 2, 3).reshape(local_rows, n_steps * n_heads, head_dim)
        attn, k_out, v_out = attention(q_rows, seq_lens, k_cache, v_cache, fresh_k, fresh_v, n_steps, N_CHIPS)
        y_steps = project(attn, w_out, x_steps, b_out)
        return y_steps, k_out, v_out

    row_spec = P(('dp', 'tp'), None, None)
    return jax.shard_map(
        local_block,
        mesh=mesh,
        in_specs=(P(None, 'dp', None), P(('dp', 'tp')), row_spec, row_spec, P(None), P(None), P(None, 'tp'), P('tp'), P(None, None), P(None), P('tp', None), P(None)),
        out_specs=(P(None, 'dp', None), row_spec, row_spec),
        check_vma=False,
    )
```

```python
import functools
import math

import jax
import jax.numpy as jnp
from jax import lax
from jax.experimental import pallas as pl
from jax.experimental.pallas import tpu as pltpu
from jax.sharding import PartitionSpec as P

LN_EPS = 1e-5
KEY_TILE = 256
FRESH_ROWS = 16
WINDOW = 16
N_CHIPS = 4
N_CORES = 2
N_PARTS = 2
LN_ROWS = 16
MESH = pl.DeviceIdType.MESH
BLOCK_VMEM = 32 * 1024 * 1024


def attend_one(q_rows, k_ref, v_ref, score_ref, seq_len, fresh_k, fresh_v, fresh_mask):
    rows, depth = q_rows.shape
    length = k_ref.shape[0]
    to_log2 = depth ** -0.5 * math.log2(math.e)
    contract_last = (((1,), (1,)), ((), ()))
    new_scores = lax.dot_general(q_rows, fresh_k, contract_last, preferred_element_type=jnp.float32)
    new_scores = jnp.where(fresh_mask, new_scores, -jnp.inf)
    best = None
    lane = lax.broadcasted_iota(jnp.int32, (rows, KEY_TILE), 1)
    for start in range(0, length, KEY_TILE):
        tile = lax.dot_general(q_rows, k_ref[start:start + KEY_TILE, :], contract_last, preferred_element_type=jnp.float32)
        tile = jnp.where(lane < seq_len - start, tile, -jnp.inf)
        score_ref[:, start:start + KEY_TILE] = tile
        best = tile if best is None else jnp.maximum(best, tile)
    top = jnp.maximum(jnp.max(best, axis=-1, keepdims=True), jnp.max(new_scores, axis=-1, keepdims=True))
    new_weights = jnp.exp2((new_scores - top) * to_log2)
    numerator = jnp.dot(new_weights.astype(jnp.bfloat16), fresh_v, preferred_element_type=jnp.float32)
    total = None
    for start in range(0, length, KEY_TILE):
        weights = jnp.exp2((score_ref[:, start:start + KEY_TILE] - top) * to_log2)
        total = weights if total is None else total + weights
        numerator = numerator + jnp.dot(weights.astype(jnp.bfloat16), v_ref[start:start + KEY_TILE, :], preferred_element_type=jnp.float32)
    denominator = jnp.sum(total, axis=-1, keepdims=True) + jnp.sum(new_weights, axis=-1, keepdims=True)
    return numerator / denominator


def block_kernel(
        len_ref, g_ref, lb_ref, bq_ref, bkv_ref, bo_ref, x_hbm, wq_hbm, wkv_hbm, wo_hbm, k_hbm, v_hbm,
        y_ref, k_buf, v_buf, fk_ref, fv_ref,
        x_buf, h_buf, gain_buf, bias_buf, wq_buf, wkv_buf, w_buf, q_buf, q_in, q_rows, score_buf, head_buf, a_src, a_buf, lhs_buf, p_buf, mid_buf, fin_buf,
        x_sems, w_sems, kv_sems, swap_sems, q_send, q_recv, a_send, a_recv, f_send, f_recv, rs_send, rs_recv, ag_send, ag_recv):
    me = lax.axis_index('tp')
    n_dev = N_CHIPS * N_CORES
    chip, core = me // N_CORES, me % N_CORES
    n_steps, group_rows, width = x_buf.shape
    n_seqs, length, depth = k_buf.shape
    q_width = wq_buf.shape[1]
    dev_heads = q_width // depth
    chip_heads = N_CORES * dev_heads
    part_seqs = n_seqs // N_PARTS
    rows = n_dev * n_steps * dev_heads
    own_rows = wo_hbm.shape[0]
    half, quarter = width // 2, width // 4
    block = n_steps * N_CORES * part_seqs

    def chip_at(k):
        return (chip + k) % N_CHIPS

    def device(k):
        return {'tp': chip_at(k) * N_CORES + core}

    def member(d):
        return (me + d) % n_dev

    right, left, partner = device(1), device(3), {'tp': chip * N_CORES + 1 - core}

    def remote(src, dst, send, recv, to):
        return pltpu.make_async_remote_copy(src_ref=src, dst_ref=dst, send_sem=send, recv_sem=recv, device_id=to, device_id_type=MESH)

    def cols(which, begin, size):
        return pl.ds(pl.multiple_of(which * half + begin, quarter), size)

    def seq_rows(d):
        return pl.ds(pl.multiple_of(member(d) * n_seqs, n_seqs), n_seqs)

    barrier = pltpu.get_barrier_semaphore()
    for d in range(1, n_dev):
        pl.semaphore_signal(barrier, inc=1, device_id={'tp': member(d)}, device_id_type=MESH)

    def x_load(s):
        return pltpu.make_async_copy(x_hbm.at[s], x_buf.at[s], x_sems.at[s])

    def kv_load(b):
        return (pltpu.make_async_copy(k_hbm.at[b], k_buf.at[b], kv_sems.at[0, b]),
                pltpu.make_async_copy(v_hbm.at[b], v_buf.at[b], kv_sems.at[1, b]))

    own_w_rows = pl.ds(pl.multiple_of(core * own_rows, own_rows), own_rows)
    wq_load = pltpu.make_async_copy(wq_hbm, wq_buf, w_sems.at[0])
    wkv_load = pltpu.make_async_copy(wkv_hbm, wkv_buf, w_sems.at[1])
    wo_load = pltpu.make_async_copy(wo_hbm.at[:, cols(core, 0, half)], w_buf.at[own_w_rows, :], w_sems.at[2])
    wo_swap = remote(wo_hbm.at[:, cols(1 - core, 0, half)], w_buf.at[own_w_rows, :], swap_sems.at[0], swap_sems.at[1], partner)
    for s in range(n_steps):
        x_load(s).start()
    wq_load.start()
    wkv_load.start()

    gain_buf[...] = jnp.broadcast_to(g_ref[...].astype(jnp.float32), gain_buf.shape)
    bias_buf[...] = jnp.broadcast_to(lb_ref[...].astype(jnp.float32), bias_buf.shape)

    def q_copy(s, d):
        return remote(q_buf.at[s, seq_rows(d)], q_in.at[me, s], q_send.at[s, d - 1], q_recv.at[s, d - 1], {'tp': member(d)})

    for s in range(n_steps):
        x_load(s).wait()

        def norm_rows(i, carry):
            where = pl.ds(pl.multiple_of(i * LN_ROWS, LN_ROWS), LN_ROWS)
            x_float = x_buf[s, where, :].astype(jnp.float32)
            centered = x_float - jnp.mean(x_float, axis=-1, keepdims=True)
            row_var = jnp.mean(centered * centered, axis=-1, keepdims=True)
            scaled = centered * lax.rsqrt(row_var + LN_EPS)
            h_buf[s, where, :] = (scaled * gain_buf[...] + bias_buf[...]).astype(h_buf.dtype)
            return carry

        lax.fori_loop(0, group_rows // LN_ROWS, norm_rows, 0)
        if s == 0:
            wq_load.wait()
            wo_load.start()
            for b in range(n_seqs):
                for copy in kv_load(b):
                    copy.start()
        for n in range(0, q_width, 256):
            part = jnp.dot(h_buf[s], wq_buf[:, n:n + 256], preferred_element_type=jnp.float32)
            q_buf[s, :, n:n + 256] = (part + bq_ref[:, n:n + 256].astype(jnp.float32)).astype(q_buf.dtype)
        if s == 0:
            pl.semaphore_wait(barrier, n_dev - 1)
        for d in range(1, n_dev):
            q_copy(s, d).start()
        if s == 0:
            wo_swap.start()
        q_in[me, s] = q_buf[s, seq_rows(0), :]

    wkv_load.wait()
    own_h = jnp.concatenate([h_buf[s, seq_rows(0), :] for s in range(n_steps)], axis=0)
    fresh = jnp.dot(own_h, wkv_buf[...], preferred_element_type=jnp.float32) + bkv_ref[...].astype(jnp.float32)
    fresh = fresh.astype(jnp.bfloat16).astype(jnp.float32)
    fk_ref[...] = jnp.zeros_like(fk_ref)
    fv_ref[...] = jnp.zeros_like(fv_ref)
    for s in range(n_steps):
        where = pl.ds(s, n_seqs, stride=FRESH_ROWS)
        fk_ref[where, :] = fresh[s * n_seqs:(s + 1) * n_seqs, :depth]
        fv_ref[where, :] = fresh[s * n_seqs:(s + 1) * n_seqs, depth:]

    for s in range(n_steps):
        for d in range(1, n_dev):
            q_copy(s, d).wait_recv()
    for u in range(n_dev):
        for s in range(n_steps):
            for h in range(dev_heads):
                first = ((u * n_steps + s) * dev_heads + h) * n_seqs
                q_rows[first:first + n_seqs, :] = q_in[u, s, :, h * depth:(h + 1) * depth].astype(jnp.float32)

    shape = (rows, FRESH_ROWS)
    step_of_row = lax.broadcasted_iota(jnp.int32, shape, 0) // dev_heads % n_steps
    fresh_mask = lax.broadcasted_iota(jnp.int32, shape, 1) <= step_of_row

    def a_copy(p, d):
        return remote(a_src.at[p, chip_at(d)], a_buf.at[p, core, chip], a_send.at[p, d - 1], a_recv.at[p, d - 1], device(d))

    def a_forward(p, d):
        where = a_buf.at[p, core, chip_at(N_CHIPS - d)]
        return remote(a_src.at[p, chip] if d == 0 else where, where, f_send.at[p, d], f_recv.at[p, d], partner)

    low, high = pl.ds(0, quarter), pl.ds(quarter, quarter)

    def rs(p, i):
        def part(k, where):
            return p_buf.at[p, chip_at(k), :, where]
        src, dst, to = (
            (part(2, low), mid_buf.at[p, 0], right),
            (part(2, high), mid_buf.at[p, 1], left),
            (part(1, high), fin_buf.at[p, 0], right),
            (part(3, low), fin_buf.at[p, 1], left),
            (part(1, low), fin_buf.at[p, 2], right),
            (part(3, high), fin_buf.at[p, 3], left),
        )[i]
        return remote(src, dst, rs_send.at[p, i], rs_recv.at[p, i], to)

    def ag(p, i):
        k, begin, size, to = (
            (0, 0, half, right),
            (0, 0, half, left),
            (3, 0, quarter, right),
            (1, quarter, quarter, left),
            (0, 0, half, partner),
            (3, 0, half, partner),
            (1, 0, half, partner),
            (2, 0, quarter, partner),
            (2, quarter, quarter, partner),
        )[i]
        where = y_ref.at[:, chip_at(k), :, p, :, cols(core, begin, size)]
        return remote(where, where, ag_send.at[p, i], ag_recv.at[p, i], to)

    def pack(p):
        for t in range(N_CHIPS):
            for s in range(n_steps):
                pieces = []
                for h in range(chip_heads):
                    u = t * N_CORES + h // dev_heads
                    first = ((u * n_steps + s) * dev_heads + h % dev_heads) * n_seqs + p * part_seqs
                    pieces.append(head_buf[first:first + part_seqs, :])
                a_src[p, t, s] = jnp.concatenate(pieces, axis=1).astype(a_src.dtype)
        for d in (2, 1, 3):
            a_copy(p, d).start()
        a_forward(p, 0).start()
        a_buf[p, core, chip] = a_src[p, chip]

    def forward(p):
        for d in (1, 3, 2):
            a_copy(p, d).wait_recv()
            a_forward(p, d).start()

    def partial(p):
        for d in range(N_CHIPS):
            a_forward(p, d).wait_recv()
        if p == 0:
            wo_load.wait()
            wo_swap.wait_recv()
        for t in range(N_CHIPS):
            for s in range(n_steps):
                pair = jnp.concatenate([a_buf[p, c, t, s].astype(jnp.float32) for c in range(N_CORES)], axis=0)
                first = (t * n_steps + s) * N_CORES * part_seqs
                lhs_buf[first:first + N_CORES * part_seqs, :] = pair.astype(lhs_buf.dtype)
        for n in range(0, half, 512):
            out = jnp.dot(lhs_buf[...], w_buf[:, n:n + 512], preferred_element_type=jnp.float32).astype(p_buf.dtype)
            for t in range(N_CHIPS):
                p_buf[p, t, :, n:n + 512] = out[t * block:(t + 1) * block]
        for i in range(4):
            rs(p, i).start()

    def add_into(target, other):
        target[...] = (target[...].astype(jnp.float32) + other[...].astype(jnp.float32)).astype(target.dtype)

    def middle(p):
        rs(p, 0).wait_recv()
        add_into(p_buf.at[p, chip_at(1), :, low], mid_buf.at[p, 0])
        rs(p, 4).start()
        rs(p, 1).wait_recv()
        add_into(p_buf.at[p, chip_at(3), :, high], mid_buf.at[p, 1])
        rs(p, 5).start()

    def finish(p):
        for i in (2, 3, 4, 5):
            rs(p, i).wait_recv()
        chip_rows = pl.ds(pl.multiple_of(chip * N_CORES * n_seqs, N_CORES * n_seqs), N_CORES * n_seqs)
        for begin, one, two in ((0, 1, 2), (quarter, 0, 3)):
            where = cols(core, begin, quarter)
            total = p_buf[p, chip, :, begin:begin + quarter].astype(jnp.float32)
            total = total + fin_buf[p, one].astype(jnp.float32)
            total = total + fin_buf[p, two].astype(jnp.float32)
            total = total + bo_ref[:, where].astype(jnp.float32)
            for s in range(n_steps):
                x_part = x_buf[s, chip_rows, where].astype(jnp.float32)
                for c in range(N_CORES):
                    first = (s * N_CORES + c) * part_seqs
                    x_first = c * n_seqs + p * part_seqs
                    y_ref[s, chip, c, p, :, where] = (x_part[x_first:x_first + part_seqs] + total[first:first + part_seqs]).astype(y_ref.dtype)
        for i in (0, 1, 4):
            ag(p, i).start()

    def relay(p):
        ag(p, 0).wait_recv()
        ag(p, 2).start()
        ag(p, 5).start()
        ag(p, 1).wait_recv()
        ag(p, 3).start()
        ag(p, 6).start()

    def last(p):
        ag(p, 2).wait_recv()
        ag(p, 7).start()
        ag(p, 3).wait_recv()
        ag(p, 8).start()

    def attend_pair(i, carry):
        for j in range(2):
            for copy in kv_load(2 * i + j):
                copy.wait()
        for j in range(2):
            b = 2 * i + j
            q_one = q_rows[pl.ds(b, rows, stride=n_seqs), :].astype(jnp.bfloat16)
            new = pl.ds(pl.multiple_of(b * FRESH_ROWS, FRESH_ROWS), FRESH_ROWS)
            out = attend_one(q_one, k_buf.at[b], v_buf.at[b], score_buf.at[j], len_ref[b],
                             fk_ref[new, :].astype(jnp.bfloat16), fv_ref[new, :].astype(jnp.bfloat16), fresh_mask)
            head_buf[pl.ds(b, rows, stride=n_seqs), :] = out
        for at, stage in STAGES_BESIDE_ATTENTION:
            @pl.when(i == at)
            def _():
                {'pack': pack, 'forward': forward, 'partial': partial, 'middle': middle}[stage](0)
        return carry

    lax.fori_loop(0, n_seqs // 2, attend_pair, 0)
    pack(1)
    finish(0)
    forward(1)
    relay(0)
    partial(1)
    last(0)
    middle(1)
    finish(1)
    relay(1)
    last(1)
    wo_swap.wait_send()
    for s in range(n_steps):
        for d in range(1, n_dev):
            q_copy(s, d).wait_send()
    for p in range(N_PARTS):
        for i in range(4, 9):
            ag(p, i).wait_recv()
        for i in range(9):
            ag(p, i).wait_send()
        for i in range(6):
            rs(p, i).wait_send()
        for d in (1, 2, 3):
            a_copy(p, d).wait_send()
        for d in range(N_CHIPS):
            a_forward(p, d).wait_send()


STAGES_BESIDE_ATTENTION = ((3, 'pack'), (5, 'forward'), (5, 'partial'), (7, 'middle'))


def store_kernel(n_steps, len_ref, fk_ref, fv_ref, y_ref, k_ref, v_ref, y_out, k_out, v_out, k_buf, v_buf, sems, y_sem):
    n_seqs, length, depth = k_buf.shape

    def store(b):
        return (pltpu.make_async_copy(k_buf.at[b], k_out.at[b], sems.at[0, b]),
                pltpu.make_async_copy(v_buf.at[b], v_out.at[b], sems.at[1, b]))

    def patch(b, buf, fresh):
        start = pl.multiple_of(jnp.minimum(len_ref[b] // 8 * 8, length - WINDOW), 8)
        offset = len_ref[b] - start
        row = lax.broadcasted_iota(jnp.int32, (WINDOW, depth), 0)
        window = buf[b, pl.ds(start, WINDOW), :].astype(jnp.float32)
        for s in range(n_steps):
            window = jnp.where(row == offset + s, fresh[b * FRESH_ROWS + s:b * FRESH_ROWS + s + 1, :], window)
        buf[b, pl.ds(start, WINDOW), :] = window.astype(buf.dtype)

    y_copy = pltpu.make_async_copy(y_ref, y_out, y_sem)
    y_copy.start()
    for b in range(n_seqs):
        patch(b, k_buf, fk_ref)
        patch(b, v_buf, fv_ref)
        for copy in store(b):
            copy.start()
    y_copy.wait()
    for b in range(n_seqs):
        for copy in store(b):
            copy.wait()


def solution(mesh):
    def local_block(x_steps, seq_lens, k_cache, v_cache, ln_gain, ln_bias, w_q, b_q, w_kv, b_kv, w_out, b_out):
        n_steps, group_rows, width = x_steps.shape
        n_seqs, length, depth = k_cache.shape
        q_width, kv_width = w_q.shape[1], w_kv.shape[1]
        n_dev = N_CHIPS * N_CORES
        part_seqs = n_seqs // N_PARTS
        rows = n_dev * n_steps * q_width // depth
        chip_width, half = N_CORES * q_width, width // 2
        block = n_steps * N_CORES * part_seqs
        smem = pl.BlockSpec(memory_space=pltpu.SMEM)
        vmem = pl.BlockSpec(memory_space=pltpu.VMEM)
        hbm = pl.BlockSpec(memory_space=pl.ANY)
        dma = pltpu.SemaphoreType.DMA
        bf16, f32 = jnp.bfloat16, jnp.float32
        y_shape = (n_steps, N_CHIPS, N_CORES, N_PARTS, part_seqs, width)
        fresh_shape = (n_seqs * FRESH_ROWS, depth)
        y_vm, k_vm, v_vm, fresh_k, fresh_v = pl.pallas_call(
            block_kernel,
            out_shape=[pltpu.VMEM(y_shape, bf16), pltpu.VMEM(k_cache.shape, bf16), pltpu.VMEM(v_cache.shape, bf16), pltpu.VMEM(fresh_shape, f32), pltpu.VMEM(fresh_shape, f32)],
            in_specs=[smem] + [vmem] * 5 + [hbm] * 6,
            out_specs=[vmem] * 5,
            scratch_shapes=[
                pltpu.VMEM(x_steps.shape, bf16),
                pltpu.VMEM(x_steps.shape, bf16),
                pltpu.VMEM((LN_ROWS, width), f32),
                pltpu.VMEM((LN_ROWS, width), f32),
                pltpu.VMEM(w_q.shape, bf16),
                pltpu.VMEM(w_kv.shape, bf16),
                pltpu.VMEM((chip_width, half), bf16),
                pltpu.VMEM((n_steps, group_rows, q_width), bf16),
                pltpu.VMEM((n_dev, n_steps, n_seqs, q_width), bf16),
                pltpu.VMEM((rows * n_seqs, depth), f32),
                pltpu.VMEM((2, rows, length), f32),
                pltpu.VMEM((rows * n_seqs, depth), f32),
                pltpu.VMEM((N_PARTS, N_CHIPS, n_steps, part_seqs, chip_width), bf16),
                pltpu.VMEM((N_PARTS, N_CORES, N_CHIPS, n_steps, part_seqs, chip_width), bf16),
                pltpu.VMEM((N_CHIPS * block, chip_width), bf16),
                pltpu.VMEM((N_PARTS, N_CHIPS, block, half), bf16),
                pltpu.VMEM((N_PARTS, 2, block, half // 2), bf16),
                pltpu.VMEM((N_PARTS, 4, block, half // 2), bf16),
                dma((n_steps,)), dma((3,)), dma((2, n_seqs)), dma((2,)),
                dma((n_steps, n_dev - 1)), dma((n_steps, n_dev - 1)),
                dma((N_PARTS, 3)), dma((N_PARTS, 3)),
                dma((N_PARTS, N_CHIPS)), dma((N_PARTS, N_CHIPS)),
                dma((N_PARTS, 6)), dma((N_PARTS, 6)),
                dma((N_PARTS, 9)), dma((N_PARTS, 9)),
            ],
            compiler_params=pltpu.CompilerParams(vmem_limit_bytes=BLOCK_VMEM, collective_id=1, has_side_effects=True),
            cost_estimate=pl.CostEstimate(flops=4 * n_seqs * rows * length * depth, bytes_accessed=4 * n_seqs * length * depth, transcendentals=n_seqs * rows * length),
        )(seq_lens, ln_gain.reshape(1, width), ln_bias.reshape(1, width), b_q.reshape(1, q_width), b_kv.reshape(1, kv_width), b_out.reshape(1, width),
          x_steps, w_q, w_kv, w_out, k_cache, v_cache)
        y_steps, k_out, v_out, _, _ = pl.pallas_call(
            functools.partial(store_kernel, n_steps),
            out_shape=[jax.ShapeDtypeStruct(y_shape, bf16), jax.ShapeDtypeStruct(k_cache.shape, bf16), jax.ShapeDtypeStruct(v_cache.shape, bf16), pltpu.VMEM(k_cache.shape, bf16), pltpu.VMEM(v_cache.shape, bf16)],
            in_specs=[smem] + [vmem] * 5,
            out_specs=[hbm] * 3 + [vmem] * 2,
            scratch_shapes=[dma((2, n_seqs)), dma],
            input_output_aliases={4: 3, 5: 4},
            compiler_params=pltpu.CompilerParams(vmem_limit_bytes=2 * 1024 * 1024),
        )(seq_lens, fresh_k, fresh_v, y_vm, k_vm, v_vm)
        return y_steps.reshape(x_steps.shape), k_out, v_out

    row_spec = P(('dp', 'tp'), None, None)
    return jax.shard_map(
        local_block,
        mesh=mesh,
        in_specs=(P(None, 'dp', None), P(('dp', 'tp')), row_spec, row_spec, P(None), P(None), P(None, 'tp'), P('tp'), P(None, None), P(None), P('tp', None), P(None)),
        out_specs=(P(None, 'dp', None), row_spec, row_spec),
        check_vma=False,
    )
```

```python
import functools
import math

import jax
import jax.numpy as jnp
from jax import lax
from jax.experimental import pallas as pl
from jax.experimental.pallas import tpu as pltpu
from jax.sharding import PartitionSpec as P

LN_EPS = 1e-5
KEY_TILE = 256
FRESH_ROWS = 16
WINDOW = 16
N_CHIPS = 4
N_CORES = 2
N_PARTS = 2
LN_ROWS = 16
MESH = pl.DeviceIdType.MESH
BLOCK_VMEM = 32 * 1024 * 1024


def attend_one(q_rows, k_ref, v_ref, score_ref, seq_len, fresh_k, fresh_v, fresh_mask):
    rows, depth = q_rows.shape
    length = k_ref.shape[0]
    to_log2 = depth ** -0.5 * math.log2(math.e)
    contract_last = (((1,), (1,)), ((), ()))
    new_scores = lax.dot_general(q_rows, fresh_k, contract_last, preferred_element_type=jnp.float32)
    new_scores = jnp.where(fresh_mask, new_scores, -jnp.inf)
    best = None
    lane = lax.broadcasted_iota(jnp.int32, (rows, KEY_TILE), 1)
    for start in range(0, length, KEY_TILE):
        tile = lax.dot_general(q_rows, k_ref[start:start + KEY_TILE, :], contract_last, preferred_element_type=jnp.float32)
        tile = jnp.where(lane < seq_len - start, tile, -jnp.inf)
        score_ref[:, start:start + KEY_TILE] = tile
        best = tile if best is None else jnp.maximum(best, tile)
    top = jnp.maximum(jnp.max(best, axis=-1, keepdims=True), jnp.max(new_scores, axis=-1, keepdims=True))
    new_weights = jnp.exp2((new_scores - top) * to_log2)
    numerator = jnp.dot(new_weights.astype(jnp.bfloat16), fresh_v, preferred_element_type=jnp.float32)
    total = None
    for start in range(0, length, KEY_TILE):
        weights = jnp.exp2((score_ref[:, start:start + KEY_TILE] - top) * to_log2)
        total = weights if total is None else total + weights
        numerator = numerator + jnp.dot(weights.astype(jnp.bfloat16), v_ref[start:start + KEY_TILE, :], preferred_element_type=jnp.float32)
    denominator = jnp.sum(total, axis=-1, keepdims=True) + jnp.sum(new_weights, axis=-1, keepdims=True)
    return numerator / denominator


def block_kernel(
        len_ref, g_ref, lb_ref, bq_ref, bkv_ref, bo_ref, x_hbm, wq_hbm, wkv_hbm, wo_hbm, k_hbm, v_hbm,
        y_ref, k_buf, v_buf, fk_ref, fv_ref,
        x_buf, h_buf, gain_buf, bias_buf, bo_buf, wq_buf, wkv_buf, w_buf, q_buf, q_in, q_rows, score_buf, head_buf, a_src, a_buf, lhs_buf, p_buf, mid_buf, fin_buf,
        x_sems, w_sems, kv_sems, swap_sems, q_send, q_recv, a_send, a_recv, f_send, f_recv, rs_send, rs_recv, ag_send, ag_recv):
    me = lax.axis_index('tp')
    n_dev = N_CHIPS * N_CORES
    chip, core = me // N_CORES, me % N_CORES
    n_steps, group_rows, width = x_buf.shape
    n_seqs, length, depth = k_buf.shape
    q_width = wq_buf.shape[1]
    dev_heads = q_width // depth
    chip_heads = N_CORES * dev_heads
    part_seqs = n_seqs // N_PARTS
    rows = n_dev * n_steps * dev_heads
    own_rows = wo_hbm.shape[0]
    half, quarter = width // 2, width // 4
    block = N_CORES * part_seqs

    def chip_at(k):
        return (chip + k) % N_CHIPS

    def device(k):
        return {'tp': chip_at(k) * N_CORES + core}

    def member(d):
        return (me + d) % n_dev

    right, left, partner = device(1), device(3), {'tp': chip * N_CORES + 1 - core}

    def remote(src, dst, send, recv, to):
        return pltpu.make_async_remote_copy(src_ref=src, dst_ref=dst, send_sem=send, recv_sem=recv, device_id=to, device_id_type=MESH)

    def cols(which, begin, size):
        return pl.ds(pl.multiple_of(which * half + begin, quarter), size)

    def seq_rows(d):
        return pl.ds(pl.multiple_of(member(d) * n_seqs, n_seqs), n_seqs)

    barrier = pltpu.get_barrier_semaphore()
    for d in range(1, n_dev):
        pl.semaphore_signal(barrier, inc=1, device_id={'tp': member(d)}, device_id_type=MESH)

    def x_load(s):
        return pltpu.make_async_copy(x_hbm.at[s], x_buf.at[s], x_sems.at[s])

    def kv_load(b):
        return (pltpu.make_async_copy(k_hbm.at[b], k_buf.at[b], kv_sems.at[0, b]),
                pltpu.make_async_copy(v_hbm.at[b], v_buf.at[b], kv_sems.at[1, b]))

    own_w_rows = pl.ds(pl.multiple_of(core * own_rows, own_rows), own_rows)
    wq_load = pltpu.make_async_copy(wq_hbm, wq_buf, w_sems.at[0])
    wkv_load = pltpu.make_async_copy(wkv_hbm, wkv_buf, w_sems.at[1])
    wo_load = pltpu.make_async_copy(wo_hbm.at[:, cols(core, 0, half)], w_buf.at[own_w_rows, :], w_sems.at[2])
    wo_swap = remote(wo_hbm.at[:, cols(1 - core, 0, half)], w_buf.at[own_w_rows, :], swap_sems.at[0], swap_sems.at[1], partner)
    for s in range(n_steps):
        x_load(s).start()
    wq_load.start()
    wkv_load.start()

    bq_row = bq_ref[...].astype(jnp.float32).reshape(1, q_width)
    bo_buf[...] = bo_ref[...].astype(jnp.float32).reshape(1, width)
    gain_buf[...] = jnp.broadcast_to(g_ref[...].astype(jnp.float32).reshape(1, width), gain_buf.shape)
    bias_buf[...] = jnp.broadcast_to(lb_ref[...].astype(jnp.float32).reshape(1, width), bias_buf.shape)

    def q_copy(s, d):
        return remote(q_buf.at[s, seq_rows(d)], q_in.at[me, s], q_send.at[s, d - 1], q_recv.at[s, d - 1], {'tp': member(d)})

    for s in range(n_steps):
        x_load(s).wait()

        def norm_rows(i, carry):
            where = pl.ds(pl.multiple_of(i * LN_ROWS, LN_ROWS), LN_ROWS)
            x_float = x_buf[s, where, :].astype(jnp.float32)
            centered = x_float - jnp.mean(x_float, axis=-1, keepdims=True)
            row_var = jnp.mean(centered * centered, axis=-1, keepdims=True)
            scaled = centered * lax.rsqrt(row_var + LN_EPS)
            h_buf[s, where, :] = (scaled * gain_buf[...] + bias_buf[...]).astype(h_buf.dtype)
            return carry

        lax.fori_loop(0, group_rows // LN_ROWS, norm_rows, 0)
        if s == 0:
            wq_load.wait()
            wo_load.start()
        for n in range(0, q_width, 256):
            part = jnp.dot(h_buf[s], wq_buf[:, n:n + 256], preferred_element_type=jnp.float32)
            q_buf[s, :, n:n + 256] = (part + bq_row[:, n:n + 256]).astype(q_buf.dtype)
        if s == 0:
            pl.semaphore_wait(barrier, n_dev - 1)
        for d in range(1, n_dev):
            q_copy(s, d).start()
        if s == 0:
            wo_swap.start()
        q_in[me, s] = q_buf[s, seq_rows(0), :]
    for b in range(n_seqs):
        for copy in kv_load(b):
            copy.start()

    wkv_load.wait()
    own_h = jnp.concatenate([h_buf[s, seq_rows(0), :] for s in range(n_steps)], axis=0)
    fresh = jnp.dot(own_h, wkv_buf[...], preferred_element_type=jnp.float32) + bkv_ref[...].astype(jnp.float32).reshape(1, -1)
    fresh = fresh.astype(jnp.bfloat16).astype(jnp.float32)
    fk_ref[...] = jnp.zeros_like(fk_ref)
    fv_ref[...] = jnp.zeros_like(fv_ref)
    for s in range(n_steps):
        where = pl.ds(s, n_seqs, stride=FRESH_ROWS)
        fk_ref[where, :] = fresh[s * n_seqs:(s + 1) * n_seqs, :depth]
        fv_ref[where, :] = fresh[s * n_seqs:(s + 1) * n_seqs, depth:]

    for s in range(n_steps):
        for d in range(1, n_dev):
            q_copy(s, d).wait_recv()
    for u in range(n_dev):
        for s in range(n_steps):
            for h in range(dev_heads):
                first = ((u * n_steps + s) * dev_heads + h) * n_seqs
                q_rows[first:first + n_seqs, :] = q_in[u, s, :, h * depth:(h + 1) * depth].astype(jnp.float32)

    shape = (rows, FRESH_ROWS)
    step_of_row = lax.broadcasted_iota(jnp.int32, shape, 0) // dev_heads % n_steps
    fresh_mask = lax.broadcasted_iota(jnp.int32, shape, 1) <= step_of_row

    def a_copy(p, d):
        return remote(a_src.at[p, chip_at(d)], a_buf.at[p, core, chip], a_send.at[p, d - 1], a_recv.at[p, d - 1], device(d))

    def a_forward(p, d):
        where = a_buf.at[p, core, chip_at(N_CHIPS - d)]
        return remote(a_src.at[p, chip] if d == 0 else where, where, f_send.at[p, d], f_recv.at[p, d], partner)

    low, high = pl.ds(0, quarter), pl.ds(quarter, quarter)

    def rs(p, s, i):
        def part(k, where):
            return p_buf.at[p, s, chip_at(k), :, where]
        src, dst, to = (
            (part(2, low), mid_buf.at[p, s, 0], right),
            (part(2, high), mid_buf.at[p, s, 1], left),
            (part(1, high), fin_buf.at[p, s, 0], right),
            (part(3, low), fin_buf.at[p, s, 1], left),
            (part(1, low), fin_buf.at[p, s, 2], right),
            (part(3, high), fin_buf.at[p, s, 3], left),
        )[i]
        return remote(src, dst, rs_send.at[p, s, i], rs_recv.at[p, s, i], to)

    def ag(p, s, i):
        k, begin, size, to = (
            (0, 0, half, right),
            (0, 0, half, left),
            (3, 0, quarter, right),
            (1, quarter, quarter, left),
            (0, 0, half, partner),
            (3, 0, half, partner),
            (1, 0, half, partner),
            (2, 0, quarter, partner),
            (2, quarter, quarter, partner),
        )[i]
        where = y_ref.at[s, chip_at(k), :, p, :, cols(core, begin, size)]
        return remote(where, where, ag_send.at[p, s, i], ag_recv.at[p, s, i], to)

    def pack(p):
        for t in range(N_CHIPS):
            for s in range(n_steps):
                pieces = []
                for h in range(chip_heads):
                    u = t * N_CORES + h // dev_heads
                    first = ((u * n_steps + s) * dev_heads + h % dev_heads) * n_seqs + p * part_seqs
                    pieces.append(head_buf[first:first + part_seqs, :])
                a_src[p, t, s] = jnp.concatenate(pieces, axis=1).astype(a_src.dtype)
        for d in (2, 1, 3):
            a_copy(p, d).start()
        a_forward(p, 0).start()
        a_buf[p, core, chip] = a_src[p, chip]

    def forward(p):
        for d in (1, 3, 2):
            a_copy(p, d).wait_recv()
            a_forward(p, d).start()

    def partial(p):
        for d in range(N_CHIPS):
            a_forward(p, d).wait_recv()
        if p == 0:
            wo_load.wait()
            wo_swap.wait_recv()
        for s in range(n_steps):
            for t in range(N_CHIPS):
                pair = jnp.concatenate([a_buf[p, c, t, s].astype(jnp.float32) for c in range(N_CORES)], axis=0)
                first = (s * N_CHIPS + t) * block
                lhs_buf[first:first + block, :] = pair.astype(lhs_buf.dtype)
        for n in range(0, half, 512):
            out = jnp.dot(lhs_buf[...], w_buf[:, n:n + 512], preferred_element_type=jnp.float32).astype(p_buf.dtype)
            for s in range(n_steps):
                for t in range(N_CHIPS):
                    first = (s * N_CHIPS + t) * block
                    p_buf[p, s, t, :, n:n + 512] = out[first:first + block]
        for pair in ((0, 1), (2, 3)):
            for s in range(n_steps):
                for i in pair:
                    rs(p, s, i).start()

    def add_into(target, other):
        target[...] = (target[...].astype(jnp.float32) + other[...].astype(jnp.float32)).astype(target.dtype)

    def middle(p, s):
        rs(p, s, 0).wait_recv()
        add_into(p_buf.at[p, s, chip_at(1), :, low], mid_buf.at[p, s, 0])
        rs(p, s, 4).start()
        rs(p, s, 1).wait_recv()
        add_into(p_buf.at[p, s, chip_at(3), :, high], mid_buf.at[p, s, 1])
        rs(p, s, 5).start()

    def finish(p, s):
        for i in (2, 3, 4, 5):
            rs(p, s, i).wait_recv()
        chip_rows = pl.ds(pl.multiple_of(chip * N_CORES * n_seqs, N_CORES * n_seqs), N_CORES * n_seqs)
        for begin, one, two in ((0, 1, 2), (quarter, 0, 3)):
            where = cols(core, begin, quarter)
            total = p_buf[p, s, chip, :, begin:begin + quarter].astype(jnp.float32)
            total = total + fin_buf[p, s, one].astype(jnp.float32)
            total = total + fin_buf[p, s, two].astype(jnp.float32)
            total = total + bo_buf[:, where]
            x_part = x_buf[s, chip_rows, where].astype(jnp.float32)
            for c in range(N_CORES):
                x_first = c * n_seqs + p * part_seqs
                y_ref[s, chip, c, p, :, where] = (x_part[x_first:x_first + part_seqs] + total[c * part_seqs:(c + 1) * part_seqs]).astype(y_ref.dtype)
        for i in (0, 1, 4):
            ag(p, s, i).start()

    def relay(p, s):
        ag(p, s, 0).wait_recv()
        ag(p, s, 2).start()
        ag(p, s, 5).start()
        ag(p, s, 1).wait_recv()
        ag(p, s, 3).start()
        ag(p, s, 6).start()

    def last(p, s):
        ag(p, s, 2).wait_recv()
        ag(p, s, 7).start()
        ag(p, s, 3).wait_recv()
        ag(p, s, 8).start()

    def each(stage, p):
        for s in range(n_steps):
            stage(p, s)

    def attend_pair(i, carry):
        for j in range(2):
            for copy in kv_load(2 * i + j):
                copy.wait()
        for j in range(2):
            b = 2 * i + j
            q_one = q_rows[pl.ds(b, rows, stride=n_seqs), :].astype(jnp.bfloat16)
            new = pl.ds(pl.multiple_of(b * FRESH_ROWS, FRESH_ROWS), FRESH_ROWS)
            out = attend_one(q_one, k_buf.at[b], v_buf.at[b], score_buf.at[j], len_ref[b],
                             fk_ref[new, :].astype(jnp.bfloat16), fv_ref[new, :].astype(jnp.bfloat16), fresh_mask)
            head_buf[pl.ds(b, rows, stride=n_seqs), :] = out
        @pl.when(i == 3)
        def _():
            pack(0)

        @pl.when(i == 5)
        def _():
            forward(0)
            partial(0)

        @pl.when(i == 7)
        def _():
            each(middle, 0)
        return carry

    lax.fori_loop(0, n_seqs // 2, attend_pair, 0)
    pack(1)
    each(finish, 0)
    forward(1)
    partial(1)
    each(relay, 0)
    each(middle, 1)
    each(last, 0)
    each(finish, 1)
    each(relay, 1)
    each(last, 1)
    wo_swap.wait_send()
    for s in range(n_steps):
        for d in range(1, n_dev):
            q_copy(s, d).wait_send()
    for p in range(N_PARTS):
        for s in range(n_steps):
            for i in range(4, 9):
                ag(p, s, i).wait_recv()
            for i in range(9):
                ag(p, s, i).wait_send()
            for i in range(6):
                rs(p, s, i).wait_send()
        for d in (1, 2, 3):
            a_copy(p, d).wait_send()
        for d in range(N_CHIPS):
            a_forward(p, d).wait_send()


def store_kernel(n_steps, len_ref, fk_ref, fv_ref, y_ref, k_ref, v_ref, y_out, k_out, v_out, k_buf, v_buf, sems, y_sem):
    n_seqs, length, depth = k_buf.shape

    def store(b):
        return (pltpu.make_async_copy(k_buf.at[b], k_out.at[b], sems.at[0, b]),
                pltpu.make_async_copy(v_buf.at[b], v_out.at[b], sems.at[1, b]))

    def patch(b, buf, fresh):
        start = pl.multiple_of(jnp.minimum(len_ref[b] // 8 * 8, length - WINDOW), 8)
        offset = len_ref[b] - start
        row = lax.broadcasted_iota(jnp.int32, (WINDOW, depth), 0)
        window = buf[b, pl.ds(start, WINDOW), :].astype(jnp.float32)
        for s in range(n_steps):
            window = jnp.where(row == offset + s, fresh[b * FRESH_ROWS + s:b * FRESH_ROWS + s + 1, :], window)
        buf[b, pl.ds(start, WINDOW), :] = window.astype(buf.dtype)

    y_copy = pltpu.make_async_copy(y_ref, y_out, y_sem)
    y_copy.start()
    for b in range(n_seqs):
        patch(b, k_buf, fk_ref)
        patch(b, v_buf, fv_ref)
        for copy in store(b):
            copy.start()
    y_copy.wait()
    for b in range(n_seqs):
        for copy in store(b):
            copy.wait()


def solution(mesh):
    def local_block(x_steps, seq_lens, k_cache, v_cache, ln_gain, ln_bias, w_q, b_q, w_kv, b_kv, w_out, b_out):
        n_steps, group_rows, width = x_steps.shape
        n_seqs, length, depth = k_cache.shape
        q_width = w_q.shape[1]
        n_dev = N_CHIPS * N_CORES
        part_seqs = n_seqs // N_PARTS
        rows = n_dev * n_steps * q_width // depth
        chip_width, half = N_CORES * q_width, width // 2
        block = N_CORES * part_seqs
        smem = pl.BlockSpec(memory_space=pltpu.SMEM)
        vmem = pl.BlockSpec(memory_space=pltpu.VMEM)
        hbm = pl.BlockSpec(memory_space=pl.ANY)
        dma = pltpu.SemaphoreType.DMA
        bf16, f32 = jnp.bfloat16, jnp.float32
        y_shape = (n_steps, N_CHIPS, N_CORES, N_PARTS, part_seqs, width)
        fresh_shape = (n_seqs * FRESH_ROWS, depth)
        y_vm, k_vm, v_vm, fresh_k, fresh_v = pl.pallas_call(
            block_kernel,
            out_shape=[pltpu.VMEM(y_shape, bf16), pltpu.VMEM(k_cache.shape, bf16), pltpu.VMEM(v_cache.shape, bf16), pltpu.VMEM(fresh_shape, f32), pltpu.VMEM(fresh_shape, f32)],
            in_specs=[smem] + [vmem] * 5 + [hbm] * 6,
            out_specs=[vmem] * 5,
            scratch_shapes=[
                pltpu.VMEM(x_steps.shape, bf16),
                pltpu.VMEM(x_steps.shape, bf16),
                pltpu.VMEM((LN_ROWS, width), f32),
                pltpu.VMEM((LN_ROWS, width), f32),
                pltpu.VMEM((1, width), f32),
                pltpu.VMEM(w_q.shape, bf16),
                pltpu.VMEM(w_kv.shape, bf16),
                pltpu.VMEM((chip_width, half), bf16),
                pltpu.VMEM((n_steps, group_rows, q_width), bf16),
                pltpu.VMEM((n_dev, n_steps, n_seqs, q_width), bf16),
                pltpu.VMEM((rows * n_seqs, depth), f32),
                pltpu.VMEM((2, rows, length), f32),
                pltpu.VMEM((rows * n_seqs, depth), f32),
                pltpu.VMEM((N_PARTS, N_CHIPS, n_steps, part_seqs, chip_width), bf16),
                pltpu.VMEM((N_PARTS, N_CORES, N_CHIPS, n_steps, part_seqs, chip_width), bf16),
                pltpu.VMEM((n_steps * N_CHIPS * block, chip_width), bf16),
                pltpu.VMEM((N_PARTS, n_steps, N_CHIPS, block, half), bf16),
                pltpu.VMEM((N_PARTS, n_steps, 2, block, half // 2), bf16),
                pltpu.VMEM((N_PARTS, n_steps, 4, block, half // 2), bf16),
                dma((n_steps,)), dma((3,)), dma((2, n_seqs)), dma((2,)),
                dma((n_steps, n_dev - 1)), dma((n_steps, n_dev - 1)),
                dma((N_PARTS, 3)), dma((N_PARTS, 3)),
                dma((N_PARTS, N_CHIPS)), dma((N_PARTS, N_CHIPS)),
                dma((N_PARTS, n_steps, 6)), dma((N_PARTS, n_steps, 6)),
                dma((N_PARTS, n_steps, 9)), dma((N_PARTS, n_steps, 9)),
            ],
            compiler_params=pltpu.CompilerParams(vmem_limit_bytes=BLOCK_VMEM, collective_id=1, has_side_effects=True),
            cost_estimate=pl.CostEstimate(flops=4 * n_seqs * rows * length * depth, bytes_accessed=4 * n_seqs * length * depth, transcendentals=n_seqs * rows * length),
        )(seq_lens, ln_gain, ln_bias, b_q, b_kv, b_out,
          x_steps, w_q, w_kv, w_out, k_cache, v_cache)
        y_steps, k_out, v_out, _, _ = pl.pallas_call(
            functools.partial(store_kernel, n_steps),
            out_shape=[jax.ShapeDtypeStruct(y_shape, bf16), jax.ShapeDtypeStruct(k_cache.shape, bf16), jax.ShapeDtypeStruct(v_cache.shape, bf16), pltpu.VMEM(k_cache.shape, bf16), pltpu.VMEM(v_cache.shape, bf16)],
            in_specs=[smem] + [vmem] * 5,
            out_specs=[hbm] * 3 + [vmem] * 2,
            scratch_shapes=[dma((2, n_seqs)), dma],
            input_output_aliases={4: 3, 5: 4},
            compiler_params=pltpu.CompilerParams(vmem_limit_bytes=2 * 1024 * 1024),
        )(seq_lens, fresh_k, fresh_v, y_vm, k_vm, v_vm)
        return y_steps.reshape(x_steps.shape), k_out, v_out

    row_spec = P(('dp', 'tp'), None, None)
    return jax.shard_map(
        local_block,
        mesh=mesh,
        in_specs=(P(None, 'dp', None), P(('dp', 'tp')), row_spec, row_spec, P(None), P(None), P(None, 'tp'), P('tp'), P(None, None), P(None), P('tp', None), P(None)),
        out_specs=(P(None, 'dp', None), row_spec, row_spec),
        check_vma=False,
    )
```

```python
import functools
import math

import jax
import jax.numpy as jnp
from jax import lax
from jax.experimental import pallas as pl
from jax.experimental.pallas import tpu as pltpu
from jax.sharding import PartitionSpec as P

LN_EPS = 1e-5
KEY_TILE = 256
LANES = 128
AHEAD = 3
FRESH_ROWS = 16
WINDOW = 16
N_CHIPS = 4
N_CORES = 2
N_PARTS = 2
LN_ROWS = 16
MESH = pl.DeviceIdType.MESH
BLOCK_VMEM = 32 * 1024 * 1024


def attend_one(q_rows, k_ref, v_ref, score_ref, prob_ref, seq_len, fresh_k, fresh_v, fresh_mask):
    rows, depth = q_rows.shape
    length = k_ref.shape[0]
    to_log2 = depth ** -0.5 * math.log2(math.e)
    contract_last = (((1,), (1,)), ((), ()))
    new_scores = lax.dot_general(q_rows, fresh_k, contract_last, preferred_element_type=jnp.float32)
    new_scores = jnp.where(fresh_mask, new_scores, -jnp.inf)
    best = None
    lane = lax.broadcasted_iota(jnp.int32, (rows, LANES), 1)
    for start in range(0, length, KEY_TILE):
        tile = lax.dot_general(q_rows, k_ref[start:start + KEY_TILE, :], contract_last, preferred_element_type=jnp.float32)
        for first in range(0, KEY_TILE, LANES):
            piece = jnp.where(lane < seq_len - (start + first), tile[:, first:first + LANES], -jnp.inf)
            score_ref[:, start + first:start + first + LANES] = piece
            best = piece if best is None else jnp.maximum(best, piece)
    top = jnp.maximum(jnp.max(best, axis=-1, keepdims=True), jnp.max(new_scores, axis=-1, keepdims=True))
    new_weights = jnp.exp2((new_scores - top) * to_log2)
    total = None
    for start in range(0, length, LANES):
        weights = jnp.exp2((score_ref[:, start:start + LANES] - top) * to_log2)
        total = weights if total is None else total + weights
        prob_ref[:, start:start + LANES] = weights.astype(prob_ref.dtype)
    numerator = jnp.dot(prob_ref[...], v_ref[...], preferred_element_type=jnp.float32)
    numerator = numerator + jnp.dot(new_weights.astype(jnp.bfloat16), fresh_v, preferred_element_type=jnp.float32)
    denominator = jnp.sum(total, axis=-1, keepdims=True) + jnp.sum(new_weights, axis=-1, keepdims=True)
    return numerator / denominator


def block_kernel(
        len_ref, g_ref, lb_ref, bq_ref, bkv_ref, bo_ref, x_hbm, wq_hbm, wkv_hbm, wo_hbm, k_hbm, v_hbm,
        y_ref, k_buf, v_buf, fk_ref, fv_ref,
        x_buf, h_buf, gain_buf, bias_buf, bo_buf, wq_buf, wkv_buf, w_buf, q_buf, q_in, q_rows, score_buf, prob_buf, head_buf, a_src, a_buf, lhs_buf, p_buf, mid_buf, fin_buf,
        x_sems, w_sems, kv_sems, swap_sems, q_send, q_recv, a_send, a_recv, f_send, f_recv, rs_send, rs_recv, ag_send, ag_recv):
    me = lax.axis_index('tp')
    n_dev = N_CHIPS * N_CORES
    chip, core = me // N_CORES, me % N_CORES
    n_steps, group_rows, width = x_buf.shape
    n_seqs, length, depth = k_buf.shape
    q_width = wq_buf.shape[1]
    dev_heads = q_width // depth
    chip_heads = N_CORES * dev_heads
    part_seqs = n_seqs // N_PARTS
    rows = n_dev * n_steps * dev_heads
    own_rows = wo_hbm.shape[0]
    half, quarter = width // 2, width // 4
    block = N_CORES * part_seqs

    def chip_at(k):
        return (chip + k) % N_CHIPS

    def device(k):
        return {'tp': chip_at(k) * N_CORES + core}

    def member(d):
        return (me + d) % n_dev

    right, left, partner = device(1), device(3), {'tp': chip * N_CORES + 1 - core}

    def remote(src, dst, send, recv, to):
        return pltpu.make_async_remote_copy(src_ref=src, dst_ref=dst, send_sem=send, recv_sem=recv, device_id=to, device_id_type=MESH)

    def cols(which, begin, size):
        return pl.ds(pl.multiple_of(which * half + begin, quarter), size)

    def seq_rows(d):
        return pl.ds(pl.multiple_of(member(d) * n_seqs, n_seqs), n_seqs)

    barrier = pltpu.get_barrier_semaphore()
    for d in range(1, n_dev):
        pl.semaphore_signal(barrier, inc=1, device_id={'tp': member(d)}, device_id_type=MESH)

    def x_load(s):
        return pltpu.make_async_copy(x_hbm.at[s], x_buf.at[s], x_sems.at[s])

    def kv_load(b):
        return (pltpu.make_async_copy(k_hbm.at[b], k_buf.at[b], kv_sems.at[0, b]),
                pltpu.make_async_copy(v_hbm.at[b], v_buf.at[b], kv_sems.at[1, b]))

    own_w_rows = pl.ds(pl.multiple_of(core * own_rows, own_rows), own_rows)
    wq_load = pltpu.make_async_copy(wq_hbm, wq_buf, w_sems.at[0])
    wkv_load = pltpu.make_async_copy(wkv_hbm, wkv_buf, w_sems.at[1])
    wo_load = pltpu.make_async_copy(wo_hbm.at[:, cols(core, 0, half)], w_buf.at[own_w_rows, :], w_sems.at[2])
    wo_swap = remote(wo_hbm.at[:, cols(1 - core, 0, half)], w_buf.at[own_w_rows, :], swap_sems.at[0], swap_sems.at[1], partner)
    for s in range(n_steps):
        x_load(s).start()
    wq_load.start()
    wkv_load.start()

    bq_row = bq_ref[...].astype(jnp.float32).reshape(1, q_width)
    bo_buf[...] = bo_ref[...].astype(jnp.float32).reshape(1, width)
    gain_buf[...] = jnp.broadcast_to(g_ref[...].astype(jnp.float32).reshape(1, width), gain_buf.shape)
    bias_buf[...] = jnp.broadcast_to(lb_ref[...].astype(jnp.float32).reshape(1, width), bias_buf.shape)

    def q_copy(s, d):
        return remote(q_buf.at[s, seq_rows(d)], q_in.at[me, s], q_send.at[s, d - 1], q_recv.at[s, d - 1], {'tp': member(d)})

    for s in range(n_steps):
        x_load(s).wait()

        def norm_rows(i, carry):
            where = pl.ds(pl.multiple_of(i * LN_ROWS, LN_ROWS), LN_ROWS)
            x_float = x_buf[s, where, :].astype(jnp.float32)
            centered = x_float - jnp.mean(x_float, axis=-1, keepdims=True)
            row_var = jnp.mean(centered * centered, axis=-1, keepdims=True)
            scaled = centered * lax.rsqrt(row_var + LN_EPS)
            h_buf[s, where, :] = (scaled * gain_buf[...] + bias_buf[...]).astype(h_buf.dtype)
            return carry

        lax.fori_loop(0, group_rows // LN_ROWS, norm_rows, 0)
        if s == 0:
            wq_load.wait()
            wo_load.start()
            for b in range(2 * AHEAD):
                for copy in kv_load(b):
                    copy.start()
        for n in range(0, q_width, 256):
            part = jnp.dot(h_buf[s], wq_buf[:, n:n + 256], preferred_element_type=jnp.float32)
            q_buf[s, :, n:n + 256] = (part + bq_row[:, n:n + 256]).astype(q_buf.dtype)
        if s == 0:
            pl.semaphore_wait(barrier, n_dev - 1)
        for d in range(1, n_dev):
            q_copy(s, d).start()
        if s == 0:
            wo_swap.start()
        q_in[me, s] = q_buf[s, seq_rows(0), :]

    wkv_load.wait()
    own_h = jnp.concatenate([h_buf[s, seq_rows(0), :] for s in range(n_steps)], axis=0)
    fresh = jnp.dot(own_h, wkv_buf[...], preferred_element_type=jnp.float32) + bkv_ref[...].astype(jnp.float32).reshape(1, -1)
    fresh = fresh.astype(jnp.bfloat16).astype(jnp.float32)
    fk_ref[...] = jnp.zeros_like(fk_ref)
    fv_ref[...] = jnp.zeros_like(fv_ref)
    for s in range(n_steps):
        where = pl.ds(s, n_seqs, stride=FRESH_ROWS)
        fk_ref[where, :] = fresh[s * n_seqs:(s + 1) * n_seqs, :depth]
        fv_ref[where, :] = fresh[s * n_seqs:(s + 1) * n_seqs, depth:]

    for s in range(n_steps):
        for d in range(1, n_dev):
            q_copy(s, d).wait_recv()
    for u in range(n_dev):
        for s in range(n_steps):
            for h in range(dev_heads):
                first = ((u * n_steps + s) * dev_heads + h) * n_seqs
                q_rows[first:first + n_seqs, :] = q_in[u, s, :, h * depth:(h + 1) * depth].astype(jnp.float32)

    shape = (rows, FRESH_ROWS)
    step_of_row = lax.broadcasted_iota(jnp.int32, shape, 0) // dev_heads % n_steps
    fresh_mask = lax.broadcasted_iota(jnp.int32, shape, 1) <= step_of_row

    def a_copy(p, d):
        return remote(a_src.at[p, chip_at(d)], a_buf.at[p, core, chip], a_send.at[p, d - 1], a_recv.at[p, d - 1], device(d))

    def a_forward(p, d):
        where = a_buf.at[p, core, chip_at(N_CHIPS - d)]
        return remote(a_src.at[p, chip] if d == 0 else where, where, f_send.at[p, d], f_recv.at[p, d], partner)

    low, high = pl.ds(0, quarter), pl.ds(quarter, quarter)

    def rs(p, s, i):
        def part(k, where):
            return p_buf.at[p, s, chip_at(k), :, where]
        src, dst, to = (
            (part(2, low), mid_buf.at[p, s, 0], right),
            (part(2, high), mid_buf.at[p, s, 1], left),
            (part(1, high), fin_buf.at[p, s, 0], right),
            (part(3, low), fin_buf.at[p, s, 1], left),
            (part(1, low), fin_buf.at[p, s, 2], right),
            (part(3, high), fin_buf.at[p, s, 3], left),
        )[i]
        return remote(src, dst, rs_send.at[p, s, i], rs_recv.at[p, s, i], to)

    def ag(p, s, i):
        k, begin, size, to = (
            (0, 0, half, right),
            (0, 0, half, left),
            (3, 0, quarter, right),
            (1, quarter, quarter, left),
            (0, 0, half, partner),
            (3, 0, half, partner),
            (1, 0, half, partner),
            (2, 0, quarter, partner),
            (2, quarter, quarter, partner),
        )[i]
        where = y_ref.at[s, chip_at(k), :, p, :, cols(core, begin, size)]
        return remote(where, where, ag_send.at[p, s, i], ag_recv.at[p, s, i], to)

    def pack(p):
        for t in range(N_CHIPS):
            for s in range(n_steps):
                pieces = []
                for h in range(chip_heads):
                    u = t * N_CORES + h // dev_heads
                    first = ((u * n_steps + s) * dev_heads + h % dev_heads) * n_seqs + p * part_seqs
                    pieces.append(head_buf[first:first + part_seqs, :])
                a_src[p, t, s] = jnp.concatenate(pieces, axis=1).astype(a_src.dtype)
        for d in (2, 1, 3):
            a_copy(p, d).start()
        a_forward(p, 0).start()
        a_buf[p, core, chip] = a_src[p, chip]

    def forward(p):
        for d in (1, 3, 2):
            a_copy(p, d).wait_recv()
            a_forward(p, d).start()

    def partial(p):
        for d in range(N_CHIPS):
            a_forward(p, d).wait_recv()
        if p == 0:
            wo_load.wait()
            wo_swap.wait_recv()
        for s in range(n_steps):
            for t in range(N_CHIPS):
                pair = jnp.concatenate([a_buf[p, c, t, s].astype(jnp.float32) for c in range(N_CORES)], axis=0)
                first = (s * N_CHIPS + t) * block
                lhs_buf[first:first + block, :] = pair.astype(lhs_buf.dtype)
        for n in range(0, half, 512):
            out = jnp.dot(lhs_buf[...], w_buf[:, n:n + 512], preferred_element_type=jnp.float32).astype(p_buf.dtype)
            for s in range(n_steps):
                for t in range(N_CHIPS):
                    first = (s * N_CHIPS + t) * block
                    p_buf[p, s, t, :, n:n + 512] = out[first:first + block]
        for pair in ((0, 1), (2, 3)):
            for s in range(n_steps):
                for i in pair:
                    rs(p, s, i).start()

    def add_into(target, other):
        target[...] = (target[...].astype(jnp.float32) + other[...].astype(jnp.float32)).astype(target.dtype)

    def middle(p, s):
        rs(p, s, 0).wait_recv()
        add_into(p_buf.at[p, s, chip_at(1), :, low], mid_buf.at[p, s, 0])
        rs(p, s, 4).start()
        rs(p, s, 1).wait_recv()
        add_into(p_buf.at[p, s, chip_at(3), :, high], mid_buf.at[p, s, 1])
        rs(p, s, 5).start()

    def finish(p, s):
        for i in (2, 3, 4, 5):
            rs(p, s, i).wait_recv()
        chip_rows = pl.ds(pl.multiple_of(chip * N_CORES * n_seqs, N_CORES * n_seqs), N_CORES * n_seqs)
        for begin, one, two in ((0, 1, 2), (quarter, 0, 3)):
            where = cols(core, begin, quarter)
            total = p_buf[p, s, chip, :, begin:begin + quarter].astype(jnp.float32)
            total = total + fin_buf[p, s, one].astype(jnp.float32)
            total = total + fin_buf[p, s, two].astype(jnp.float32)
            total = total + bo_buf[:, where]
            x_part = x_buf[s, chip_rows, where].astype(jnp.float32)
            for c in range(N_CORES):
                x_first = c * n_seqs + p * part_seqs
                y_ref[s, chip, c, p, :, where] = (x_part[x_first:x_first + part_seqs] + total[c * part_seqs:(c + 1) * part_seqs]).astype(y_ref.dtype)
        for i in (0, 1, 4):
            ag(p, s, i).start()

    def relay(p, s):
        ag(p, s, 0).wait_recv()
        ag(p, s, 2).start()
        ag(p, s, 5).start()
        ag(p, s, 1).wait_recv()
        ag(p, s, 3).start()
        ag(p, s, 6).start()

    def last(p, s):
        ag(p, s, 2).wait_recv()
        ag(p, s, 7).start()
        ag(p, s, 3).wait_recv()
        ag(p, s, 8).start()

    def each(stage, p):
        for s in range(n_steps):
            stage(p, s)

    def attend_pair(i, carry):
        @pl.when(i < n_seqs // 2 - AHEAD)
        def _():
            for j in range(2):
                for copy in kv_load(2 * (i + AHEAD) + j):
                    copy.start()

        for j in range(2):
            for copy in kv_load(2 * i + j):
                copy.wait()
        for j in range(2):
            b = 2 * i + j
            q_one = q_rows[pl.ds(b, rows, stride=n_seqs), :].astype(jnp.bfloat16)
            new = pl.ds(pl.multiple_of(b * FRESH_ROWS, FRESH_ROWS), FRESH_ROWS)
            out = attend_one(q_one, k_buf.at[b], v_buf.at[b], score_buf.at[j], prob_buf.at[j], len_ref[b],
                             fk_ref[new, :].astype(jnp.bfloat16), fv_ref[new, :].astype(jnp.bfloat16), fresh_mask)
            head_buf[pl.ds(b, rows, stride=n_seqs), :] = out
        @pl.when(i == 3)
        def _():
            pack(0)

        @pl.when(i == 5)
        def _():
            forward(0)
            partial(0)

        @pl.when(i == 7)
        def _():
            each(middle, 0)
        return carry

    lax.fori_loop(0, n_seqs // 2, attend_pair, 0)
    pack(1)
    each(finish, 0)
    forward(1)
    partial(1)
    each(relay, 0)
    each(middle, 1)
    each(last, 0)
    each(finish, 1)
    each(relay, 1)
    each(last, 1)
    wo_swap.wait_send()
    for s in range(n_steps):
        for d in range(1, n_dev):
            q_copy(s, d).wait_send()
    for p in range(N_PARTS):
        for s in range(n_steps):
            for i in range(4, 9):
                ag(p, s, i).wait_recv()
            for i in range(9):
                ag(p, s, i).wait_send()
            for i in range(6):
                rs(p, s, i).wait_send()
        for d in (1, 2, 3):
            a_copy(p, d).wait_send()
        for d in range(N_CHIPS):
            a_forward(p, d).wait_send()


def store_kernel(n_steps, len_ref, fk_ref, fv_ref, y_ref, k_ref, v_ref, y_out, k_out, v_out, k_buf, v_buf, sems, y_sem):
    n_seqs, length, depth = k_buf.shape

    def store(b):
        return (pltpu.make_async_copy(k_buf.at[b], k_out.at[b], sems.at[0, b]),
                pltpu.make_async_copy(v_buf.at[b], v_out.at[b], sems.at[1, b]))

    def patch(b, buf, fresh):
        start = pl.multiple_of(jnp.minimum(len_ref[b] // 8 * 8, length - WINDOW), 8)
        offset = len_ref[b] - start
        row = lax.broadcasted_iota(jnp.int32, (WINDOW, depth), 0)
        window = buf[b, pl.ds(start, WINDOW), :].astype(jnp.float32)
        for s in range(n_steps):
            window = jnp.where(row == offset + s, fresh[b * FRESH_ROWS + s:b * FRESH_ROWS + s + 1, :], window)
        buf[b, pl.ds(start, WINDOW), :] = window.astype(buf.dtype)

    y_copy = pltpu.make_async_copy(y_ref, y_out, y_sem)
    y_copy.start()
    for b in range(n_seqs):
        patch(b, k_buf, fk_ref)
        patch(b, v_buf, fv_ref)
        for copy in store(b):
            copy.start()
    y_copy.wait()
    for b in range(n_seqs):
        for copy in store(b):
            copy.wait()


def solution(mesh):
    def local_block(x_steps, seq_lens, k_cache, v_cache, ln_gain, ln_bias, w_q, b_q, w_kv, b_kv, w_out, b_out):
        n_steps, group_rows, width = x_steps.shape
        n_seqs, length, depth = k_cache.shape
        q_width = w_q.shape[1]
        n_dev = N_CHIPS * N_CORES
        part_seqs = n_seqs // N_PARTS
        rows = n_dev * n_steps * q_width // depth
        chip_width, half = N_CORES * q_width, width // 2
        block = N_CORES * part_seqs
        smem = pl.BlockSpec(memory_space=pltpu.SMEM)
        vmem = pl.BlockSpec(memory_space=pltpu.VMEM)
        hbm = pl.BlockSpec(memory_space=pl.ANY)
        dma = pltpu.SemaphoreType.DMA
        bf16, f32 = jnp.bfloat16, jnp.float32
        y_shape = (n_steps, N_CHIPS, N_CORES, N_PARTS, part_seqs, width)
        fresh_shape = (n_seqs * FRESH_ROWS, depth)
        y_vm, k_vm, v_vm, fresh_k, fresh_v = pl.pallas_call(
            block_kernel,
            out_shape=[pltpu.VMEM(y_shape, bf16), pltpu.VMEM(k_cache.shape, bf16), pltpu.VMEM(v_cache.shape, bf16), pltpu.VMEM(fresh_shape, f32), pltpu.VMEM(fresh_shape, f32)],
            in_specs=[smem] + [vmem] * 5 + [hbm] * 6,
            out_specs=[vmem] * 5,
            scratch_shapes=[
                pltpu.VMEM(x_steps.shape, bf16),
                pltpu.VMEM(x_steps.shape, bf16),
                pltpu.VMEM((LN_ROWS, width), f32),
                pltpu.VMEM((LN_ROWS, width), f32),
                pltpu.VMEM((1, width), f32),
                pltpu.VMEM(w_q.shape, bf16),
                pltpu.VMEM(w_kv.shape, bf16),
                pltpu.VMEM((chip_width, half), bf16),
                pltpu.VMEM((n_steps, group_rows, q_width), bf16),
                pltpu.VMEM((n_dev, n_steps, n_seqs, q_width), bf16),
                pltpu.VMEM((rows * n_seqs, depth), f32),
                pltpu.VMEM((2, rows, length), f32),
                pltpu.VMEM((2, rows, length), bf16),
                pltpu.VMEM((rows * n_seqs, depth), f32),
                pltpu.VMEM((N_PARTS, N_CHIPS, n_steps, part_seqs, chip_width), bf16),
                pltpu.VMEM((N_PARTS, N_CORES, N_CHIPS, n_steps, part_seqs, chip_width), bf16),
                pltpu.VMEM((n_steps * N_CHIPS * block, chip_width), bf16),
                pltpu.VMEM((N_PARTS, n_steps, N_CHIPS, block, half), bf16),
                pltpu.VMEM((N_PARTS, n_steps, 2, block, half // 2), bf16),
                pltpu.VMEM((N_PARTS, n_steps, 4, block, half // 2), bf16),
                dma((n_steps,)), dma((3,)), dma((2, n_seqs)), dma((2,)),
                dma((n_steps, n_dev - 1)), dma((n_steps, n_dev - 1)),
                dma((N_PARTS, 3)), dma((N_PARTS, 3)),
                dma((N_PARTS, N_CHIPS)), dma((N_PARTS, N_CHIPS)),
                dma((N_PARTS, n_steps, 6)), dma((N_PARTS, n_steps, 6)),
                dma((N_PARTS, n_steps, 9)), dma((N_PARTS, n_steps, 9)),
            ],
            compiler_params=pltpu.CompilerParams(vmem_limit_bytes=BLOCK_VMEM, collective_id=1, has_side_effects=True),
            cost_estimate=pl.CostEstimate(flops=4 * n_seqs * rows * length * depth, bytes_accessed=4 * n_seqs * length * depth, transcendentals=n_seqs * rows * length),
        )(seq_lens, ln_gain, ln_bias, b_q, b_kv, b_out,
          x_steps, w_q, w_kv, w_out, k_cache, v_cache)
        y_steps, k_out, v_out, _, _ = pl.pallas_call(
            functools.partial(store_kernel, n_steps),
            out_shape=[jax.ShapeDtypeStruct(y_shape, bf16), jax.ShapeDtypeStruct(k_cache.shape, bf16), jax.ShapeDtypeStruct(v_cache.shape, bf16), pltpu.VMEM(k_cache.shape, bf16), pltpu.VMEM(v_cache.shape, bf16)],
            in_specs=[smem] + [vmem] * 5,
            out_specs=[hbm] * 3 + [vmem] * 2,
            scratch_shapes=[dma((2, n_seqs)), dma],
            input_output_aliases={4: 3, 5: 4},
            compiler_params=pltpu.CompilerParams(vmem_limit_bytes=2 * 1024 * 1024),
        )(seq_lens, fresh_k, fresh_v, y_vm, k_vm, v_vm)
        return y_steps.reshape(x_steps.shape), k_out, v_out

    row_spec = P(('dp', 'tp'), None, None)
    return jax.shard_map(
        local_block,
        mesh=mesh,
        in_specs=(P(None, 'dp', None), P(('dp', 'tp')), row_spec, row_spec, P(None), P(None), P(None, 'tp'), P('tp'), P(None, None), P(None), P('tp', None), P(None)),
        out_specs=(P(None, 'dp', None), row_spec, row_spec),
        check_vma=False,
    )
```

```python
import functools
import math

import jax
import jax.numpy as jnp
from jax import lax
from jax.experimental import pallas as pl
from jax.experimental.pallas import tpu as pltpu
from jax.sharding import PartitionSpec as P

LN_EPS = 1e-5
KEY_TILE = 256
LANES = 128
AHEAD = 3
FRESH_ROWS = 16
WINDOW = 16
N_CHIPS = 4
N_CORES = 2
N_PARTS = 2
LN_ROWS = 16
MESH = pl.DeviceIdType.MESH
BLOCK_VMEM = 32 * 1024 * 1024


def attend_one(q_rows, k_ref, v_ref, score_ref, prob_ref, seq_len, fresh_k, fresh_v, fresh_mask):
    rows, depth = q_rows.shape
    length = k_ref.shape[0]
    to_log2 = depth ** -0.5 * math.log2(math.e)
    contract_last = (((1,), (1,)), ((), ()))
    new_scores = lax.dot_general(q_rows, fresh_k, contract_last, preferred_element_type=jnp.float32)
    new_scores = jnp.where(fresh_mask, new_scores, -jnp.inf)
    best = None
    lane = lax.broadcasted_iota(jnp.int32, (rows, LANES), 1)
    for start in range(0, length, KEY_TILE):
        tile = lax.dot_general(q_rows, k_ref[start:start + KEY_TILE, :], contract_last, preferred_element_type=jnp.float32)
        for first in range(0, KEY_TILE, LANES):
            piece = jnp.where(lane < seq_len - (start + first), tile[:, first:first + LANES], -jnp.inf)
            score_ref[:, start + first:start + first + LANES] = piece
            best = piece if best is None else jnp.maximum(best, piece)
    top = jnp.maximum(jnp.max(best, axis=-1, keepdims=True), jnp.max(new_scores, axis=-1, keepdims=True))
    new_weights = jnp.exp2((new_scores - top) * to_log2)
    total = None
    for start in range(0, length, LANES):
        weights = jnp.exp2((score_ref[:, start:start + LANES] - top) * to_log2)
        total = weights if total is None else total + weights
        prob_ref[:, start:start + LANES] = weights.astype(prob_ref.dtype)
    numerator = jnp.dot(prob_ref[...], v_ref[...], preferred_element_type=jnp.float32)
    numerator = numerator + jnp.dot(new_weights.astype(jnp.bfloat16), fresh_v, preferred_element_type=jnp.float32)
    denominator = jnp.sum(total, axis=-1, keepdims=True) + jnp.sum(new_weights, axis=-1, keepdims=True)
    return numerator / denominator


def query_kernel(
        g_ref, lb_ref, bq_ref, bkv_ref, x_hbm, wq_hbm, wkv_hbm,
        q_in, fk_ref, fv_ref,
        x_buf, h_buf, gain_buf, bias_buf, wq_buf, wkv_buf, q_buf,
        x_sems, w_sems, q_send, q_recv):
    me = lax.axis_index('tp')
    n_dev = N_CHIPS * N_CORES
    n_steps, group_rows, width = x_buf.shape
    n_seqs, q_width = q_in.shape[2], wq_buf.shape[1]
    depth = fk_ref.shape[1]

    def member(d):
        return (me + d) % n_dev

    def remote(src, dst, send, recv, to):
        return pltpu.make_async_remote_copy(src_ref=src, dst_ref=dst, send_sem=send, recv_sem=recv, device_id=to, device_id_type=MESH)

    def seq_rows(d):
        return pl.ds(pl.multiple_of(member(d) * n_seqs, n_seqs), n_seqs)

    barrier = pltpu.get_barrier_semaphore()
    for d in range(1, n_dev):
        pl.semaphore_signal(barrier, inc=1, device_id={'tp': member(d)}, device_id_type=MESH)

    def x_load(s):
        return pltpu.make_async_copy(x_hbm.at[s], x_buf.at[s], x_sems.at[s])

    wq_load = pltpu.make_async_copy(wq_hbm, wq_buf, w_sems.at[0])
    wkv_load = pltpu.make_async_copy(wkv_hbm, wkv_buf, w_sems.at[1])
    for s in range(n_steps):
        x_load(s).start()
    wq_load.start()
    wkv_load.start()

    bq_row = bq_ref[...].astype(jnp.float32).reshape(1, q_width)
    gain_buf[...] = jnp.broadcast_to(g_ref[...].astype(jnp.float32).reshape(1, width), gain_buf.shape)
    bias_buf[...] = jnp.broadcast_to(lb_ref[...].astype(jnp.float32).reshape(1, width), bias_buf.shape)

    def q_copy(s, d):
        return remote(q_buf.at[s, seq_rows(d)], q_in.at[me, s], q_send.at[s, d - 1], q_recv.at[s, d - 1], {'tp': member(d)})

    for s in range(n_steps):
        x_load(s).wait()

        def norm_rows(i, carry):
            where = pl.ds(pl.multiple_of(i * LN_ROWS, LN_ROWS), LN_ROWS)
            x_float = x_buf[s, where, :].astype(jnp.float32)
            centered = x_float - jnp.mean(x_float, axis=-1, keepdims=True)
            row_var = jnp.mean(centered * centered, axis=-1, keepdims=True)
            scaled = centered * lax.rsqrt(row_var + LN_EPS)
            h_buf[s, where, :] = (scaled * gain_buf[...] + bias_buf[...]).astype(h_buf.dtype)
            return carry

        lax.fori_loop(0, group_rows // LN_ROWS, norm_rows, 0)
        if s == 0:
            wq_load.wait()
        for n in range(0, q_width, 256):
            part = jnp.dot(h_buf[s], wq_buf[:, n:n + 256], preferred_element_type=jnp.float32)
            q_buf[s, :, n:n + 256] = (part + bq_row[:, n:n + 256]).astype(q_buf.dtype)
        if s == 0:
            pl.semaphore_wait(barrier, n_dev - 1)
        for d in range(1, n_dev):
            q_copy(s, d).start()
        q_in[me, s] = q_buf[s, seq_rows(0), :]

    wkv_load.wait()
    own_h = jnp.concatenate([h_buf[s, seq_rows(0), :] for s in range(n_steps)], axis=0)
    fresh = jnp.dot(own_h, wkv_buf[...], preferred_element_type=jnp.float32) + bkv_ref[...].astype(jnp.float32).reshape(1, -1)
    fresh = fresh.astype(jnp.bfloat16).astype(jnp.float32)
    fk_ref[...] = jnp.zeros_like(fk_ref)
    fv_ref[...] = jnp.zeros_like(fv_ref)
    for s in range(n_steps):
        where = pl.ds(s, n_seqs, stride=FRESH_ROWS)
        fk_ref[where, :] = fresh[s * n_seqs:(s + 1) * n_seqs, :depth]
        fv_ref[where, :] = fresh[s * n_seqs:(s + 1) * n_seqs, depth:]

    for s in range(n_steps):
        for d in range(1, n_dev):
            q_copy(s, d).wait_recv()
    for s in range(n_steps):
        for d in range(1, n_dev):
            q_copy(s, d).wait_send()


def block_kernel(
        len_ref, q_in, fk_ref, fv_ref, bo_ref, x_hbm, wo_hbm, k_hbm, v_hbm,
        y_ref, k_buf, v_buf,
        x_buf, w_buf, bo_buf, q_rows, score_buf, prob_buf, head_buf, a_src, a_buf, lhs_buf, p_buf, mid_buf, fin_buf,
        w_sems, kv_sems, swap_sems, a_send, a_recv, f_send, f_recv, rs_send, rs_recv, ag_send, ag_recv):
    me = lax.axis_index('tp')
    n_dev = N_CHIPS * N_CORES
    chip, core = me // N_CORES, me % N_CORES
    n_steps, _, half = x_buf.shape
    width, quarter = 2 * half, half // 2
    n_seqs, length, depth = k_buf.shape
    q_width = q_in.shape[3]
    dev_heads = q_width // depth
    chip_heads = N_CORES * dev_heads
    part_seqs = n_seqs // N_PARTS
    rows = n_dev * n_steps * dev_heads
    own_rows = wo_hbm.shape[0]
    block = N_CORES * part_seqs

    def chip_at(k):
        return (chip + k) % N_CHIPS

    def device(k):
        return {'tp': chip_at(k) * N_CORES + core}

    right, left, far, partner = device(1), device(3), device(2), {'tp': chip * N_CORES + 1 - core}

    def remote(src, dst, send, recv, to):
        return pltpu.make_async_remote_copy(src_ref=src, dst_ref=dst, send_sem=send, recv_sem=recv, device_id=to, device_id_type=MESH)

    def cols(which, begin, size):
        return pl.ds(pl.multiple_of(which * half + begin, quarter), size)

    barrier = pltpu.get_barrier_semaphore()
    for peer in (right, left, far, partner):
        pl.semaphore_signal(barrier, inc=1, device_id=peer, device_id_type=MESH)

    def kv_load(b):
        return (pltpu.make_async_copy(k_hbm.at[b], k_buf.at[b], kv_sems.at[0, b]),
                pltpu.make_async_copy(v_hbm.at[b], v_buf.at[b], kv_sems.at[1, b]))

    for b in range(2 * AHEAD):
        for copy in kv_load(b):
            copy.start()
    own_w_rows = pl.ds(pl.multiple_of(core * own_rows, own_rows), own_rows)
    chip_rows = pl.ds(pl.multiple_of(chip * N_CORES * n_seqs, N_CORES * n_seqs), N_CORES * n_seqs)
    wo_load = pltpu.make_async_copy(wo_hbm.at[:, cols(core, 0, half)], w_buf.at[own_w_rows, :], w_sems.at[0])
    wo_swap = remote(wo_hbm.at[:, cols(1 - core, 0, half)], w_buf.at[own_w_rows, :], swap_sems.at[0], swap_sems.at[1], partner)
    x_load = pltpu.make_async_copy(x_hbm.at[:, chip_rows, cols(core, 0, half)], x_buf, w_sems.at[1])
    wo_load.start()
    x_load.start()
    bo_buf[...] = bo_ref[...].astype(jnp.float32).reshape(1, width)
    pl.semaphore_wait(barrier, 4)
    wo_swap.start()

    for u in range(n_dev):
        for s in range(n_steps):
            for h in range(dev_heads):
                first = ((u * n_steps + s) * dev_heads + h) * n_seqs
                q_rows[first:first + n_seqs, :] = q_in[u, s, :, h * depth:(h + 1) * depth].astype(jnp.float32)

    shape = (rows, FRESH_ROWS)
    step_of_row = lax.broadcasted_iota(jnp.int32, shape, 0) // dev_heads % n_steps
    fresh_mask = lax.broadcasted_iota(jnp.int32, shape, 1) <= step_of_row

    def a_copy(p, d):
        return remote(a_src.at[p, chip_at(d)], a_buf.at[p, core, chip], a_send.at[p, d - 1], a_recv.at[p, d - 1], device(d))

    def a_forward(p, d):
        where = a_buf.at[p, core, chip_at(N_CHIPS - d)]
        return remote(a_src.at[p, chip] if d == 0 else where, where, f_send.at[p, d], f_recv.at[p, d], partner)

    low, high = pl.ds(0, quarter), pl.ds(quarter, quarter)

    def rs(p, s, i):
        def part(k, where):
            return p_buf.at[p, s, chip_at(k), :, where]
        src, dst, to = (
            (part(2, low), mid_buf.at[p, s, 0], right),
            (part(2, high), mid_buf.at[p, s, 1], left),
            (part(1, high), fin_buf.at[p, s, 0], right),
            (part(3, low), fin_buf.at[p, s, 1], left),
            (part(1, low), fin_buf.at[p, s, 2], right),
            (part(3, high), fin_buf.at[p, s, 3], left),
        )[i]
        return remote(src, dst, rs_send.at[p, s, i], rs_recv.at[p, s, i], to)

    def ag(p, s, i):
        k, begin, size, to = (
            (0, 0, half, right),
            (0, 0, half, left),
            (3, 0, quarter, right),
            (1, quarter, quarter, left),
            (0, 0, half, partner),
            (3, 0, half, partner),
            (1, 0, half, partner),
            (2, 0, quarter, partner),
            (2, quarter, quarter, partner),
        )[i]
        where = y_ref.at[s, chip_at(k), :, p, :, cols(core, begin, size)]
        return remote(where, where, ag_send.at[p, s, i], ag_recv.at[p, s, i], to)

    def pack(p):
        for t in range(N_CHIPS):
            for s in range(n_steps):
                pieces = []
                for h in range(chip_heads):
                    u = t * N_CORES + h // dev_heads
                    first = ((u * n_steps + s) * dev_heads + h % dev_heads) * n_seqs + p * part_seqs
                    pieces.append(head_buf[first:first + part_seqs, :])
                a_src[p, t, s] = jnp.concatenate(pieces, axis=1).astype(a_src.dtype)
        for d in (2, 1, 3):
            a_copy(p, d).start()
        a_forward(p, 0).start()
        a_buf[p, core, chip] = a_src[p, chip]

    def forward(p):
        for d in (1, 3, 2):
            a_copy(p, d).wait_recv()
            a_forward(p, d).start()

    def partial(p):
        for d in range(N_CHIPS):
            a_forward(p, d).wait_recv()
        if p == 0:
            wo_load.wait()
            wo_swap.wait_recv()
            x_load.wait()
        for s in range(n_steps):
            for t in range(N_CHIPS):
                pair = jnp.concatenate([a_buf[p, c, t, s].astype(jnp.float32) for c in range(N_CORES)], axis=0)
                first = (s * N_CHIPS + t) * block
                lhs_buf[first:first + block, :] = pair.astype(lhs_buf.dtype)
        for n in range(0, half, 512):
            out = jnp.dot(lhs_buf[...], w_buf[:, n:n + 512], preferred_element_type=jnp.float32).astype(p_buf.dtype)
            for s in range(n_steps):
                for t in range(N_CHIPS):
                    first = (s * N_CHIPS + t) * block
                    p_buf[p, s, t, :, n:n + 512] = out[first:first + block]
        for pair in ((0, 1), (2, 3)):
            for s in range(n_steps):
                for i in pair:
                    rs(p, s, i).start()

    def add_into(target, other):
        target[...] = (target[...].astype(jnp.float32) + other[...].astype(jnp.float32)).astype(target.dtype)

    def middle(p, s):
        rs(p, s, 0).wait_recv()
        add_into(p_buf.at[p, s, chip_at(1), :, low], mid_buf.at[p, s, 0])
        rs(p, s, 4).start()
        rs(p, s, 1).wait_recv()
        add_into(p_buf.at[p, s, chip_at(3), :, high], mid_buf.at[p, s, 1])
        rs(p, s, 5).start()

    def finish(p, s):
        for i in (2, 3, 4, 5):
            rs(p, s, i).wait_recv()
        for begin, one, two in ((0, 1, 2), (quarter, 0, 3)):
            where = cols(core, begin, quarter)
            total = p_buf[p, s, chip, :, begin:begin + quarter].astype(jnp.float32)
            total = total + fin_buf[p, s, one].astype(jnp.float32)
            total = total + fin_buf[p, s, two].astype(jnp.float32)
            total = total + bo_buf[:, where]
            x_part = x_buf[s, :, begin:begin + quarter].astype(jnp.float32)
            for c in range(N_CORES):
                x_first = c * n_seqs + p * part_seqs
                y_ref[s, chip, c, p, :, where] = (x_part[x_first:x_first + part_seqs] + total[c * part_seqs:(c + 1) * part_seqs]).astype(y_ref.dtype)
        for i in (0, 1, 4):
            ag(p, s, i).start()

    def relay(p, s):
        ag(p, s, 0).wait_recv()
        ag(p, s, 2).start()
        ag(p, s, 5).start()
        ag(p, s, 1).wait_recv()
        ag(p, s, 3).start()
        ag(p, s, 6).start()

    def last(p, s):
        ag(p, s, 2).wait_recv()
        ag(p, s, 7).start()
        ag(p, s, 3).wait_recv()
        ag(p, s, 8).start()

    def each(stage, p):
        for s in range(n_steps):
            stage(p, s)

    def attend_pair(i, carry):
        @pl.when(i < n_seqs // 2 - AHEAD)
        def _():
            for j in range(2):
                for copy in kv_load(2 * (i + AHEAD) + j):
                    copy.start()

        for j in range(2):
            for copy in kv_load(2 * i + j):
                copy.wait()
        for j in range(2):
            b = 2 * i + j
            q_one = q_rows[pl.ds(b, rows, stride=n_seqs), :].astype(jnp.bfloat16)
            new = pl.ds(pl.multiple_of(b * FRESH_ROWS, FRESH_ROWS), FRESH_ROWS)
            out = attend_one(q_one, k_buf.at[b], v_buf.at[b], score_buf.at[j], prob_buf.at[j], len_ref[b],
                             fk_ref[new, :].astype(jnp.bfloat16), fv_ref[new, :].astype(jnp.bfloat16), fresh_mask)
            head_buf[pl.ds(b, rows, stride=n_seqs), :] = out
        @pl.when(i == 3)
        def _():
            pack(0)

        @pl.when(i == 5)
        def _():
            forward(0)
            partial(0)

        @pl.when(i == 7)
        def _():
            each(middle, 0)
        return carry

    lax.fori_loop(0, n_seqs // 2, attend_pair, 0)
    pack(1)
    each(finish, 0)
    forward(1)
    partial(1)
    each(relay, 0)
    each(middle, 1)
    each(last, 0)
    each(finish, 1)
    each(relay, 1)
    each(last, 1)
    wo_swap.wait_send()
    for p in range(N_PARTS):
        for s in range(n_steps):
            for i in range(4, 9):
                ag(p, s, i).wait_recv()
            for i in range(9):
                ag(p, s, i).wait_send()
            for i in range(6):
                rs(p, s, i).wait_send()
        for d in (1, 2, 3):
            a_copy(p, d).wait_send()
        for d in range(N_CHIPS):
            a_forward(p, d).wait_send()


def store_kernel(n_steps, len_ref, fk_ref, fv_ref, y_ref, k_ref, v_ref, y_out, k_out, v_out, k_buf, v_buf, sems, y_sem):
    n_seqs, length, depth = k_buf.shape

    def store(b):
        return (pltpu.make_async_copy(k_buf.at[b], k_out.at[b], sems.at[0, b]),
                pltpu.make_async_copy(v_buf.at[b], v_out.at[b], sems.at[1, b]))

    def patch(b, buf, fresh):
        start = pl.multiple_of(jnp.minimum(len_ref[b] // 8 * 8, length - WINDOW), 8)
        offset = len_ref[b] - start
        row = lax.broadcasted_iota(jnp.int32, (WINDOW, depth), 0)
        window = buf[b, pl.ds(start, WINDOW), :].astype(jnp.float32)
        for s in range(n_steps):
            window = jnp.where(row == offset + s, fresh[b * FRESH_ROWS + s:b * FRESH_ROWS + s + 1, :], window)
        buf[b, pl.ds(start, WINDOW), :] = window.astype(buf.dtype)

    y_copy = pltpu.make_async_copy(y_ref, y_out, y_sem)
    y_copy.start()
    for b in range(n_seqs):
        patch(b, k_buf, fk_ref)
        patch(b, v_buf, fv_ref)
        for copy in store(b):
            copy.start()
    y_copy.wait()
    for b in range(n_seqs):
        for copy in store(b):
            copy.wait()


def solution(mesh):
    def local_block(x_steps, seq_lens, k_cache, v_cache, ln_gain, ln_bias, w_q, b_q, w_kv, b_kv, w_out, b_out):
        n_steps, group_rows, width = x_steps.shape
        n_seqs, length, depth = k_cache.shape
        q_width = w_q.shape[1]
        n_dev = N_CHIPS * N_CORES
        part_seqs = n_seqs // N_PARTS
        rows = n_dev * n_steps * q_width // depth
        chip_width, half = N_CORES * q_width, width // 2
        block = N_CORES * part_seqs
        smem = pl.BlockSpec(memory_space=pltpu.SMEM)
        vmem = pl.BlockSpec(memory_space=pltpu.VMEM)
        hbm = pl.BlockSpec(memory_space=pl.ANY)
        dma = pltpu.SemaphoreType.DMA
        bf16, f32 = jnp.bfloat16, jnp.float32
        y_shape = (n_steps, N_CHIPS, N_CORES, N_PARTS, part_seqs, width)
        fresh_shape = (n_seqs * FRESH_ROWS, depth)
        q_in, fresh_k, fresh_v = pl.pallas_call(
            query_kernel,
            out_shape=[pltpu.VMEM((n_dev, n_steps, n_seqs, q_width), bf16), pltpu.VMEM(fresh_shape, f32), pltpu.VMEM(fresh_shape, f32)],
            in_specs=[vmem] * 4 + [hbm] * 3,
            out_specs=[vmem] * 3,
            scratch_shapes=[
                pltpu.VMEM(x_steps.shape, bf16),
                pltpu.VMEM(x_steps.shape, bf16),
                pltpu.VMEM((LN_ROWS, width), f32),
                pltpu.VMEM((LN_ROWS, width), f32),
                pltpu.VMEM(w_q.shape, bf16),
                pltpu.VMEM(w_kv.shape, bf16),
                pltpu.VMEM((n_steps, group_rows, q_width), bf16),
                dma((n_steps,)), dma((2,)),
                dma((n_steps, n_dev - 1)), dma((n_steps, n_dev - 1)),
            ],
            compiler_params=pltpu.CompilerParams(vmem_limit_bytes=20 * 1024 * 1024, collective_id=2, has_side_effects=True),
        )(ln_gain, ln_bias, b_q, b_kv, x_steps, w_q, w_kv)
        y_vm, k_vm, v_vm = pl.pallas_call(
            block_kernel,
            out_shape=[pltpu.VMEM(y_shape, bf16), pltpu.VMEM(k_cache.shape, bf16), pltpu.VMEM(v_cache.shape, bf16)],
            in_specs=[smem] + [vmem] * 4 + [hbm] * 4,
            out_specs=[vmem] * 3,
            scratch_shapes=[
                pltpu.VMEM((n_steps, N_CORES * n_seqs, half), bf16),
                pltpu.VMEM((chip_width, half), bf16),
                pltpu.VMEM((1, width), f32),
                pltpu.VMEM((rows * n_seqs, depth), f32),
                pltpu.VMEM((2, rows, length), f32),
                pltpu.VMEM((2, rows, length), bf16),
                pltpu.VMEM((rows * n_seqs, depth), f32),
                pltpu.VMEM((N_PARTS, N_CHIPS, n_steps, part_seqs, chip_width), bf16),
                pltpu.VMEM((N_PARTS, N_CORES, N_CHIPS, n_steps, part_seqs, chip_width), bf16),
                pltpu.VMEM((n_steps * N_CHIPS * block, chip_width), bf16),
                pltpu.VMEM((N_PARTS, n_steps, N_CHIPS, block, half), bf16),
                pltpu.VMEM((N_PARTS, n_steps, 2, block, half // 2), bf16),
                pltpu.VMEM((N_PARTS, n_steps, 4, block, half // 2), bf16),
                dma((2,)), dma((2, n_seqs)), dma((2,)),
                dma((N_PARTS, 3)), dma((N_PARTS, 3)),
                dma((N_PARTS, N_CHIPS)), dma((N_PARTS, N_CHIPS)),
                dma((N_PARTS, n_steps, 6)), dma((N_PARTS, n_steps, 6)),
                dma((N_PARTS, n_steps, 9)), dma((N_PARTS, n_steps, 9)),
            ],
            compiler_params=pltpu.CompilerParams(vmem_limit_bytes=BLOCK_VMEM, collective_id=1, has_side_effects=True),
        )(seq_lens, q_in, fresh_k, fresh_v, b_out, x_steps, w_out, k_cache, v_cache)
        y_steps, k_out, v_out, _, _ = pl.pallas_call(
            functools.partial(store_kernel, n_steps),
            out_shape=[jax.ShapeDtypeStruct(y_shape, bf16), jax.ShapeDtypeStruct(k_cache.shape, bf16), jax.ShapeDtypeStruct(v_cache.shape, bf16), pltpu.VMEM(k_cache.shape, bf16), pltpu.VMEM(v_cache.shape, bf16)],
            in_specs=[smem] + [vmem] * 5,
            out_specs=[hbm] * 3 + [vmem] * 2,
            scratch_shapes=[dma((2, n_seqs)), dma],
            input_output_aliases={4: 3, 5: 4},
            compiler_params=pltpu.CompilerParams(vmem_limit_bytes=2 * 1024 * 1024),
        )(seq_lens, fresh_k, fresh_v, y_vm, k_vm, v_vm)
        return y_steps.reshape(x_steps.shape), k_out, v_out

    row_spec = P(('dp', 'tp'), None, None)
    return jax.shard_map(
        local_block,
        mesh=mesh,
        in_specs=(P(None, 'dp', None), P(('dp', 'tp')), row_spec, row_spec, P(None), P(None), P(None, 'tp'), P('tp'), P(None, None), P(None), P('tp', None), P(None)),
        out_specs=(P(None, 'dp', None), row_spec, row_spec),
        check_vma=False,
    )
```

```python
import functools
import math

import jax
import jax.numpy as jnp
from jax import lax
from jax.experimental import pallas as pl
from jax.experimental.pallas import tpu as pltpu
from jax.sharding import PartitionSpec as P

LN_EPS = 1e-5
KEY_TILE = 256
LANES = 128
ROW_BLOCK = 16
FRESH_ROWS = 16
WINDOW = 16
N_CHIPS = 4
N_CORES = 2
N_PARTS = 2
LN_ROWS = 16
MESH = pl.DeviceIdType.MESH
BLOCK_VMEM = 32 * 1024 * 1024


CONTRACT_LAST = (((1,), (1,)), ((), ()))


def score_one(q_rows, k_ref, score_ref, seq_len):
    lane = lax.broadcasted_iota(jnp.int32, (q_rows.shape[0], LANES), 1)
    for start in range(0, k_ref.shape[0], KEY_TILE):
        tile = lax.dot_general(q_rows, k_ref[start:start + KEY_TILE, :], CONTRACT_LAST, preferred_element_type=jnp.float32)
        for first in range(0, KEY_TILE, LANES):
            score_ref[:, start + first:start + first + LANES] = jnp.where(lane < seq_len - (start + first), tile[:, first:first + LANES], -jnp.inf)


def attend_one(q_rows, v_ref, score_ref, prob_ref, fresh_k, fresh_v, fresh_mask):
    rows, depth = q_rows.shape
    length = v_ref.shape[0]
    to_log2 = depth ** -0.5 * math.log2(math.e)
    new_scores = lax.dot_general(q_rows, fresh_k, CONTRACT_LAST, preferred_element_type=jnp.float32)
    new_scores = jnp.where(fresh_mask, new_scores, -jnp.inf)
    new_weights, totals = [], []
    for row in range(0, rows, ROW_BLOCK):
        part = slice(row, row + ROW_BLOCK)
        best = score_ref[part, 0:LANES]
        for start in range(LANES, length, LANES):
            best = jnp.maximum(best, score_ref[part, start:start + LANES])
        top = jnp.maximum(jnp.max(best, axis=-1, keepdims=True), jnp.max(new_scores[part], axis=-1, keepdims=True))
        new = jnp.exp2((new_scores[part] - top) * to_log2)
        total = None
        for start in range(0, length, LANES):
            weights = jnp.exp2((score_ref[part, start:start + LANES] - top) * to_log2)
            total = weights if total is None else total + weights
            prob_ref[part, start:start + LANES] = weights.astype(prob_ref.dtype)
        new_weights.append(new)
        totals.append(jnp.sum(total, axis=-1, keepdims=True) + jnp.sum(new, axis=-1, keepdims=True))
    numerator = jnp.dot(prob_ref[...], v_ref[...], preferred_element_type=jnp.float32)
    numerator = numerator + jnp.dot(jnp.concatenate(new_weights, axis=0).astype(jnp.bfloat16), fresh_v, preferred_element_type=jnp.float32)
    return numerator / jnp.concatenate(totals, axis=0)


def block_kernel(
        len_ref, g_ref, lb_ref, bq_ref, bkv_ref, bo_ref, x_hbm, wq_hbm, wkv_hbm, wo_hbm, k_hbm, v_hbm,
        y_ref, k_buf, v_buf, fk_ref, fv_ref,
        x_buf, h_buf, gain_buf, bias_buf, bo_buf, wq_buf, wkv_buf, w_buf, q_buf, q_in, q_rows, score_buf, prob_buf, head_buf, a_src, a_buf, lhs_buf, p_buf, mid_buf, fin_buf,
        x_sems, w_sems, kv_sems, swap_sems, q_send, q_recv, a_send, a_recv, f_send, f_recv, rs_send, rs_recv, ag_send, ag_recv):
    me = lax.axis_index('tp')
    n_dev = N_CHIPS * N_CORES
    chip, core = me // N_CORES, me % N_CORES
    n_steps, group_rows, width = x_buf.shape
    n_seqs, length, depth = k_buf.shape
    q_width = wq_buf.shape[1]
    dev_heads = q_width // depth
    chip_heads = N_CORES * dev_heads
    part_seqs = n_seqs // N_PARTS
    rows = n_dev * n_steps * dev_heads
    own_rows = wo_hbm.shape[0]
    half, quarter = width // 2, width // 4
    block = N_CORES * part_seqs

    def chip_at(k):
        return (chip + k) % N_CHIPS

    def device(k):
        return {'tp': chip_at(k) * N_CORES + core}

    def member(d):
        return (me + d) % n_dev

    right, left, partner = device(1), device(3), {'tp': chip * N_CORES + 1 - core}

    def remote(src, dst, send, recv, to):
        return pltpu.make_async_remote_copy(src_ref=src, dst_ref=dst, send_sem=send, recv_sem=recv, device_id=to, device_id_type=MESH)

    def cols(which, begin, size):
        return pl.ds(pl.multiple_of(which * half + begin, quarter), size)

    def seq_rows(d):
        return pl.ds(pl.multiple_of(member(d) * n_seqs, n_seqs), n_seqs)

    barrier = pltpu.get_barrier_semaphore()
    for d in range(1, n_dev):
        pl.semaphore_signal(barrier, inc=1, device_id={'tp': member(d)}, device_id_type=MESH)

    def x_load(s):
        return pltpu.make_async_copy(x_hbm.at[s], x_buf.at[s], x_sems.at[s])

    def kv_load(b):
        return (pltpu.make_async_copy(k_hbm.at[b], k_buf.at[b], kv_sems.at[0, b]),
                pltpu.make_async_copy(v_hbm.at[b], v_buf.at[b], kv_sems.at[1, b]))

    own_w_rows = pl.ds(pl.multiple_of(core * own_rows, own_rows), own_rows)
    wq_load = pltpu.make_async_copy(wq_hbm, wq_buf, w_sems.at[0])
    wkv_load = pltpu.make_async_copy(wkv_hbm, wkv_buf, w_sems.at[1])
    wo_load = pltpu.make_async_copy(wo_hbm.at[:, cols(core, 0, half)], w_buf.at[own_w_rows, :], w_sems.at[2])
    wo_swap = remote(wo_hbm.at[:, cols(1 - core, 0, half)], w_buf.at[own_w_rows, :], swap_sems.at[0], swap_sems.at[1], partner)
    x_load(0).start()
    wq_load.start()

    bq_row = bq_ref[...].astype(jnp.float32).reshape(1, q_width)
    bo_buf[...] = bo_ref[...].astype(jnp.float32).reshape(1, width)
    gain_buf[...] = jnp.broadcast_to(g_ref[...].astype(jnp.float32).reshape(1, width), gain_buf.shape)
    bias_buf[...] = jnp.broadcast_to(lb_ref[...].astype(jnp.float32).reshape(1, width), bias_buf.shape)

    def q_copy(s, d):
        return remote(q_buf.at[s, seq_rows(d)], q_in.at[me, s], q_send.at[s, d - 1], q_recv.at[s, d - 1], {'tp': member(d)})

    for s in range(n_steps):
        x_load(s).wait()
        if s == 0:
            for later in range(1, n_steps):
                x_load(later).start()
            wkv_load.start()

        def norm_rows(i, carry):
            where = pl.ds(pl.multiple_of(i * LN_ROWS, LN_ROWS), LN_ROWS)
            x_float = x_buf[s, where, :].astype(jnp.float32)
            centered = x_float - jnp.mean(x_float, axis=-1, keepdims=True)
            row_var = jnp.mean(centered * centered, axis=-1, keepdims=True)
            scaled = centered * lax.rsqrt(row_var + LN_EPS)
            h_buf[s, where, :] = (scaled * gain_buf[...] + bias_buf[...]).astype(h_buf.dtype)
            return carry

        lax.fori_loop(0, group_rows // LN_ROWS, norm_rows, 0)
        if s == 0:
            wq_load.wait()
            wo_load.start()
        for n in range(0, q_width, 256):
            part = jnp.dot(h_buf[s], wq_buf[:, n:n + 256], preferred_element_type=jnp.float32)
            q_buf[s, :, n:n + 256] = (part + bq_row[:, n:n + 256]).astype(q_buf.dtype)
        if s == 0:
            pl.semaphore_wait(barrier, n_dev - 1)
        for d in range(1, n_dev):
            q_copy(s, d).start()
        if s == 0:
            wo_swap.start()
        for b in range(s * n_seqs // 4, n_seqs if s == n_steps - 1 else (s + 1) * n_seqs // 4):
            for copy in kv_load(b):
                copy.start()
        q_in[me, s] = q_buf[s, seq_rows(0), :]

    wkv_load.wait()
    own_h = jnp.concatenate([h_buf[s, seq_rows(0), :] for s in range(n_steps)], axis=0)
    fresh = jnp.dot(own_h, wkv_buf[...], preferred_element_type=jnp.float32) + bkv_ref[...].astype(jnp.float32).reshape(1, -1)
    fresh = fresh.astype(jnp.bfloat16).astype(jnp.float32)
    fk_ref[...] = jnp.zeros_like(fk_ref)
    fv_ref[...] = jnp.zeros_like(fv_ref)
    for s in range(n_steps):
        where = pl.ds(s, n_seqs, stride=FRESH_ROWS)
        fk_ref[where, :] = fresh[s * n_seqs:(s + 1) * n_seqs, :depth]
        fv_ref[where, :] = fresh[s * n_seqs:(s + 1) * n_seqs, depth:]

    for s in range(n_steps):
        for d in range(1, n_dev):
            q_copy(s, d).wait_recv()
    for u in range(n_dev):
        for s in range(n_steps):
            for h in range(dev_heads):
                first = ((u * n_steps + s) * dev_heads + h) * n_seqs
                q_rows[first:first + n_seqs, :] = q_in[u, s, :, h * depth:(h + 1) * depth].astype(jnp.float32)

    shape = (rows, FRESH_ROWS)
    step_of_row = lax.broadcasted_iota(jnp.int32, shape, 0) // dev_heads % n_steps
    fresh_mask = lax.broadcasted_iota(jnp.int32, shape, 1) <= step_of_row

    def a_copy(p, d):
        return remote(a_src.at[p, chip_at(d)], a_buf.at[p, core, chip], a_send.at[p, d - 1], a_recv.at[p, d - 1], device(d))

    def a_forward(p, d):
        where = a_buf.at[p, core, chip_at(N_CHIPS - d)]
        return remote(a_src.at[p, chip] if d == 0 else where, where, f_send.at[p, d], f_recv.at[p, d], partner)

    low, high = pl.ds(0, quarter), pl.ds(quarter, quarter)

    def rs(p, s, i):
        def part(k, where):
            return p_buf.at[p, s, chip_at(k), :, where]
        src, dst, to = (
            (part(2, low), mid_buf.at[p, s, 0], right),
            (part(2, high), mid_buf.at[p, s, 1], left),
            (part(1, high), fin_buf.at[p, s, 0], right),
            (part(3, low), fin_buf.at[p, s, 1], left),
            (part(1, low), fin_buf.at[p, s, 2], right),
            (part(3, high), fin_buf.at[p, s, 3], left),
        )[i]
        return remote(src, dst, rs_send.at[p, s, i], rs_recv.at[p, s, i], to)

    def ag(p, s, i):
        k, begin, size, to = (
            (0, 0, half, right),
            (0, 0, half, left),
            (3, 0, quarter, right),
            (1, quarter, quarter, left),
            (0, 0, half, partner),
            (3, 0, half, partner),
            (1, 0, half, partner),
            (2, 0, quarter, partner),
            (2, quarter, quarter, partner),
        )[i]
        where = y_ref.at[s, chip_at(k), :, p, :, cols(core, begin, size)]
        return remote(where, where, ag_send.at[p, s, i], ag_recv.at[p, s, i], to)

    def pack(p):
        for t in range(N_CHIPS):
            for s in range(n_steps):
                pieces = []
                for h in range(chip_heads):
                    u = t * N_CORES + h // dev_heads
                    first = ((u * n_steps + s) * dev_heads + h % dev_heads) * n_seqs + p * part_seqs
                    pieces.append(head_buf[first:first + part_seqs, :])
                a_src[p, t, s] = jnp.concatenate(pieces, axis=1).astype(a_src.dtype)
        for d in (2, 1, 3):
            a_copy(p, d).start()
        a_forward(p, 0).start()
        a_buf[p, core, chip] = a_src[p, chip]

    def forward(p):
        for d in (1, 3, 2):
            a_copy(p, d).wait_recv()
            a_forward(p, d).start()

    def partial(p):
        for d in range(N_CHIPS):
            a_forward(p, d).wait_recv()
        if p == 0:
            wo_load.wait()
            wo_swap.wait_recv()
        for s in range(n_steps):
            for t in range(N_CHIPS):
                pair = jnp.concatenate([a_buf[p, c, t, s].astype(jnp.float32) for c in range(N_CORES)], axis=0)
                first = (s * N_CHIPS + t) * block
                lhs_buf[first:first + block, :] = pair.astype(lhs_buf.dtype)
        for n in range(0, half, 512):
            out = jnp.dot(lhs_buf[...], w_buf[:, n:n + 512], preferred_element_type=jnp.float32).astype(p_buf.dtype)
            for s in range(n_steps):
                for t in range(N_CHIPS):
                    first = (s * N_CHIPS + t) * block
                    p_buf[p, s, t, :, n:n + 512] = out[first:first + block]
        for pair in ((0, 1), (2, 3)):
            for s in range(n_steps):
                for i in pair:
                    rs(p, s, i).start()

    def add_into(target, other):
        target[...] = (target[...].astype(jnp.float32) + other[...].astype(jnp.float32)).astype(target.dtype)

    def middle(p, s):
        rs(p, s, 0).wait_recv()
        add_into(p_buf.at[p, s, chip_at(1), :, low], mid_buf.at[p, s, 0])
        rs(p, s, 4).start()
        rs(p, s, 1).wait_recv()
        add_into(p_buf.at[p, s, chip_at(3), :, high], mid_buf.at[p, s, 1])
        rs(p, s, 5).start()

    def finish(p, s):
        for i in (2, 3, 4, 5):
            rs(p, s, i).wait_recv()
        chip_rows = pl.ds(pl.multiple_of(chip * N_CORES * n_seqs, N_CORES * n_seqs), N_CORES * n_seqs)
        for begin, one, two in ((0, 1, 2), (quarter, 0, 3)):
            where = cols(core, begin, quarter)
            total = p_buf[p, s, chip, :, begin:begin + quarter].astype(jnp.float32)
            total = total + fin_buf[p, s, one].astype(jnp.float32)
            total = total + fin_buf[p, s, two].astype(jnp.float32)
            total = total + bo_buf[:, where]
            x_part = x_buf[s, chip_rows, where].astype(jnp.float32)
            for c in range(N_CORES):
                x_first = c * n_seqs + p * part_seqs
                y_ref[s, chip, c, p, :, where] = (x_part[x_first:x_first + part_seqs] + total[c * part_seqs:(c + 1) * part_seqs]).astype(y_ref.dtype)
        for i in (0, 1, 4):
            ag(p, s, i).start()

    def relay(p, s):
        ag(p, s, 0).wait_recv()
        ag(p, s, 2).start()
        ag(p, s, 5).start()
        ag(p, s, 1).wait_recv()
        ag(p, s, 3).start()
        ag(p, s, 6).start()

    def last(p, s):
        ag(p, s, 2).wait_recv()
        ag(p, s, 7).start()
        ag(p, s, 3).wait_recv()
        ag(p, s, 8).start()

    def each(stage, p):
        for s in range(n_steps):
            stage(p, s)

    def query(b):
        return q_rows[pl.ds(b, rows, stride=n_seqs), :].astype(jnp.bfloat16)

    def score(b, slot):
        score_one(query(b), k_buf.at[b], score_buf.at[slot], len_ref[b])

    def attend(b, slot):
        new = pl.ds(pl.multiple_of(b * FRESH_ROWS, FRESH_ROWS), FRESH_ROWS)
        out = attend_one(query(b), v_buf.at[b], score_buf.at[slot], prob_buf.at[slot],
                         fk_ref[new, :].astype(jnp.bfloat16), fv_ref[new, :].astype(jnp.bfloat16), fresh_mask)
        head_buf[pl.ds(b, rows, stride=n_seqs), :] = out

    def wait_caches(b):
        for copy in kv_load(b):
            copy.wait()

    def attend_pair(i, carry):
        first = 2 * i
        after = jnp.minimum(first + 2, n_seqs - 1)
        wait_caches(first + 1)

        @pl.when(first + 2 < n_seqs)
        def _():
            wait_caches(after)

        score(first + 1, 1)
        attend(first, 0)
        score(after, 0)
        attend(first + 1, 1)

        @pl.when(i == n_seqs // 4 - 1)
        def _():
            pack(0)
        return carry

    wait_caches(0)
    score(0, 0)
    lax.fori_loop(0, n_seqs // 2, attend_pair, 0)
    pack(1)
    forward(0)
    partial(0)
    forward(1)
    partial(1)
    each(middle, 0)
    each(middle, 1)
    each(finish, 0)
    each(finish, 1)
    each(relay, 0)
    each(relay, 1)
    each(last, 0)
    each(last, 1)
    wo_swap.wait_send()
    for s in range(n_steps):
        for d in range(1, n_dev):
            q_copy(s, d).wait_send()
    for p in range(N_PARTS):
        for s in range(n_steps):
            for i in range(4, 9):
                ag(p, s, i).wait_recv()
            for i in range(9):
                ag(p, s, i).wait_send()
            for i in range(6):
                rs(p, s, i).wait_send()
        for d in (1, 2, 3):
            a_copy(p, d).wait_send()
        for d in range(N_CHIPS):
            a_forward(p, d).wait_send()


def store_kernel(n_steps, len_ref, fk_ref, fv_ref, y_ref, k_ref, v_ref, y_out, k_out, v_out, k_buf, v_buf, sems, y_sem):
    n_seqs, length, depth = k_buf.shape

    def store(b):
        return (pltpu.make_async_copy(k_buf.at[b], k_out.at[b], sems.at[0, b]),
                pltpu.make_async_copy(v_buf.at[b], v_out.at[b], sems.at[1, b]))

    def patch(b, buf, fresh):
        start = pl.multiple_of(jnp.minimum(len_ref[b] // 8 * 8, length - WINDOW), 8)
        offset = len_ref[b] - start
        row = lax.broadcasted_iota(jnp.int32, (WINDOW, depth), 0)
        window = buf[b, pl.ds(start, WINDOW), :].astype(jnp.float32)
        for s in range(n_steps):
            window = jnp.where(row == offset + s, fresh[b * FRESH_ROWS + s:b * FRESH_ROWS + s + 1, :], window)
        buf[b, pl.ds(start, WINDOW), :] = window.astype(buf.dtype)

    y_copy = pltpu.make_async_copy(y_ref, y_out, y_sem)
    y_copy.start()
    for b in range(n_seqs):
        patch(b, k_buf, fk_ref)
        patch(b, v_buf, fv_ref)
        for copy in store(b):
            copy.start()
    y_copy.wait()
    for b in range(n_seqs):
        for copy in store(b):
            copy.wait()


def solution(mesh):
    def local_block(x_steps, seq_lens, k_cache, v_cache, ln_gain, ln_bias, w_q, b_q, w_kv, b_kv, w_out, b_out):
        n_steps, group_rows, width = x_steps.shape
        n_seqs, length, depth = k_cache.shape
        q_width = w_q.shape[1]
        n_dev = N_CHIPS * N_CORES
        part_seqs = n_seqs // N_PARTS
        rows = n_dev * n_steps * q_width // depth
        chip_width, half = N_CORES * q_width, width // 2
        block = N_CORES * part_seqs
        smem = pl.BlockSpec(memory_space=pltpu.SMEM)
        vmem = pl.BlockSpec(memory_space=pltpu.VMEM)
        hbm = pl.BlockSpec(memory_space=pl.ANY)
        dma = pltpu.SemaphoreType.DMA
        bf16, f32 = jnp.bfloat16, jnp.float32
        y_shape = (n_steps, N_CHIPS, N_CORES, N_PARTS, part_seqs, width)
        fresh_shape = (n_seqs * FRESH_ROWS, depth)
        y_vm, k_vm, v_vm, fresh_k, fresh_v = pl.pallas_call(
            block_kernel,
            out_shape=[pltpu.VMEM(y_shape, bf16), pltpu.VMEM(k_cache.shape, bf16), pltpu.VMEM(v_cache.shape, bf16), pltpu.VMEM(fresh_shape, f32), pltpu.VMEM(fresh_shape, f32)],
            in_specs=[smem] + [vmem] * 5 + [hbm] * 6,
            out_specs=[vmem] * 5,
            scratch_shapes=[
                pltpu.VMEM(x_steps.shape, bf16),
                pltpu.VMEM(x_steps.shape, bf16),
                pltpu.VMEM((LN_ROWS, width), f32),
                pltpu.VMEM((LN_ROWS, width), f32),
                pltpu.VMEM((1, width), f32),
                pltpu.VMEM(w_q.shape, bf16),
                pltpu.VMEM(w_kv.shape, bf16),
                pltpu.VMEM((chip_width, half), bf16),
                pltpu.VMEM((n_steps, group_rows, q_width), bf16),
                pltpu.VMEM((n_dev, n_steps, n_seqs, q_width), bf16),
                pltpu.VMEM((rows * n_seqs, depth), f32),
                pltpu.VMEM((2, rows, length), f32),
                pltpu.VMEM((2, rows, length), bf16),
                pltpu.VMEM((rows * n_seqs, depth), f32),
                pltpu.VMEM((N_PARTS, N_CHIPS, n_steps, part_seqs, chip_width), bf16),
                pltpu.VMEM((N_PARTS, N_CORES, N_CHIPS, n_steps, part_seqs, chip_width), bf16),
                pltpu.VMEM((n_steps * N_CHIPS * block, chip_width), bf16),
                pltpu.VMEM((N_PARTS, n_steps, N_CHIPS, block, half), bf16),
                pltpu.VMEM((N_PARTS, n_steps, 2, block, half // 2), bf16),
                pltpu.VMEM((N_PARTS, n_steps, 4, block, half // 2), bf16),
                dma((n_steps,)), dma((3,)), dma((2, n_seqs)), dma((2,)),
                dma((n_steps, n_dev - 1)), dma((n_steps, n_dev - 1)),
                dma((N_PARTS, 3)), dma((N_PARTS, 3)),
                dma((N_PARTS, N_CHIPS)), dma((N_PARTS, N_CHIPS)),
                dma((N_PARTS, n_steps, 6)), dma((N_PARTS, n_steps, 6)),
                dma((N_PARTS, n_steps, 9)), dma((N_PARTS, n_steps, 9)),
            ],
            compiler_params=pltpu.CompilerParams(vmem_limit_bytes=BLOCK_VMEM, collective_id=1, has_side_effects=True),
            cost_estimate=pl.CostEstimate(flops=4 * n_seqs * rows * length * depth, bytes_accessed=4 * n_seqs * length * depth, transcendentals=n_seqs * rows * length),
        )(seq_lens, ln_gain, ln_bias, b_q, b_kv, b_out,
          x_steps, w_q, w_kv, w_out, k_cache, v_cache)
        y_steps, k_out, v_out, _, _ = pl.pallas_call(
            functools.partial(store_kernel, n_steps),
            out_shape=[jax.ShapeDtypeStruct(y_shape, bf16), jax.ShapeDtypeStruct(k_cache.shape, bf16), jax.ShapeDtypeStruct(v_cache.shape, bf16), pltpu.VMEM(k_cache.shape, bf16), pltpu.VMEM(v_cache.shape, bf16)],
            in_specs=[smem] + [vmem] * 5,
            out_specs=[hbm] * 3 + [vmem] * 2,
            scratch_shapes=[dma((2, n_seqs)), dma],
            input_output_aliases={4: 3, 5: 4},
            compiler_params=pltpu.CompilerParams(vmem_limit_bytes=2 * 1024 * 1024),
        )(seq_lens, fresh_k, fresh_v, y_vm, k_vm, v_vm)
        return y_steps.reshape(x_steps.shape), k_out, v_out

    row_spec = P(('dp', 'tp'), None, None)
    return jax.shard_map(
        local_block,
        mesh=mesh,
        in_specs=(P(None, 'dp', None), P(('dp', 'tp')), row_spec, row_spec, P(None), P(None), P(None, 'tp'), P('tp'), P(None, None), P(None), P('tp', None), P(None)),
        out_specs=(P(None, 'dp', None), row_spec, row_spec),
        check_vma=False,
    )
```

```python
import functools
import math

import jax
import jax.numpy as jnp
from jax import lax
from jax.experimental import pallas as pl
from jax.experimental.pallas import tpu as pltpu
from jax.sharding import PartitionSpec as P

LN_EPS = 1e-5
KEY_TILE = 256
LANES = 128
AHEAD = 4
FRESH_ROWS = 16
WINDOW = 16
N_CHIPS = 4
N_CORES = 2
LN_ROWS = 16
MESH = pl.DeviceIdType.MESH
FRONT_VMEM = 62 * 1024 * 1024
ATTENTION_VMEM = 62 * 1024 * 1024
BACK_VMEM = 59 * 1024 * 1024
KEY_RANGE = 1024


def attend_one(length, q_rows, k_ref, v_ref, score_ref, prob_ref, seq_len, fresh_k, fresh_v, fresh_mask):
    rows, depth = q_rows.shape
    to_log2 = depth ** -0.5 * math.log2(math.e)
    contract_last = (((1,), (1,)), ((), ()))
    new_scores = lax.dot_general(q_rows, fresh_k, contract_last, preferred_element_type=jnp.float32)
    new_scores = jnp.where(fresh_mask, new_scores, -jnp.inf)
    best = None
    lane = lax.broadcasted_iota(jnp.int32, (rows, LANES), 1)
    for start in range(0, length, KEY_TILE):
        tile = lax.dot_general(q_rows, k_ref[start:start + KEY_TILE, :], contract_last, preferred_element_type=jnp.float32)
        for first in range(0, KEY_TILE, LANES):
            piece = jnp.where(lane < seq_len - (start + first), tile[:, first:first + LANES], -jnp.inf)
            score_ref[:, start + first:start + first + LANES] = piece
            best = piece if best is None else jnp.maximum(best, piece)
    top = jnp.maximum(jnp.max(best, axis=-1, keepdims=True), jnp.max(new_scores, axis=-1, keepdims=True))
    new_weights = jnp.exp2((new_scores - top) * to_log2)
    total = None
    for start in range(0, length, LANES):
        weights = jnp.exp2((score_ref[:, start:start + LANES] - top) * to_log2)
        total = weights if total is None else total + weights
        prob_ref[:, start:start + LANES] = weights.astype(prob_ref.dtype)
    numerator = jnp.dot(prob_ref[:, :length], v_ref[:length, :], preferred_element_type=jnp.float32)
    numerator = numerator + jnp.dot(new_weights.astype(jnp.bfloat16), fresh_v, preferred_element_type=jnp.float32)
    denominator = jnp.sum(total, axis=-1, keepdims=True) + jnp.sum(new_weights, axis=-1, keepdims=True)
    return numerator / denominator


def query_kernel(
        g_ref, lb_ref, bq_ref, bkv_ref, x_hbm, wq_hbm, wkv_hbm,
        q_in, fk_ref, fv_ref,
        x_buf, h_buf, gain_buf, bias_buf, wq_buf, wkv_buf, q_buf,
        x_sems, w_sems, q_send, q_recv):
    me = lax.axis_index('tp')
    n_dev = N_CHIPS * N_CORES
    n_steps, group_rows, width = x_buf.shape
    n_seqs, q_width = q_in.shape[2], wq_buf.shape[1]
    depth = fk_ref.shape[1]

    def member(d):
        return (me + d) % n_dev

    def remote(src, dst, send, recv, to):
        return pltpu.make_async_remote_copy(src_ref=src, dst_ref=dst, send_sem=send, recv_sem=recv, device_id=to, device_id_type=MESH)

    def seq_rows(d):
        return pl.ds(pl.multiple_of(member(d) * n_seqs, n_seqs), n_seqs)

    barrier = pltpu.get_barrier_semaphore()
    for d in range(1, n_dev):
        pl.semaphore_signal(barrier, inc=1, device_id={'tp': member(d)}, device_id_type=MESH)

    def x_load(s):
        return pltpu.make_async_copy(x_hbm.at[s], x_buf.at[s], x_sems.at[s])

    wq_load = pltpu.make_async_copy(wq_hbm, wq_buf, w_sems.at[0])
    wkv_load = pltpu.make_async_copy(wkv_hbm, wkv_buf, w_sems.at[1])
    x_load(0).start()
    wq_load.start()

    bq_row = bq_ref[...].astype(jnp.float32).reshape(1, q_width)
    gain_buf[...] = jnp.broadcast_to(g_ref[...].astype(jnp.float32).reshape(1, width), gain_buf.shape)
    bias_buf[...] = jnp.broadcast_to(lb_ref[...].astype(jnp.float32).reshape(1, width), bias_buf.shape)

    def q_copy(s, d):
        return remote(q_buf.at[s, seq_rows(d)], q_in.at[me, s], q_send.at[s, d - 1], q_recv.at[s, d - 1], {'tp': member(d)})

    for s in range(n_steps):
        x_load(s).wait()
        if s == 0:
            for later in range(1, n_steps):
                x_load(later).start()
            wkv_load.start()

        def norm_rows(i, carry):
            where = pl.ds(pl.multiple_of(i * LN_ROWS, LN_ROWS), LN_ROWS)
            x_float = x_buf[s, where, :].astype(jnp.float32)
            centered = x_float - jnp.mean(x_float, axis=-1, keepdims=True)
            row_var = jnp.mean(centered * centered, axis=-1, keepdims=True)
            scaled = centered * lax.rsqrt(row_var + LN_EPS)
            h_buf[s, where, :] = (scaled * gain_buf[...] + bias_buf[...]).astype(h_buf.dtype)
            return carry

        lax.fori_loop(0, group_rows // LN_ROWS, norm_rows, 0)
        if s == 0:
            wq_load.wait()
        for n in range(0, q_width, 256):
            part = jnp.dot(h_buf[s], wq_buf[:, n:n + 256], preferred_element_type=jnp.float32)
            q_buf[s, :, n:n + 256] = (part + bq_row[:, n:n + 256]).astype(q_buf.dtype)
        if s == 0:
            pl.semaphore_wait(barrier, n_dev - 1)
        for d in range(1, n_dev):
            q_copy(s, d).start()
        q_in[me, s] = q_buf[s, seq_rows(0), :]

    wkv_load.wait()
    own_h = jnp.concatenate([h_buf[s, seq_rows(0), :] for s in range(n_steps)], axis=0)
    fresh = jnp.dot(own_h, wkv_buf[...], preferred_element_type=jnp.float32) + bkv_ref[...].astype(jnp.float32).reshape(1, -1)
    fresh = fresh.astype(jnp.bfloat16).astype(jnp.float32)
    fk_ref[...] = jnp.zeros_like(fk_ref)
    fv_ref[...] = jnp.zeros_like(fv_ref)
    for s in range(n_steps):
        where = pl.ds(s, n_seqs, stride=FRESH_ROWS)
        fk_ref[where, :] = fresh[s * n_seqs:(s + 1) * n_seqs, :depth]
        fv_ref[where, :] = fresh[s * n_seqs:(s + 1) * n_seqs, depth:]

    for s in range(n_steps):
        for d in range(1, n_dev):
            q_copy(s, d).wait_recv()
    for s in range(n_steps):
        for d in range(1, n_dev):
            q_copy(s, d).wait_send()


def attention_kernel(len_ref, q_in, fk_ref, fv_ref, k_hbm, v_hbm, out_ref, k_out, v_out, k_buf, v_buf, q_rows, score_buf, prob_buf, head_buf, sems, out_sems):
    n_seqs, length, depth = k_buf.shape
    n_dev, n_steps, _, q_width = q_in.shape
    dev_heads = q_width // depth
    rows = n_dev * n_steps * dev_heads

    def fetch(b):
        return (pltpu.make_async_copy(k_hbm.at[b], k_buf.at[b], sems.at[0, b]),
                pltpu.make_async_copy(v_hbm.at[b], v_buf.at[b], sems.at[1, b]))

    def store(b):
        return (pltpu.make_async_copy(k_buf.at[b], k_out.at[b], out_sems.at[0, b]),
                pltpu.make_async_copy(v_buf.at[b], v_out.at[b], out_sems.at[1, b]))

    def patch(b, buf, fresh):
        start = pl.multiple_of(jnp.minimum(len_ref[b] // 8 * 8, length - WINDOW), 8)
        offset = len_ref[b] - start
        row = lax.broadcasted_iota(jnp.int32, (WINDOW, depth), 0)
        window = buf[b, pl.ds(start, WINDOW), :].astype(jnp.float32)
        for s in range(n_steps):
            window = jnp.where(row == offset + s, fresh[pl.ds(b * FRESH_ROWS + s, 1), :], window)
        buf[b, pl.ds(start, WINDOW), :] = window.astype(buf.dtype)

    def land(i):
        for j in range(2):
            b = 2 * i + j
            for copy in fetch(b):
                copy.wait()
            patch(b, k_buf, fk_ref)
            patch(b, v_buf, fv_ref)
            for copy in store(b):
                copy.start()

    for b in range(2 * AHEAD):
        for copy in fetch(b):
            copy.start()
    for u in range(n_dev):
        for s in range(n_steps):
            for h in range(dev_heads):
                first = ((u * n_steps + s) * dev_heads + h) * n_seqs
                q_rows[first:first + n_seqs, :] = q_in[u, s, :, h * depth:(h + 1) * depth].astype(jnp.float32)
    shape = (rows, FRESH_ROWS)
    step_of_row = lax.broadcasted_iota(jnp.int32, shape, 0) // dev_heads % n_steps
    fresh_mask = lax.broadcasted_iota(jnp.int32, shape, 1) <= step_of_row
    land(0)

    def attend_pair(i, carry):
        @pl.when(i < n_seqs // 2 - AHEAD)
        def _():
            for j in range(2):
                for copy in fetch(2 * (i + AHEAD) + j):
                    copy.start()

        @pl.when(i < n_seqs // 2 - 1)
        def _():
            land(i + 1)

        longest = jnp.maximum(len_ref[2 * i], len_ref[2 * i + 1])
        for first in range(0, length, KEY_RANGE):
            @pl.when((longest > first) & (longest <= first + KEY_RANGE))
            def _():
                for j in range(2):
                    b = 2 * i + j
                    q_one = q_rows[pl.ds(b, rows, stride=n_seqs), :].astype(jnp.bfloat16)
                    new = pl.ds(pl.multiple_of(b * FRESH_ROWS, FRESH_ROWS), FRESH_ROWS)
                    out = attend_one(first + KEY_RANGE, q_one, k_buf.at[b], v_buf.at[b], score_buf.at[j], prob_buf.at[j], len_ref[b],
                                     fk_ref[new, :].astype(jnp.bfloat16), fv_ref[new, :].astype(jnp.bfloat16), fresh_mask)
                    head_buf[pl.ds(b, rows, stride=n_seqs), :] = out
        return carry

    lax.fori_loop(0, n_seqs // 2, attend_pair, 0)
    for t in range(N_CHIPS):
        for s in range(n_steps):
            pieces = []
            for h in range(N_CORES * dev_heads):
                u = t * N_CORES + h // dev_heads
                first = ((u * n_steps + s) * dev_heads + h % dev_heads) * n_seqs
                pieces.append(head_buf[first:first + n_seqs, :])
            out_ref[t, s] = jnp.concatenate(pieces, axis=1).astype(out_ref.dtype)
    for b in range(n_seqs):
        for copy in store(b):
            copy.wait()


def project_kernel(n_steps, a_ref, w_ref, x_ref, b_ref, y_ref, w_buf, x_buf, a_buf, p_buf, mid_buf, fin_buf,
                   load_sems, w_sems, a_send, a_recv, f_send, f_recv, rs_send, rs_recv, ag_send, ag_recv):
    me = lax.axis_index('tp')
    chip, core = me // 2, me % 2
    n_seqs = a_ref.shape[2]
    block = 2 * n_seqs
    own_rows, width = w_ref.shape
    half = width // 2
    quarter = half // 2

    def chip_at(k):
        return (chip + k) % N_CHIPS

    def device(k):
        return {'tp': chip_at(k) * 2 + core}

    right, left, far, partner = device(1), device(3), device(2), {'tp': chip * 2 + 1 - core}

    barrier = pltpu.get_barrier_semaphore()
    for peer in (right, left, far, partner):
        pl.semaphore_signal(barrier, inc=1, device_id=peer, device_id_type=MESH)

    def cols(which, begin, size):
        return pl.ds(pl.multiple_of(which * half + begin, quarter), size)

    def rows_of(k):
        return pl.ds(pl.multiple_of(chip_at(k) * block, block), block)

    own_w_rows = pl.ds(pl.multiple_of(core * own_rows, own_rows), own_rows)
    w_load = pltpu.make_async_copy(w_ref.at[:, cols(core, 0, half)], w_buf.at[own_w_rows, :], load_sems.at[0])
    x_load = pltpu.make_async_copy(x_ref.at[:, rows_of(0), cols(core, 0, half)], x_buf, load_sems.at[1])
    w_load.start()
    x_load.start()
    pl.semaphore_wait(barrier, 4)

    def remote(src, dst, send, recv, to):
        return pltpu.make_async_remote_copy(src_ref=src, dst_ref=dst, send_sem=send, recv_sem=recv, device_id=to, device_id_type=MESH)

    def a_copy(s, d):
        return remote(a_ref.at[chip_at(d), s], a_buf.at[core, chip, s], a_send.at[s, d - 1], a_recv.at[s, d - 1], device(d))

    def a_forward(s, d):
        src = a_ref.at[chip, s] if d == 0 else a_buf.at[core, chip_at(N_CHIPS - d), s]
        return remote(src, a_buf.at[core, chip_at(N_CHIPS - d), s], f_send.at[s, d], f_recv.at[s, d], partner)

    for s in range(n_steps):
        for d in (2, 1, 3):
            a_copy(s, d).start()
        if s == 0:
            w_swap = remote(w_ref.at[:, cols(1 - core, 0, half)], w_buf.at[own_w_rows, :], w_sems.at[0], w_sems.at[1], partner)
            w_swap.start()
    for s in range(n_steps):
        a_forward(s, 0).start()
        a_buf[core, chip, s] = a_ref[chip, s]

    low, high = pl.ds(0, quarter), pl.ds(quarter, quarter)

    def rs(s, i):
        part = p_buf.at[s]
        src, dst, to = (
            (part.at[rows_of(2), low], mid_buf.at[s, 0], right),
            (part.at[rows_of(2), high], mid_buf.at[s, 1], left),
            (part.at[rows_of(1), high], fin_buf.at[s, 0], right),
            (part.at[rows_of(3), low], fin_buf.at[s, 1], left),
            (part.at[rows_of(1), low], fin_buf.at[s, 2], right),
            (part.at[rows_of(3), high], fin_buf.at[s, 3], left),
        )[i]
        return remote(src, dst, rs_send.at[s, i], rs_recv.at[s, i], to)

    def ag(s, i):
        k, begin, size, to = (
            (0, 0, half, right),
            (0, 0, half, left),
            (3, 0, quarter, right),
            (1, quarter, quarter, left),
            (0, 0, half, partner),
            (3, 0, half, partner),
            (1, 0, half, partner),
            (2, 0, quarter, partner),
            (2, quarter, quarter, partner),
        )[i]
        where = y_ref.at[s, rows_of(k), cols(core, begin, size)]
        return remote(where, where, ag_send.at[s, i], ag_recv.at[s, i], to)

    def partial(s):
        for d in (1, 3, 2):
            a_copy(s, d).wait_recv()
            a_forward(s, d).start()
        for d in range(N_CHIPS):
            a_forward(s, d).wait_recv()
        if s == 0:
            w_load.wait()
            w_swap.wait_recv()
        lhs = jnp.concatenate([a_buf[c, t, s] for t in range(N_CHIPS) for c in range(2)], axis=0)
        for n in range(0, half, 512):
            p_buf[s, :, n:n + 512] = jnp.dot(lhs, w_buf[:, n:n + 512], preferred_element_type=jnp.float32).astype(p_buf.dtype)
        for i in range(4):
            rs(s, i).start()

    def add_into(target, other):
        target[...] = (target[...].astype(jnp.float32) + other[...].astype(jnp.float32)).astype(target.dtype)

    def middle(s):
        rs(s, 0).wait_recv()
        add_into(p_buf.at[s, rows_of(1), low], mid_buf.at[s, 0])
        rs(s, 4).start()
        rs(s, 1).wait_recv()
        add_into(p_buf.at[s, rows_of(3), high], mid_buf.at[s, 1])
        rs(s, 5).start()

    def finish(s):
        for i in (2, 3, 4, 5):
            rs(s, i).wait_recv()
        if s == 0:
            x_load.wait()
        bias_row = b_ref[cols(core, 0, half)].astype(jnp.float32).reshape(1, half)
        for begin, one, two in ((0, 1, 2), (quarter, 0, 3)):
            total = p_buf[s, rows_of(0), begin:begin + quarter].astype(jnp.float32)
            total = total + fin_buf[s, one].astype(jnp.float32)
            total = total + fin_buf[s, two].astype(jnp.float32)
            total = total + x_buf[s, :, begin:begin + quarter].astype(jnp.float32)
            total = total + bias_row[:, begin:begin + quarter]
            y_ref[s, rows_of(0), cols(core, begin, quarter)] = total.astype(y_ref.dtype)
        for i in (0, 1, 4):
            ag(s, i).start()

    def relay(s):
        ag(s, 0).wait_recv()
        ag(s, 2).start()
        ag(s, 5).start()
        ag(s, 1).wait_recv()
        ag(s, 3).start()
        ag(s, 6).start()

    def last(s):
        ag(s, 2).wait_recv()
        ag(s, 7).start()
        ag(s, 3).wait_recv()
        ag(s, 8).start()

    stages = (partial, middle, finish, relay, last)
    for t in range(n_steps + len(stages) - 1):
        for i, stage in enumerate(stages):
            if 0 <= t - i < n_steps:
                stage(t - i)
    w_swap.wait_send()
    for s in range(n_steps):
        for i in range(4, 9):
            ag(s, i).wait_recv()
        for i in range(9):
            ag(s, i).wait_send()
        for i in range(6):
            rs(s, i).wait_send()
        for d in (1, 2, 3):
            a_copy(s, d).wait_send()
        for d in range(N_CHIPS):
            a_forward(s, d).wait_send()


def solution(mesh):
    def local_block(x_steps, seq_lens, k_cache, v_cache, ln_gain, ln_bias, w_q, b_q, w_kv, b_kv, w_out, b_out):
        n_steps, group_rows, width = x_steps.shape
        n_seqs, length, depth = k_cache.shape
        q_width = w_q.shape[1]
        n_dev = N_CHIPS * N_CORES
        rows = n_dev * n_steps * q_width // depth
        chip_width, half = N_CORES * q_width, width // 2
        block = N_CORES * n_seqs
        smem = pl.BlockSpec(memory_space=pltpu.SMEM)
        vmem = pl.BlockSpec(memory_space=pltpu.VMEM)
        hbm = pl.BlockSpec(memory_space=pltpu.HBM)
        dma = pltpu.SemaphoreType.DMA
        bf16, f32 = jnp.bfloat16, jnp.float32
        fresh_shape = (n_seqs * FRESH_ROWS, depth)
        q_in, fresh_k, fresh_v = pl.pallas_call(
            query_kernel,
            out_shape=[pltpu.VMEM((n_dev, n_steps, n_seqs, q_width), bf16), pltpu.VMEM(fresh_shape, f32), pltpu.VMEM(fresh_shape, f32)],
            in_specs=[vmem] * 4 + [hbm] * 3,
            out_specs=[vmem] * 3,
            scratch_shapes=[
                pltpu.VMEM(x_steps.shape, bf16),
                pltpu.VMEM(x_steps.shape, bf16),
                pltpu.VMEM((LN_ROWS, width), f32),
                pltpu.VMEM((LN_ROWS, width), f32),
                pltpu.VMEM(w_q.shape, bf16),
                pltpu.VMEM(w_kv.shape, bf16),
                pltpu.VMEM((n_steps, group_rows, q_width), bf16),
                dma((n_steps,)), dma((2,)),
                dma((n_steps, n_dev - 1)), dma((n_steps, n_dev - 1)),
            ],
            compiler_params=pltpu.CompilerParams(vmem_limit_bytes=FRONT_VMEM, collective_id=2, has_side_effects=True),
        )(ln_gain, ln_bias, b_q, b_kv, x_steps, w_q, w_kv)
        attn, k_out, v_out = pl.pallas_call(
            attention_kernel,
            out_shape=[pltpu.VMEM((N_CHIPS, n_steps, n_seqs, chip_width), bf16), jax.ShapeDtypeStruct(k_cache.shape, bf16), jax.ShapeDtypeStruct(v_cache.shape, bf16)],
            in_specs=[smem] + [vmem] * 3 + [hbm] * 2,
            out_specs=[vmem, hbm, hbm],
            scratch_shapes=[
                pltpu.VMEM(k_cache.shape, bf16),
                pltpu.VMEM(v_cache.shape, bf16),
                pltpu.VMEM((rows * n_seqs, depth), f32),
                pltpu.VMEM((2, rows, length), f32),
                pltpu.VMEM((2, rows, length), bf16),
                pltpu.VMEM((rows * n_seqs, depth), f32),
                dma((2, n_seqs)), dma((2, n_seqs)),
            ],
            compiler_params=pltpu.CompilerParams(vmem_limit_bytes=ATTENTION_VMEM),
            cost_estimate=pl.CostEstimate(flops=4 * n_seqs * rows * length * depth, bytes_accessed=8 * n_seqs * length * depth, transcendentals=n_seqs * rows * length),
        )(seq_lens, q_in, fresh_k, fresh_v, k_cache, v_cache)
        y_steps = pl.pallas_call(
            functools.partial(project_kernel, n_steps),
            out_shape=jax.ShapeDtypeStruct(x_steps.shape, bf16),
            in_specs=[vmem, hbm, hbm, vmem],
            out_specs=vmem,
            scratch_shapes=[
                pltpu.VMEM((chip_width, half), bf16),
                pltpu.VMEM((n_steps, block, half), bf16),
                pltpu.VMEM((2, N_CHIPS, n_steps, n_seqs, chip_width), bf16),
                pltpu.VMEM((n_steps, N_CHIPS * block, half), bf16),
                pltpu.VMEM((n_steps, 2, block, half // 2), bf16),
                pltpu.VMEM((n_steps, 4, block, half // 2), bf16),
                dma((2,)), dma((2,)),
                dma((n_steps, 3)), dma((n_steps, 3)),
                dma((n_steps, 4)), dma((n_steps, 4)),
                dma((n_steps, 6)), dma((n_steps, 6)),
                dma((n_steps, 9)), dma((n_steps, 9)),
            ],
            compiler_params=pltpu.CompilerParams(vmem_limit_bytes=BACK_VMEM, collective_id=1, has_side_effects=True),
            cost_estimate=pl.CostEstimate(flops=2 * n_steps * N_CHIPS * block * chip_width * half, bytes_accessed=4 * width * chip_width, transcendentals=0),
        )(attn, w_out, x_steps, b_out)
        return y_steps, k_out, v_out

    row_spec = P(('dp', 'tp'), None, None)
    return jax.shard_map(
        local_block,
        mesh=mesh,
        in_specs=(P(None, 'dp', None), P(('dp', 'tp')), row_spec, row_spec, P(None), P(None), P(None, 'tp'), P('tp'), P(None, None), P(None), P('tp', None), P(None)),
        out_specs=(P(None, 'dp', None), row_spec, row_spec),
        check_vma=False,
    )
```

```python
import functools
import math

import jax
import jax.numpy as jnp
from jax import lax
from jax.experimental import pallas as pl
from jax.experimental.pallas import tpu as pltpu
from jax.sharding import PartitionSpec as P

LN_EPS = 1e-5
KEY_TILE = 256
LANES = 128
FRESH_ROWS = 16
WINDOW = 16
N_CHIPS = 4
N_CORES = 2
N_PARTS = 2
LN_ROWS = 16
MESH = pl.DeviceIdType.MESH
BLOCK_VMEM = 32 * 1024 * 1024


CONTRACT_LAST = (((1,), (1,)), ((), ()))


def score_tile(q_rows, k_ref, score_ref, start, seq_len, best):
    tile = lax.dot_general(q_rows, k_ref[start:start + KEY_TILE, :], CONTRACT_LAST, preferred_element_type=jnp.float32)
    lane = lax.broadcasted_iota(jnp.int32, tile.shape, 1)
    tile = jnp.where(lane < seq_len - start, tile, -jnp.inf)
    score_ref[:, start:start + KEY_TILE] = tile
    high = jnp.maximum(tile[:, :LANES], tile[:, LANES:])
    return high if best is None else jnp.maximum(best, high)


def attend_one(q_rows, v_ref, score_ref, best, fresh_k, fresh_v, fresh_mask, beside):
    length, depth = v_ref.shape
    to_log2 = depth ** -0.5 * math.log2(math.e)
    new_scores = lax.dot_general(q_rows, fresh_k, CONTRACT_LAST, preferred_element_type=jnp.float32)
    new_scores = jnp.where(fresh_mask, new_scores, -jnp.inf)
    top = jnp.maximum(jnp.max(best, axis=-1, keepdims=True), jnp.max(new_scores, axis=-1, keepdims=True))
    new_weights = jnp.exp2((new_scores - top) * to_log2)
    numerator = jnp.dot(new_weights.astype(jnp.bfloat16), fresh_v, preferred_element_type=jnp.float32)
    total = None
    for start in range(0, length, KEY_TILE):
        beside(start)
        weights = jnp.exp2((score_ref[:, start:start + KEY_TILE] - top) * to_log2)
        folded = weights[:, :LANES] + weights[:, LANES:]
        total = folded if total is None else total + folded
        numerator = numerator + jnp.dot(weights.astype(jnp.bfloat16), v_ref[start:start + KEY_TILE, :], preferred_element_type=jnp.float32)
    return numerator / (jnp.sum(total, axis=-1, keepdims=True) + jnp.sum(new_weights, axis=-1, keepdims=True))


def block_kernel(
        len_ref, g_ref, lb_ref, bq_ref, bkv_ref, bo_ref, x_hbm, wq_hbm, wkv_hbm, wo_hbm, k_hbm, v_hbm,
        y_ref, k_buf, v_buf, fk_ref, fv_ref,
        x_buf, own_x, own_h, h_buf, gain_buf, bias_buf, bo_buf, wq_buf, wkv_buf, w_buf, swap_buf, q_buf, q_in, q_rows, score_buf, best_buf, head_buf, a_src, a_buf, lhs_buf, p_buf, mid_buf, fin_buf,
        x_sems, w_sems, kv_sems, swap_sems, q_send, q_recv, a_send, a_recv, f_send, f_recv, rs_send, rs_recv, ag_send, ag_recv):
    me = lax.axis_index('tp')
    n_dev = N_CHIPS * N_CORES
    chip, core = me // N_CORES, me % N_CORES
    n_steps, _, width = own_x.shape
    n_seqs, length, depth = k_buf.shape
    q_width = wq_buf.shape[1]
    dev_heads = q_width // depth
    chip_heads = N_CORES * dev_heads
    part_seqs = n_seqs // N_PARTS
    rows = n_dev * n_steps * dev_heads
    own_rows = wo_hbm.shape[0]
    half, quarter = width // 2, width // 4
    block = N_CORES * part_seqs

    def chip_at(k):
        return (chip + k) % N_CHIPS

    def device(k):
        return {'tp': chip_at(k) * N_CORES + core}

    def member(d):
        return (me + d) % n_dev

    right, left, partner = device(1), device(3), {'tp': chip * N_CORES + 1 - core}

    def remote(src, dst, send, recv, to):
        return pltpu.make_async_remote_copy(src_ref=src, dst_ref=dst, send_sem=send, recv_sem=recv, device_id=to, device_id_type=MESH)

    def cols(which, begin, size):
        return pl.ds(pl.multiple_of(which * half + begin, quarter), size)

    barrier = pltpu.get_barrier_semaphore()
    for d in range(1, n_dev):
        pl.semaphore_signal(barrier, inc=1, device_id={'tp': member(d)}, device_id_type=MESH)

    def x_load(p):
        return pltpu.make_async_copy(x_hbm.at[:, :, p], x_buf.at[p], x_sems.at[p])

    def kv_load(b):
        return (pltpu.make_async_copy(k_hbm.at[b], k_buf.at[b], kv_sems.at[0, b]),
                pltpu.make_async_copy(v_hbm.at[b], v_buf.at[b], kv_sems.at[1, b]))

    own_x_loads = [pltpu.make_async_copy(x_hbm.at[:, me, p], own_x.at[:, p * part_seqs:(p + 1) * part_seqs, :], x_sems.at[N_PARTS + p]) for p in range(N_PARTS)]
    own_w_rows = pl.ds(pl.multiple_of(core * own_rows, own_rows), own_rows)
    wq_load = pltpu.make_async_copy(wq_hbm, wq_buf, w_sems.at[0])
    wkv_load = pltpu.make_async_copy(wkv_hbm, wkv_buf, w_sems.at[1])
    wo_load = pltpu.make_async_copy(wo_hbm.at[:, cols(core, 0, half)], w_buf.at[own_w_rows, :], w_sems.at[2])
    swap_load = pltpu.make_async_copy(wo_hbm.at[:, cols(1 - core, 0, half)], swap_buf, w_sems.at[3])
    wo_swap = remote(swap_buf, w_buf.at[own_w_rows, :], swap_sems.at[0], swap_sems.at[1], partner)
    x_load(0).start()
    wq_load.start()

    bq_row = bq_ref[...].astype(jnp.float32).reshape(1, q_width)
    bo_buf[...] = bo_ref[...].astype(jnp.float32).reshape(1, width)
    gain_buf[...] = jnp.broadcast_to(g_ref[...].astype(jnp.float32).reshape(1, width), gain_buf.shape)
    bias_buf[...] = jnp.broadcast_to(lb_ref[...].astype(jnp.float32).reshape(1, width), bias_buf.shape)

    def norm(x_float):
        centered = x_float - jnp.mean(x_float, axis=-1, keepdims=True)
        row_var = jnp.mean(centered * centered, axis=-1, keepdims=True)
        scaled = centered * lax.rsqrt(row_var + LN_EPS)
        return (scaled * gain_buf[...] + bias_buf[...]).astype(h_buf.dtype)

    def q_copy(p, d):
        return remote(q_buf.at[p, :, member(d)], q_in.at[p, me], q_send.at[p, d - 1], q_recv.at[p, d - 1], {'tp': member(d)})

    group = LN_ROWS // part_seqs
    for p in range(N_PARTS):
        x_load(p).wait()
        if p == 0:
            for later in range(1, N_PARTS):
                x_load(later).start()
            for copy in own_x_loads:
                copy.start()
            wkv_load.start()

        for s in range(n_steps):
            def norm_rows(i, carry):
                x_float = jnp.concatenate([x_buf[p, s, i * group + j].astype(jnp.float32) for j in range(group)], axis=0)
                where = pl.ds(pl.multiple_of((s * n_dev // group + i) * LN_ROWS, LN_ROWS), LN_ROWS)
                h_buf[p, where, :] = norm(x_float)
                return carry

            lax.fori_loop(0, n_dev // group, norm_rows, 0)
        if p == 0:
            wq_load.wait()
            swap_load.start()
            wo_load.start()
        for n in range(0, q_width, 256):
            part = jnp.dot(h_buf[p], wq_buf[:, n:n + 256], preferred_element_type=jnp.float32) + bq_row[:, n:n + 256]
            for s in range(n_steps):
                for u in range(n_dev):
                    first = (s * n_dev + u) * part_seqs
                    q_buf[p, s, u, :, n:n + 256] = part[first:first + part_seqs].astype(q_buf.dtype)
        if p == 0:
            pl.semaphore_wait(barrier, n_dev - 1)
        for d in range(1, n_dev):
            q_copy(p, d).start()
        if p == 0:
            swap_load.wait()
            wo_swap.start()
        for b in range(p * part_seqs, (p + 1) * part_seqs):
            for copy in kv_load(b):
                copy.start()
        q_in[p, me] = q_buf[p, :, me]

    for copy in own_x_loads:
        copy.wait()
    for s in range(n_steps):
        own_h[s * n_seqs:(s + 1) * n_seqs, :] = norm(own_x[s].astype(jnp.float32))
    wkv_load.wait()
    fresh = jnp.dot(own_h[...], wkv_buf[...], preferred_element_type=jnp.float32) + bkv_ref[...].astype(jnp.float32).reshape(1, -1)
    fresh = fresh.astype(jnp.bfloat16).astype(jnp.float32)
    fk_ref[...] = jnp.zeros_like(fk_ref)
    fv_ref[...] = jnp.zeros_like(fv_ref)
    for s in range(n_steps):
        where = pl.ds(s, n_seqs, stride=FRESH_ROWS)
        fk_ref[where, :] = fresh[s * n_seqs:(s + 1) * n_seqs, :depth]
        fv_ref[where, :] = fresh[s * n_seqs:(s + 1) * n_seqs, depth:]

    def unpack(p):
        for d in range(1, n_dev):
            q_copy(p, d).wait_recv()
        for u in range(n_dev):
            for s in range(n_steps):
                for h in range(dev_heads):
                    first = ((u * n_steps + s) * dev_heads + h) * n_seqs + p * part_seqs
                    q_rows[first:first + part_seqs, :] = q_in[p, u, s, :, h * depth:(h + 1) * depth].astype(jnp.float32)

    shape = (rows, FRESH_ROWS)
    step_of_row = lax.broadcasted_iota(jnp.int32, shape, 0) // dev_heads % n_steps
    fresh_mask = lax.broadcasted_iota(jnp.int32, shape, 1) <= step_of_row

    def a_copy(p, d):
        return remote(a_src.at[p, chip_at(d)], a_buf.at[p, core, chip], a_send.at[p, d - 1], a_recv.at[p, d - 1], device(d))

    def a_forward(p, d):
        where = a_buf.at[p, core, chip_at(N_CHIPS - d)]
        return remote(a_src.at[p, chip] if d == 0 else where, where, f_send.at[p, d], f_recv.at[p, d], partner)

    low, high = pl.ds(0, quarter), pl.ds(quarter, quarter)

    def rs(p, s, i):
        def part(k, where):
            return p_buf.at[p, s, chip_at(k), :, where]
        src, dst, to = (
            (part(2, low), mid_buf.at[p, s, 0], right),
            (part(2, high), mid_buf.at[p, s, 1], left),
            (part(1, high), fin_buf.at[p, s, 0], right),
            (part(3, low), fin_buf.at[p, s, 1], left),
            (part(1, low), fin_buf.at[p, s, 2], right),
            (part(3, high), fin_buf.at[p, s, 3], left),
        )[i]
        return remote(src, dst, rs_send.at[p, s, i], rs_recv.at[p, s, i], to)

    def ag(p, s, i):
        k, begin, size, to = (
            (0, 0, half, right),
            (0, 0, half, left),
            (3, 0, quarter, right),
            (1, quarter, quarter, left),
            (0, 0, half, partner),
            (3, 0, half, partner),
            (1, 0, half, partner),
            (2, 0, quarter, partner),
            (2, quarter, quarter, partner),
        )[i]
        where = y_ref.at[s, chip_at(k), :, p, :, cols(core, begin, size)]
        return remote(where, where, ag_send.at[p, s, i], ag_recv.at[p, s, i], to)

    def pack(p):
        for t in range(N_CHIPS):
            for s in range(n_steps):
                pieces = []
                for h in range(chip_heads):
                    u = t * N_CORES + h // dev_heads
                    first = ((u * n_steps + s) * dev_heads + h % dev_heads) * n_seqs + p * part_seqs
                    pieces.append(head_buf[first:first + part_seqs, :])
                a_src[p, t, s] = jnp.concatenate(pieces, axis=1).astype(a_src.dtype)
        for d in (2, 1, 3):
            a_copy(p, d).start()
        a_forward(p, 0).start()
        a_buf[p, core, chip] = a_src[p, chip]

    def forward(p):
        for d in (1, 3, 2):
            a_copy(p, d).wait_recv()
            a_forward(p, d).start()

    def partial(p):
        for d in range(N_CHIPS):
            a_forward(p, d).wait_recv()
        if p == 0:
            wo_load.wait()
            wo_swap.wait_recv()
        for s in range(n_steps):
            for t in range(N_CHIPS):
                pair = jnp.concatenate([a_buf[p, c, t, s].astype(jnp.float32) for c in range(N_CORES)], axis=0)
                first = (s * N_CHIPS + t) * block
                lhs_buf[first:first + block, :] = pair.astype(lhs_buf.dtype)
        for n in range(0, half, 512):
            out = jnp.dot(lhs_buf[...], w_buf[:, n:n + 512], preferred_element_type=jnp.float32).astype(p_buf.dtype)
            for s in range(n_steps):
                for t in range(N_CHIPS):
                    first = (s * N_CHIPS + t) * block
                    p_buf[p, s, t, :, n:n + 512] = out[first:first + block]
        for pair in ((0, 1), (2, 3)):
            for s in range(n_steps):
                for i in pair:
                    rs(p, s, i).start()

    def add_into(target, other):
        target[...] = (target[...].astype(jnp.float32) + other[...].astype(jnp.float32)).astype(target.dtype)

    def middle(p, s):
        rs(p, s, 0).wait_recv()
        add_into(p_buf.at[p, s, chip_at(1), :, low], mid_buf.at[p, s, 0])
        rs(p, s, 4).start()
        rs(p, s, 1).wait_recv()
        add_into(p_buf.at[p, s, chip_at(3), :, high], mid_buf.at[p, s, 1])
        rs(p, s, 5).start()

    def finish(p, s):
        for i in (2, 3, 4, 5):
            rs(p, s, i).wait_recv()
        for begin, one, two in ((0, 1, 2), (quarter, 0, 3)):
            where = cols(core, begin, quarter)
            total = p_buf[p, s, chip, :, begin:begin + quarter].astype(jnp.float32)
            total = total + fin_buf[p, s, one].astype(jnp.float32)
            total = total + fin_buf[p, s, two].astype(jnp.float32)
            total = total + bo_buf[:, where]
            for c in range(N_CORES):
                x_part = x_buf[p, s, chip * N_CORES + c, :, where].astype(jnp.float32)
                y_ref[s, chip, c, p, :, where] = (x_part + total[c * part_seqs:(c + 1) * part_seqs]).astype(y_ref.dtype)
        for i in (0, 1, 4):
            ag(p, s, i).start()

    def relay(p, s):
        ag(p, s, 0).wait_recv()
        ag(p, s, 2).start()
        ag(p, s, 5).start()
        ag(p, s, 1).wait_recv()
        ag(p, s, 3).start()
        ag(p, s, 6).start()

    def last(p, s):
        ag(p, s, 2).wait_recv()
        ag(p, s, 7).start()
        ag(p, s, 3).wait_recv()
        ag(p, s, 8).start()

    def each(stage, p):
        for s in range(n_steps):
            stage(p, s)

    def query(b):
        return q_rows[pl.ds(b, rows, stride=n_seqs), :].astype(jnp.bfloat16)

    def attend(b, slot, after):
        new = pl.ds(pl.multiple_of(b * FRESH_ROWS, FRESH_ROWS), FRESH_ROWS)
        q_after = query(after)
        maxima = [None]

        def beside(start):
            maxima[0] = score_tile(q_after, k_buf.at[after], score_buf.at[1 - slot], start, len_ref[after], maxima[0])

        out = attend_one(query(b), v_buf.at[b], score_buf.at[slot], best_buf[slot],
                         fk_ref[new, :].astype(jnp.bfloat16), fv_ref[new, :].astype(jnp.bfloat16), fresh_mask, beside)
        best_buf[1 - slot] = maxima[0]
        head_buf[pl.ds(b, rows, stride=n_seqs), :] = out

    def wait_caches(b):
        for copy in kv_load(b):
            copy.wait()

    def attend_pair(i, carry):
        first = 2 * i
        after = jnp.minimum(first + 2, n_seqs - 1)
        wait_caches(first + 1)

        @pl.when(first + 2 < n_seqs)
        def _():
            wait_caches(after)

        attend(first, 0, first + 1)
        attend(first + 1, 1, after)

        @pl.when(i == part_seqs // 2 - 2)
        def _():
            unpack(1)

        @pl.when(i == part_seqs // 2 - 1)
        def _():
            pack(0)

        @pl.when(i == n_seqs // 2 - 2)
        def _():
            forward(0)

        return carry

    unpack(0)
    wait_caches(0)
    best = None
    for start in range(0, length, KEY_TILE):
        best = score_tile(query(0), k_buf.at[0], score_buf.at[0], start, len_ref[0], best)
    best_buf[0] = best
    lax.fori_loop(0, n_seqs // 2, attend_pair, 0)
    pack(1)
    partial(0)
    forward(1)
    each(middle, 0)
    partial(1)
    each(finish, 0)
    each(middle, 1)
    each(relay, 0)
    each(finish, 1)
    each(last, 0)
    each(relay, 1)
    each(last, 1)
    wo_swap.wait_send()
    for p in range(N_PARTS):
        for d in range(1, n_dev):
            q_copy(p, d).wait_send()
        for s in range(n_steps):
            for i in range(4, 9):
                ag(p, s, i).wait_recv()
            for i in range(9):
                ag(p, s, i).wait_send()
            for i in range(6):
                rs(p, s, i).wait_send()
        for d in (1, 2, 3):
            a_copy(p, d).wait_send()
        for d in range(N_CHIPS):
            a_forward(p, d).wait_send()


def store_kernel(n_steps, len_ref, fk_ref, fv_ref, y_ref, k_ref, v_ref, y_out, k_out, v_out, k_buf, v_buf, sems, y_sem):
    n_seqs, length, depth = k_buf.shape

    def store(b):
        return (pltpu.make_async_copy(k_buf.at[b], k_out.at[b], sems.at[0, b]),
                pltpu.make_async_copy(v_buf.at[b], v_out.at[b], sems.at[1, b]))

    def patch(b, buf, fresh):
        start = pl.multiple_of(jnp.minimum(len_ref[b] // 8 * 8, length - WINDOW), 8)
        offset = len_ref[b] - start
        row = lax.broadcasted_iota(jnp.int32, (WINDOW, depth), 0)
        window = buf[b, pl.ds(start, WINDOW), :].astype(jnp.float32)
        for s in range(n_steps):
            window = jnp.where(row == offset + s, fresh[b * FRESH_ROWS + s:b * FRESH_ROWS + s + 1, :], window)
        buf[b, pl.ds(start, WINDOW), :] = window.astype(buf.dtype)

    y_copy = pltpu.make_async_copy(y_ref, y_out, y_sem)
    y_copy.start()
    for b in range(n_seqs):
        patch(b, k_buf, fk_ref)
        patch(b, v_buf, fv_ref)
        for copy in store(b):
            copy.start()
    y_copy.wait()
    for b in range(n_seqs):
        for copy in store(b):
            copy.wait()


def solution(mesh):
    def local_block(x_steps, seq_lens, k_cache, v_cache, ln_gain, ln_bias, w_q, b_q, w_kv, b_kv, w_out, b_out):
        n_steps, _, width = x_steps.shape
        n_seqs, length, depth = k_cache.shape
        q_width = w_q.shape[1]
        n_dev = N_CHIPS * N_CORES
        part_seqs = n_seqs // N_PARTS
        rows = n_dev * n_steps * q_width // depth
        chip_width, half = N_CORES * q_width, width // 2
        block = N_CORES * part_seqs
        smem = pl.BlockSpec(memory_space=pltpu.SMEM)
        vmem = pl.BlockSpec(memory_space=pltpu.VMEM)
        hbm = pl.BlockSpec(memory_space=pl.ANY)
        dma = pltpu.SemaphoreType.DMA
        bf16, f32 = jnp.bfloat16, jnp.float32
        y_shape = (n_steps, N_CHIPS, N_CORES, N_PARTS, part_seqs, width)
        fresh_shape = (n_seqs * FRESH_ROWS, depth)
        y_vm, k_vm, v_vm, fresh_k, fresh_v = pl.pallas_call(
            block_kernel,
            out_shape=[pltpu.VMEM(y_shape, bf16), pltpu.VMEM(k_cache.shape, bf16), pltpu.VMEM(v_cache.shape, bf16), pltpu.VMEM(fresh_shape, f32), pltpu.VMEM(fresh_shape, f32)],
            in_specs=[smem] + [vmem] * 5 + [hbm] * 6,
            out_specs=[vmem] * 5,
            scratch_shapes=[
                pltpu.VMEM((N_PARTS, n_steps, n_dev, part_seqs, width), bf16),
                pltpu.VMEM((n_steps, n_seqs, width), bf16),
                pltpu.VMEM((n_steps * n_seqs, width), bf16),
                pltpu.VMEM((N_PARTS, n_steps * n_dev * part_seqs, width), bf16),
                pltpu.VMEM((LN_ROWS, width), f32),
                pltpu.VMEM((LN_ROWS, width), f32),
                pltpu.VMEM((1, width), f32),
                pltpu.VMEM(w_q.shape, bf16),
                pltpu.VMEM(w_kv.shape, bf16),
                pltpu.VMEM((chip_width, half), bf16),
                pltpu.VMEM((q_width, half), bf16),
                pltpu.VMEM((N_PARTS, n_steps, n_dev, part_seqs, q_width), bf16),
                pltpu.VMEM((N_PARTS, n_dev, n_steps, part_seqs, q_width), bf16),
                pltpu.VMEM((rows * n_seqs, depth), f32),
                pltpu.VMEM((2, rows, length), f32),
                pltpu.VMEM((2, rows, LANES), f32),
                pltpu.VMEM((rows * n_seqs, depth), f32),
                pltpu.VMEM((N_PARTS, N_CHIPS, n_steps, part_seqs, chip_width), bf16),
                pltpu.VMEM((N_PARTS, N_CORES, N_CHIPS, n_steps, part_seqs, chip_width), bf16),
                pltpu.VMEM((n_steps * N_CHIPS * block, chip_width), bf16),
                pltpu.VMEM((N_PARTS, n_steps, N_CHIPS, block, half), bf16),
                pltpu.VMEM((N_PARTS, n_steps, 2, block, half // 2), bf16),
                pltpu.VMEM((N_PARTS, n_steps, 4, block, half // 2), bf16),
                dma((2 * N_PARTS,)), dma((4,)), dma((2, n_seqs)), dma((2,)),
                dma((N_PARTS, n_dev - 1)), dma((N_PARTS, n_dev - 1)),
                dma((N_PARTS, 3)), dma((N_PARTS, 3)),
                dma((N_PARTS, N_CHIPS)), dma((N_PARTS, N_CHIPS)),
                dma((N_PARTS, n_steps, 6)), dma((N_PARTS, n_steps, 6)),
                dma((N_PARTS, n_steps, 9)), dma((N_PARTS, n_steps, 9)),
            ],
            compiler_params=pltpu.CompilerParams(vmem_limit_bytes=BLOCK_VMEM, collective_id=1, has_side_effects=True),
            cost_estimate=pl.CostEstimate(flops=4 * n_seqs * rows * length * depth, bytes_accessed=4 * n_seqs * length * depth, transcendentals=n_seqs * rows * length),
        )(seq_lens, ln_gain, ln_bias, b_q, b_kv, b_out,
          x_steps.reshape(n_steps, n_dev, N_PARTS, part_seqs, width), w_q, w_kv, w_out, k_cache, v_cache)
        y_steps, k_out, v_out, _, _ = pl.pallas_call(
            functools.partial(store_kernel, n_steps),
            out_shape=[jax.ShapeDtypeStruct(y_shape, bf16), jax.ShapeDtypeStruct(k_cache.shape, bf16), jax.ShapeDtypeStruct(v_cache.shape, bf16), pltpu.VMEM(k_cache.shape, bf16), pltpu.VMEM(v_cache.shape, bf16)],
            in_specs=[smem] + [vmem] * 5,
            out_specs=[hbm] * 3 + [vmem] * 2,
            scratch_shapes=[dma((2, n_seqs)), dma],
            input_output_aliases={4: 3, 5: 4},
            compiler_params=pltpu.CompilerParams(vmem_limit_bytes=2 * 1024 * 1024),
        )(seq_lens, fresh_k, fresh_v, y_vm, k_vm, v_vm)
        return y_steps.reshape(x_steps.shape), k_out, v_out

    row_spec = P(('dp', 'tp'), None, None)
    return jax.shard_map(
        local_block,
        mesh=mesh,
        in_specs=(P(None, 'dp', None), P(('dp', 'tp')), row_spec, row_spec, P(None), P(None), P(None, 'tp'), P('tp'), P(None, None), P(None), P('tp', None), P(None)),
        out_specs=(P(None, 'dp', None), row_spec, row_spec),
        check_vma=False,
    )
```

```python
import functools
import math

import jax
import jax.numpy as jnp
from jax import lax
from jax.experimental import pallas as pl
from jax.experimental.pallas import tpu as pltpu
from jax.sharding import PartitionSpec as P

LN_EPS = 1e-5
KEY_TILE = 256
LANES = 128
FRESH_ROWS = 16
WINDOW = 16
N_CHIPS = 4
N_CORES = 2
N_PARTS = 2
LN_ROWS = 16
MESH = pl.DeviceIdType.MESH
BLOCK_VMEM = 32 * 1024 * 1024


CONTRACT_LAST = (((1,), (1,)), ((), ()))


def score_tile(q_rows, k_ref, score_ref, start, seq_len, best):
    tile = lax.dot_general(q_rows, k_ref[start:start + KEY_TILE, :], CONTRACT_LAST, preferred_element_type=jnp.float32)
    lane = lax.broadcasted_iota(jnp.int32, tile.shape, 1)
    tile = jnp.where(lane < seq_len - start, tile, -jnp.inf)
    score_ref[:, start:start + KEY_TILE] = tile
    high = jnp.maximum(tile[:, :LANES], tile[:, LANES:])
    return high if best is None else jnp.maximum(best, high)


def attend_one(q_rows, v_ref, score_ref, best, fresh_k, fresh_v, fresh_mask, beside):
    length, depth = v_ref.shape
    to_log2 = depth ** -0.5 * math.log2(math.e)
    new_scores = lax.dot_general(q_rows, fresh_k, CONTRACT_LAST, preferred_element_type=jnp.float32)
    new_scores = jnp.where(fresh_mask, new_scores, -jnp.inf)
    top = jnp.maximum(jnp.max(best, axis=-1, keepdims=True), jnp.max(new_scores, axis=-1, keepdims=True))
    new_weights = jnp.exp2((new_scores - top) * to_log2)
    numerator = jnp.dot(new_weights.astype(jnp.bfloat16), fresh_v, preferred_element_type=jnp.float32)
    total = None
    for start in range(0, length, KEY_TILE):
        beside(start)
        weights = jnp.exp2((score_ref[:, start:start + KEY_TILE] - top) * to_log2)
        folded = weights[:, :LANES] + weights[:, LANES:]
        total = folded if total is None else total + folded
        numerator = numerator + jnp.dot(weights.astype(jnp.bfloat16), v_ref[start:start + KEY_TILE, :], preferred_element_type=jnp.float32)
    return numerator / (jnp.sum(total, axis=-1, keepdims=True) + jnp.sum(new_weights, axis=-1, keepdims=True))


def block_kernel(
        len_hbm, g_hbm, lb_hbm, bq_hbm, bkv_hbm, bo_hbm, x_hbm, wq_hbm, wkv_hbm, wo_hbm, k_hbm, v_hbm,
        y_ref, k_buf, v_buf, fk_ref, fv_ref,
        len_ref, g_ref, lb_ref, bq_ref, bkv_ref, bo_ref, x_buf, own_x, own_h, h_buf, gain_buf, bias_buf, bo_buf, wq_buf, wkv_buf, w_buf, swap_buf, q_buf, q_in, q_rows, score_buf, best_buf, head_buf, a_src, a_buf, lhs_buf, p_buf, mid_buf, fin_buf,
        vec_sems, x_sems, w_sems, kv_sems, swap_sems, q_send, q_recv, a_send, a_recv, f_send, f_recv, rs_send, rs_recv, ag_send, ag_recv):
    me = lax.axis_index('tp')
    n_dev = N_CHIPS * N_CORES
    chip, core = me // N_CORES, me % N_CORES
    n_steps, _, width = own_x.shape
    n_seqs, length, depth = k_buf.shape
    q_width = wq_buf.shape[1]
    dev_heads = q_width // depth
    chip_heads = N_CORES * dev_heads
    part_seqs = n_seqs // N_PARTS
    rows = n_dev * n_steps * dev_heads
    own_rows = wo_hbm.shape[0]
    half, quarter = width // 2, width // 4
    block = N_CORES * part_seqs

    def chip_at(k):
        return (chip + k) % N_CHIPS

    def device(k):
        return {'tp': chip_at(k) * N_CORES + core}

    def member(d):
        return (me + d) % n_dev

    right, left, partner = device(1), device(3), {'tp': chip * N_CORES + 1 - core}

    def remote(src, dst, send, recv, to):
        return pltpu.make_async_remote_copy(src_ref=src, dst_ref=dst, send_sem=send, recv_sem=recv, device_id=to, device_id_type=MESH)

    def cols(which, begin, size):
        return pl.ds(pl.multiple_of(which * half + begin, quarter), size)

    def x_load(p):
        return pltpu.make_async_copy(x_hbm.at[:, :, p], x_buf.at[p], x_sems.at[p])

    def kv_load(b):
        return (pltpu.make_async_copy(k_hbm.at[b], k_buf.at[b], kv_sems.at[0, b]),
                pltpu.make_async_copy(v_hbm.at[b], v_buf.at[b], kv_sems.at[1, b]))

    own_x_loads = [pltpu.make_async_copy(x_hbm.at[:, me, p], own_x.at[:, p * part_seqs:(p + 1) * part_seqs, :], x_sems.at[N_PARTS + p]) for p in range(N_PARTS)]
    own_w_rows = pl.ds(pl.multiple_of(core * own_rows, own_rows), own_rows)
    wq_load = pltpu.make_async_copy(wq_hbm, wq_buf, w_sems.at[0])
    wkv_load = pltpu.make_async_copy(wkv_hbm, wkv_buf, w_sems.at[1])
    wo_load = pltpu.make_async_copy(wo_hbm.at[:, cols(core, 0, half)], w_buf.at[own_w_rows, :], w_sems.at[2])
    swap_load = pltpu.make_async_copy(wo_hbm.at[:, cols(1 - core, 0, half)], swap_buf, w_sems.at[3])
    wo_swap = remote(swap_buf, w_buf.at[own_w_rows, :], swap_sems.at[0], swap_sems.at[1], partner)
    vector_loads = [pltpu.make_async_copy(src, dst, vec_sems.at[i]) for i, (src, dst) in enumerate(
        ((g_hbm, g_ref), (lb_hbm, lb_ref), (bq_hbm, bq_ref), (bkv_hbm, bkv_ref), (bo_hbm, bo_ref), (len_hbm, len_ref)))]
    for copy in vector_loads:
        copy.start()
    x_load(0).start()
    wq_load.start()

    barrier = pltpu.get_barrier_semaphore()
    for d in range(1, n_dev):
        pl.semaphore_signal(barrier, inc=1, device_id={'tp': member(d)}, device_id_type=MESH)

    for copy in vector_loads:
        copy.wait()

    bq_row = bq_ref[...].astype(jnp.float32).reshape(1, q_width)
    bo_buf[...] = bo_ref[...].astype(jnp.float32).reshape(1, width)
    gain_buf[...] = jnp.broadcast_to(g_ref[...].astype(jnp.float32).reshape(1, width), gain_buf.shape)
    bias_buf[...] = jnp.broadcast_to(lb_ref[...].astype(jnp.float32).reshape(1, width), bias_buf.shape)

    def norm(x_float):
        centered = x_float - jnp.mean(x_float, axis=-1, keepdims=True)
        row_var = jnp.mean(centered * centered, axis=-1, keepdims=True)
        scaled = centered * lax.rsqrt(row_var + LN_EPS)
        return (scaled * gain_buf[...] + bias_buf[...]).astype(h_buf.dtype)

    def q_copy(p, d):
        return remote(q_buf.at[p, :, member(d)], q_in.at[p, me], q_send.at[p, d - 1], q_recv.at[p, d - 1], {'tp': member(d)})

    group = LN_ROWS // part_seqs
    for p in range(N_PARTS):
        x_load(p).wait()
        if p == 0:
            for later in range(1, N_PARTS):
                x_load(later).start()
            for copy in own_x_loads:
                copy.start()
            wkv_load.start()

        for s in range(n_steps):
            def norm_rows(i, carry):
                x_float = jnp.concatenate([x_buf[p, s, i * group + j].astype(jnp.float32) for j in range(group)], axis=0)
                where = pl.ds(pl.multiple_of((s * n_dev // group + i) * LN_ROWS, LN_ROWS), LN_ROWS)
                h_buf[p, where, :] = norm(x_float)
                return carry

            lax.fori_loop(0, n_dev // group, norm_rows, 0)
        if p == 0:
            wq_load.wait()
            swap_load.start()
            wo_load.start()
        for n in range(0, q_width, 256):
            part = jnp.dot(h_buf[p], wq_buf[:, n:n + 256], preferred_element_type=jnp.float32) + bq_row[:, n:n + 256]
            for s in range(n_steps):
                for u in range(n_dev):
                    first = (s * n_dev + u) * part_seqs
                    q_buf[p, s, u, :, n:n + 256] = part[first:first + part_seqs].astype(q_buf.dtype)
        if p == 0:
            pl.semaphore_wait(barrier, n_dev - 1)
        for d in range(1, n_dev):
            q_copy(p, d).start()
        if p == 0:
            swap_load.wait()
            wo_swap.start()
        for b in range(p * part_seqs, (p + 1) * part_seqs):
            for copy in kv_load(b):
                copy.start()
        q_in[p, me] = q_buf[p, :, me]

    for copy in own_x_loads:
        copy.wait()
    for s in range(n_steps):
        own_h[s * n_seqs:(s + 1) * n_seqs, :] = norm(own_x[s].astype(jnp.float32))
    wkv_load.wait()
    fresh = jnp.dot(own_h[...], wkv_buf[...], preferred_element_type=jnp.float32) + bkv_ref[...].astype(jnp.float32).reshape(1, -1)
    fresh = fresh.astype(jnp.bfloat16).astype(jnp.float32)
    fk_ref[...] = jnp.zeros_like(fk_ref)
    fv_ref[...] = jnp.zeros_like(fv_ref)
    for s in range(n_steps):
        where = pl.ds(s, n_seqs, stride=FRESH_ROWS)
        fk_ref[where, :] = fresh[s * n_seqs:(s + 1) * n_seqs, :depth]
        fv_ref[where, :] = fresh[s * n_seqs:(s + 1) * n_seqs, depth:]

    def unpack(p):
        for d in range(1, n_dev):
            q_copy(p, d).wait_recv()
        for u in range(n_dev):
            for s in range(n_steps):
                for h in range(dev_heads):
                    first = ((u * n_steps + s) * dev_heads + h) * n_seqs + p * part_seqs
                    q_rows[first:first + part_seqs, :] = q_in[p, u, s, :, h * depth:(h + 1) * depth].astype(jnp.float32)

    shape = (rows, FRESH_ROWS)
    step_of_row = lax.broadcasted_iota(jnp.int32, shape, 0) // dev_heads % n_steps
    fresh_mask = lax.broadcasted_iota(jnp.int32, shape, 1) <= step_of_row

    def a_copy(p, d):
        return remote(a_src.at[p, chip_at(d)], a_buf.at[p, core, chip], a_send.at[p, d - 1], a_recv.at[p, d - 1], device(d))

    def a_forward(p, d):
        where = a_buf.at[p, core, chip_at(N_CHIPS - d)]
        return remote(a_src.at[p, chip] if d == 0 else where, where, f_send.at[p, d], f_recv.at[p, d], partner)

    low, high = pl.ds(0, quarter), pl.ds(quarter, quarter)

    def rs(p, s, i):
        def part(k, where):
            return p_buf.at[p, s, chip_at(k), :, where]
        src, dst, to = (
            (part(2, low), mid_buf.at[p, s, 0], right),
            (part(2, high), mid_buf.at[p, s, 1], left),
            (part(1, high), fin_buf.at[p, s, 0], right),
            (part(3, low), fin_buf.at[p, s, 1], left),
            (part(1, low), fin_buf.at[p, s, 2], right),
            (part(3, high), fin_buf.at[p, s, 3], left),
        )[i]
        return remote(src, dst, rs_send.at[p, s, i], rs_recv.at[p, s, i], to)

    def ag(p, s, i):
        k, begin, size, to = (
            (0, 0, half, right),
            (0, 0, half, left),
            (3, 0, quarter, right),
            (1, quarter, quarter, left),
            (0, 0, half, partner),
            (3, 0, half, partner),
            (1, 0, half, partner),
            (2, 0, quarter, partner),
            (2, quarter, quarter, partner),
        )[i]
        where = y_ref.at[s, chip_at(k), :, p, :, cols(core, begin, size)]
        return remote(where, where, ag_send.at[p, s, i], ag_recv.at[p, s, i], to)

    def pack(p):
        for t in range(N_CHIPS):
            for s in range(n_steps):
                pieces = []
                for h in range(chip_heads):
                    u = t * N_CORES + h // dev_heads
                    first = ((u * n_steps + s) * dev_heads + h % dev_heads) * n_seqs + p * part_seqs
                    pieces.append(head_buf[first:first + part_seqs, :])
                a_src[p, t, s] = jnp.concatenate(pieces, axis=1).astype(a_src.dtype)
        for d in (2, 1, 3):
            a_copy(p, d).start()
        a_forward(p, 0).start()
        a_buf[p, core, chip] = a_src[p, chip]

    def forward(p):
        for d in (1, 3, 2):
            a_copy(p, d).wait_recv()
            a_forward(p, d).start()

    def partial(p):
        for d in range(N_CHIPS):
            a_forward(p, d).wait_recv()
        if p == 0:
            wo_load.wait()
            wo_swap.wait_recv()
        for s in range(n_steps):
            for t in range(N_CHIPS):
                pair = jnp.concatenate([a_buf[p, c, t, s].astype(jnp.float32) for c in range(N_CORES)], axis=0)
                first = (s * N_CHIPS + t) * block
                lhs_buf[first:first + block, :] = pair.astype(lhs_buf.dtype)
        for n in range(0, half, 512):
            out = jnp.dot(lhs_buf[...], w_buf[:, n:n + 512], preferred_element_type=jnp.float32).astype(p_buf.dtype)
            for s in range(n_steps):
                for t in range(N_CHIPS):
                    first = (s * N_CHIPS + t) * block
                    p_buf[p, s, t, :, n:n + 512] = out[first:first + block]
        for pair in ((0, 1), (2, 3)):
            for s in range(n_steps):
                for i in pair:
                    rs(p, s, i).start()

    def add_into(target, other):
        target[...] = (target[...].astype(jnp.float32) + other[...].astype(jnp.float32)).astype(target.dtype)

    def middle(p, s):
        rs(p, s, 0).wait_recv()
        add_into(p_buf.at[p, s, chip_at(1), :, low], mid_buf.at[p, s, 0])
        rs(p, s, 4).start()
        rs(p, s, 1).wait_recv()
        add_into(p_buf.at[p, s, chip_at(3), :, high], mid_buf.at[p, s, 1])
        rs(p, s, 5).start()

    def finish(p, s):
        for i in (2, 3, 4, 5):
            rs(p, s, i).wait_recv()
        for begin, one, two in ((0, 1, 2), (quarter, 0, 3)):
            where = cols(core, begin, quarter)
            total = p_buf[p, s, chip, :, begin:begin + quarter].astype(jnp.float32)
            total = total + fin_buf[p, s, one].astype(jnp.float32)
            total = total + fin_buf[p, s, two].astype(jnp.float32)
            total = total + bo_buf[:, where]
            for c in range(N_CORES):
                x_part = x_buf[p, s, chip * N_CORES + c, :, where].astype(jnp.float32)
                y_ref[s, chip, c, p, :, where] = (x_part + total[c * part_seqs:(c + 1) * part_seqs]).astype(y_ref.dtype)
        for i in (0, 1, 4):
            ag(p, s, i).start()

    def relay(p, s):
        ag(p, s, 0).wait_recv()
        ag(p, s, 2).start()
        ag(p, s, 5).start()
        ag(p, s, 1).wait_recv()
        ag(p, s, 3).start()
        ag(p, s, 6).start()

    def last(p, s):
        ag(p, s, 2).wait_recv()
        ag(p, s, 7).start()
        ag(p, s, 3).wait_recv()
        ag(p, s, 8).start()

    def each(stage, p):
        for s in range(n_steps):
            stage(p, s)

    def query(b):
        return q_rows[pl.ds(b, rows, stride=n_seqs), :].astype(jnp.bfloat16)

    def attend(b, slot, after):
        new = pl.ds(pl.multiple_of(b * FRESH_ROWS, FRESH_ROWS), FRESH_ROWS)
        q_after = query(after)
        maxima = [None]

        def beside(start):
            maxima[0] = score_tile(q_after, k_buf.at[after], score_buf.at[1 - slot], start, len_ref[after], maxima[0])

        out = attend_one(query(b), v_buf.at[b], score_buf.at[slot], best_buf[slot],
                         fk_ref[new, :].astype(jnp.bfloat16), fv_ref[new, :].astype(jnp.bfloat16), fresh_mask, beside)
        best_buf[1 - slot] = maxima[0]
        head_buf[pl.ds(b, rows, stride=n_seqs), :] = out

    def wait_caches(b):
        for copy in kv_load(b):
            copy.wait()

    def attend_pair(i, carry):
        first = 2 * i
        after = jnp.minimum(first + 2, n_seqs - 1)
        wait_caches(first + 1)

        @pl.when(first + 2 < n_seqs)
        def _():
            wait_caches(after)

        attend(first, 0, first + 1)
        attend(first + 1, 1, after)

        @pl.when(i == part_seqs // 2 - 2)
        def _():
            unpack(1)

        @pl.when(i == part_seqs // 2 - 1)
        def _():
            pack(0)

        @pl.when(i == n_seqs // 2 - 2)
        def _():
            forward(0)

        return carry

    unpack(0)
    wait_caches(0)
    best = None
    for start in range(0, length, KEY_TILE):
        best = score_tile(query(0), k_buf.at[0], score_buf.at[0], start, len_ref[0], best)
    best_buf[0] = best
    lax.fori_loop(0, n_seqs // 2, attend_pair, 0)
    pack(1)
    partial(0)
    forward(1)
    each(middle, 0)
    partial(1)
    each(finish, 0)
    each(middle, 1)
    each(relay, 0)
    each(finish, 1)
    each(last, 0)
    each(relay, 1)
    each(last, 1)
    wo_swap.wait_send()
    for p in range(N_PARTS):
        for d in range(1, n_dev):
            q_copy(p, d).wait_send()
        for s in range(n_steps):
            for i in range(4, 9):
                ag(p, s, i).wait_recv()
            for i in range(9):
                ag(p, s, i).wait_send()
            for i in range(6):
                rs(p, s, i).wait_send()
        for d in (1, 2, 3):
            a_copy(p, d).wait_send()
        for d in range(N_CHIPS):
            a_forward(p, d).wait_send()


def store_kernel(n_steps, len_ref, fk_ref, fv_ref, y_ref, k_ref, v_ref, y_out, k_out, v_out, k_buf, v_buf, sems, y_sem):
    n_seqs, length, depth = k_buf.shape

    def store(b):
        return (pltpu.make_async_copy(k_buf.at[b], k_out.at[b], sems.at[0, b]),
                pltpu.make_async_copy(v_buf.at[b], v_out.at[b], sems.at[1, b]))

    def patch(b, buf, fresh):
        start = pl.multiple_of(jnp.minimum(len_ref[b] // 8 * 8, length - WINDOW), 8)
        offset = len_ref[b] - start
        row = lax.broadcasted_iota(jnp.int32, (WINDOW, depth), 0)
        window = buf[b, pl.ds(start, WINDOW), :].astype(jnp.float32)
        for s in range(n_steps):
            window = jnp.where(row == offset + s, fresh[b * FRESH_ROWS + s:b * FRESH_ROWS + s + 1, :], window)
        buf[b, pl.ds(start, WINDOW), :] = window.astype(buf.dtype)

    y_copy = pltpu.make_async_copy(y_ref, y_out, y_sem)
    y_copy.start()
    for b in range(n_seqs):
        patch(b, k_buf, fk_ref)
        patch(b, v_buf, fv_ref)
        for copy in store(b):
            copy.start()
    y_copy.wait()
    for b in range(n_seqs):
        for copy in store(b):
            copy.wait()


def solution(mesh):
    def local_block(x_steps, seq_lens, k_cache, v_cache, ln_gain, ln_bias, w_q, b_q, w_kv, b_kv, w_out, b_out):
        n_steps, _, width = x_steps.shape
        n_seqs, length, depth = k_cache.shape
        q_width = w_q.shape[1]
        n_dev = N_CHIPS * N_CORES
        part_seqs = n_seqs // N_PARTS
        rows = n_dev * n_steps * q_width // depth
        chip_width, half = N_CORES * q_width, width // 2
        block = N_CORES * part_seqs
        smem = pl.BlockSpec(memory_space=pltpu.SMEM)
        vmem = pl.BlockSpec(memory_space=pltpu.VMEM)
        hbm = pl.BlockSpec(memory_space=pl.ANY)
        dma = pltpu.SemaphoreType.DMA
        bf16, f32 = jnp.bfloat16, jnp.float32
        y_shape = (n_steps, N_CHIPS, N_CORES, N_PARTS, part_seqs, width)
        fresh_shape = (n_seqs * FRESH_ROWS, depth)
        y_vm, k_vm, v_vm, fresh_k, fresh_v = pl.pallas_call(
            block_kernel,
            out_shape=[pltpu.VMEM(y_shape, bf16), pltpu.VMEM(k_cache.shape, bf16), pltpu.VMEM(v_cache.shape, bf16), pltpu.VMEM(fresh_shape, f32), pltpu.VMEM(fresh_shape, f32)],
            in_specs=[hbm] * 12,
            out_specs=[vmem] * 5,
            scratch_shapes=[
                pltpu.SMEM(seq_lens.shape, jnp.int32),
                pltpu.VMEM(ln_gain.shape, bf16),
                pltpu.VMEM(ln_bias.shape, bf16),
                pltpu.VMEM(b_q.shape, bf16),
                pltpu.VMEM(b_kv.shape, bf16),
                pltpu.VMEM(b_out.shape, bf16),
                pltpu.VMEM((N_PARTS, n_steps, n_dev, part_seqs, width), bf16),
                pltpu.VMEM((n_steps, n_seqs, width), bf16),
                pltpu.VMEM((n_steps * n_seqs, width), bf16),
                pltpu.VMEM((N_PARTS, n_steps * n_dev * part_seqs, width), bf16),
                pltpu.VMEM((LN_ROWS, width), f32),
                pltpu.VMEM((LN_ROWS, width), f32),
                pltpu.VMEM((1, width), f32),
                pltpu.VMEM(w_q.shape, bf16),
                pltpu.VMEM(w_kv.shape, bf16),
                pltpu.VMEM((chip_width, half), bf16),
                pltpu.VMEM((q_width, half), bf16),
                pltpu.VMEM((N_PARTS, n_steps, n_dev, part_seqs, q_width), bf16),
                pltpu.VMEM((N_PARTS, n_dev, n_steps, part_seqs, q_width), bf16),
                pltpu.VMEM((rows * n_seqs, depth), f32),
                pltpu.VMEM((2, rows, length), f32),
                pltpu.VMEM((2, rows, LANES), f32),
                pltpu.VMEM((rows * n_seqs, depth), f32),
                pltpu.VMEM((N_PARTS, N_CHIPS, n_steps, part_seqs, chip_width), bf16),
                pltpu.VMEM((N_PARTS, N_CORES, N_CHIPS, n_steps, part_seqs, chip_width), bf16),
                pltpu.VMEM((n_steps * N_CHIPS * block, chip_width), bf16),
                pltpu.VMEM((N_PARTS, n_steps, N_CHIPS, block, half), bf16),
                pltpu.VMEM((N_PARTS, n_steps, 2, block, half // 2), bf16),
                pltpu.VMEM((N_PARTS, n_steps, 4, block, half // 2), bf16),
                dma((6,)), dma((2 * N_PARTS,)), dma((4,)), dma((2, n_seqs)), dma((2,)),
                dma((N_PARTS, n_dev - 1)), dma((N_PARTS, n_dev - 1)),
                dma((N_PARTS, 3)), dma((N_PARTS, 3)),
                dma((N_PARTS, N_CHIPS)), dma((N_PARTS, N_CHIPS)),
                dma((N_PARTS, n_steps, 6)), dma((N_PARTS, n_steps, 6)),
                dma((N_PARTS, n_steps, 9)), dma((N_PARTS, n_steps, 9)),
            ],
            compiler_params=pltpu.CompilerParams(vmem_limit_bytes=BLOCK_VMEM, collective_id=1, has_side_effects=True),
            cost_estimate=pl.CostEstimate(flops=4 * n_seqs * rows * length * depth, bytes_accessed=4 * n_seqs * length * depth, transcendentals=n_seqs * rows * length),
        )(seq_lens, ln_gain, ln_bias, b_q, b_kv, b_out,
          x_steps.reshape(n_steps, n_dev, N_PARTS, part_seqs, width), w_q, w_kv, w_out, k_cache, v_cache)
        y_steps, k_out, v_out, _, _ = pl.pallas_call(
            functools.partial(store_kernel, n_steps),
            out_shape=[jax.ShapeDtypeStruct(y_shape, bf16), jax.ShapeDtypeStruct(k_cache.shape, bf16), jax.ShapeDtypeStruct(v_cache.shape, bf16), pltpu.VMEM(k_cache.shape, bf16), pltpu.VMEM(v_cache.shape, bf16)],
            in_specs=[smem] + [vmem] * 5,
            out_specs=[hbm] * 3 + [vmem] * 2,
            scratch_shapes=[dma((2, n_seqs)), dma],
            input_output_aliases={4: 3, 5: 4},
            compiler_params=pltpu.CompilerParams(vmem_limit_bytes=2 * 1024 * 1024),
        )(seq_lens, fresh_k, fresh_v, y_vm, k_vm, v_vm)
        return y_steps.reshape(x_steps.shape), k_out, v_out

    row_spec = P(('dp', 'tp'), None, None)
    return jax.shard_map(
        local_block,
        mesh=mesh,
        in_specs=(P(None, 'dp', None), P(('dp', 'tp')), row_spec, row_spec, P(None), P(None), P(None, 'tp'), P('tp'), P(None, None), P(None), P('tp', None), P(None)),
        out_specs=(P(None, 'dp', None), row_spec, row_spec),
        check_vma=False,
    )
```

```python
import functools
import math

import jax
import jax.numpy as jnp
from jax import lax
from jax.experimental import pallas as pl
from jax.experimental.pallas import tpu as pltpu
from jax.sharding import PartitionSpec as P

LN_EPS = 1e-5
KEY_TILE = 256
LANES = 128
FRESH_ROWS = 16
WINDOW = 16
N_CHIPS = 4
N_CORES = 2
N_PARTS = 2
LN_ROWS = 16
MESH = pl.DeviceIdType.MESH
BLOCK_VMEM = 32 * 1024 * 1024


CONTRACT_LAST = (((1,), (1,)), ((), ()))


def score_tile(q_rows, k_ref, score_ref, start, seq_len, best):
    tile = lax.dot_general(q_rows, k_ref[start:start + KEY_TILE, :], CONTRACT_LAST, preferred_element_type=jnp.float32)
    lane = lax.broadcasted_iota(jnp.int32, tile.shape, 1)
    tile = jnp.where(lane < seq_len - start, tile, -jnp.inf)
    score_ref[:, start:start + KEY_TILE] = tile
    high = jnp.maximum(tile[:, :LANES], tile[:, LANES:])
    return high if best is None else jnp.maximum(best, high)


def attend_one(q_rows, v_ref, score_ref, best, fresh_k, fresh_v, fresh_mask, beside):
    length, depth = v_ref.shape
    to_log2 = depth ** -0.5 * math.log2(math.e)
    new_scores = lax.dot_general(q_rows, fresh_k, CONTRACT_LAST, preferred_element_type=jnp.float32)
    new_scores = jnp.where(fresh_mask, new_scores, -jnp.inf)
    top = jnp.maximum(jnp.max(best, axis=-1, keepdims=True), jnp.max(new_scores, axis=-1, keepdims=True))
    new_weights = jnp.exp2((new_scores - top) * to_log2)
    numerator = jnp.dot(new_weights.astype(jnp.bfloat16), fresh_v, preferred_element_type=jnp.float32)
    total, pieces = None, []
    for start in range(0, length, KEY_TILE):
        beside(start)
        weights = jnp.exp2((score_ref[:, start:start + KEY_TILE] - top) * to_log2)
        folded = weights[:, :LANES] + weights[:, LANES:]
        total = folded if total is None else total + folded
        pieces.append(weights.astype(jnp.bfloat16))
    numerator = numerator + jnp.dot(jnp.concatenate(pieces, axis=1), v_ref[...], preferred_element_type=jnp.float32)
    return numerator / (jnp.sum(total, axis=-1, keepdims=True) + jnp.sum(new_weights, axis=-1, keepdims=True))


def block_kernel(
        len_hbm, g_hbm, lb_hbm, bq_hbm, bkv_hbm, bo_hbm, x_hbm, wq_hbm, wkv_hbm, wo_hbm, k_hbm, v_hbm,
        y_ref, k_buf, v_buf, fk_ref, fv_ref,
        len_ref, g_ref, lb_ref, bq_ref, bkv_ref, bo_ref, x_buf, own_x, own_h, h_buf, gain_buf, bias_buf, bo_buf, wq_buf, wkv_buf, w_buf, swap_buf, q_buf, q_in, q_rows, score_buf, best_buf, head_buf, a_src, a_buf, lhs_buf, p_buf, mid_buf, fin_buf,
        vec_sems, x_sems, w_sems, kv_sems, swap_sems, q_send, q_recv, a_send, a_recv, f_send, f_recv, rs_send, rs_recv, ag_send, ag_recv):
    me = lax.axis_index('tp')
    n_dev = N_CHIPS * N_CORES
    chip, core = me // N_CORES, me % N_CORES
    n_steps, _, width = own_x.shape
    n_seqs, length, depth = k_buf.shape
    q_width = wq_buf.shape[1]
    dev_heads = q_width // depth
    chip_heads = N_CORES * dev_heads
    part_seqs = n_seqs // N_PARTS
    rows = n_dev * n_steps * dev_heads
    own_rows = wo_hbm.shape[0]
    half, quarter = width // 2, width // 4
    block = N_CORES * part_seqs

    def chip_at(k):
        return (chip + k) % N_CHIPS

    def device(k):
        return {'tp': chip_at(k) * N_CORES + core}

    def member(d):
        return (me + d) % n_dev

    right, left, partner = device(1), device(3), {'tp': chip * N_CORES + 1 - core}

    def remote(src, dst, send, recv, to):
        return pltpu.make_async_remote_copy(src_ref=src, dst_ref=dst, send_sem=send, recv_sem=recv, device_id=to, device_id_type=MESH)

    def cols(which, begin, size):
        return pl.ds(pl.multiple_of(which * half + begin, quarter), size)

    def x_load(p):
        return pltpu.make_async_copy(x_hbm.at[:, :, p], x_buf.at[p], x_sems.at[p])

    def kv_load(b):
        return (pltpu.make_async_copy(k_hbm.at[b], k_buf.at[b], kv_sems.at[0, b]),
                pltpu.make_async_copy(v_hbm.at[b], v_buf.at[b], kv_sems.at[1, b]))

    own_x_loads = [pltpu.make_async_copy(x_hbm.at[:, me, p], own_x.at[:, p * part_seqs:(p + 1) * part_seqs, :], x_sems.at[N_PARTS + p]) for p in range(N_PARTS)]
    own_w_rows = pl.ds(pl.multiple_of(core * own_rows, own_rows), own_rows)
    wq_load = pltpu.make_async_copy(wq_hbm, wq_buf, w_sems.at[0])
    wkv_load = pltpu.make_async_copy(wkv_hbm, wkv_buf, w_sems.at[1])
    wo_load = pltpu.make_async_copy(wo_hbm.at[:, cols(core, 0, half)], w_buf.at[own_w_rows, :], w_sems.at[2])
    swap_load = pltpu.make_async_copy(wo_hbm.at[:, cols(1 - core, 0, half)], swap_buf, w_sems.at[3])
    wo_swap = remote(swap_buf, w_buf.at[own_w_rows, :], swap_sems.at[0], swap_sems.at[1], partner)
    vector_loads = [pltpu.make_async_copy(src, dst, vec_sems.at[i]) for i, (src, dst) in enumerate(
        ((g_hbm, g_ref), (lb_hbm, lb_ref), (bq_hbm, bq_ref), (bkv_hbm, bkv_ref), (bo_hbm, bo_ref), (len_hbm, len_ref)))]
    for copy in vector_loads:
        copy.start()
    x_load(0).start()
    wq_load.start()

    barrier = pltpu.get_barrier_semaphore()
    for d in range(1, n_dev):
        pl.semaphore_signal(barrier, inc=1, device_id={'tp': member(d)}, device_id_type=MESH)

    for copy in vector_loads:
        copy.wait()

    bq_row = bq_ref[...].astype(jnp.float32).reshape(1, q_width)
    bo_buf[...] = bo_ref[...].astype(jnp.float32).reshape(1, width)
    gain_buf[...] = jnp.broadcast_to(g_ref[...].astype(jnp.float32).reshape(1, width), gain_buf.shape)
    bias_buf[...] = jnp.broadcast_to(lb_ref[...].astype(jnp.float32).reshape(1, width), bias_buf.shape)

    def norm(x_float):
        centered = x_float - jnp.mean(x_float, axis=-1, keepdims=True)
        row_var = jnp.mean(centered * centered, axis=-1, keepdims=True)
        scaled = centered * lax.rsqrt(row_var + LN_EPS)
        return (scaled * gain_buf[...] + bias_buf[...]).astype(h_buf.dtype)

    def q_copy(p, d):
        return remote(q_buf.at[p, :, member(d)], q_in.at[p, me], q_send.at[p, d - 1], q_recv.at[p, d - 1], {'tp': member(d)})

    group = LN_ROWS // part_seqs
    for p in range(N_PARTS):
        x_load(p).wait()
        if p == 0:
            for later in range(1, N_PARTS):
                x_load(later).start()
            for copy in own_x_loads:
                copy.start()
            wkv_load.start()

        for s in range(n_steps):
            def norm_rows(i, carry):
                x_float = jnp.concatenate([x_buf[p, s, i * group + j].astype(jnp.float32) for j in range(group)], axis=0)
                where = pl.ds(pl.multiple_of((s * n_dev // group + i) * LN_ROWS, LN_ROWS), LN_ROWS)
                h_buf[p, where, :] = norm(x_float)
                return carry

            lax.fori_loop(0, n_dev // group, norm_rows, 0)
        if p == 0:
            wq_load.wait()
            swap_load.start()
            wo_load.start()
        for n in range(0, q_width, 256):
            part = jnp.dot(h_buf[p], wq_buf[:, n:n + 256], preferred_element_type=jnp.float32) + bq_row[:, n:n + 256]
            for s in range(n_steps):
                for u in range(n_dev):
                    first = (s * n_dev + u) * part_seqs
                    q_buf[p, s, u, :, n:n + 256] = part[first:first + part_seqs].astype(q_buf.dtype)
        if p == 0:
            pl.semaphore_wait(barrier, n_dev - 1)
        for d in range(1, n_dev):
            q_copy(p, d).start()
        if p == 0:
            swap_load.wait()
            wo_swap.start()
        for b in range(p * part_seqs, (p + 1) * part_seqs):
            for copy in kv_load(b):
                copy.start()
        q_in[p, me] = q_buf[p, :, me]

    for copy in own_x_loads:
        copy.wait()
    for s in range(n_steps):
        own_h[s * n_seqs:(s + 1) * n_seqs, :] = norm(own_x[s].astype(jnp.float32))
    wkv_load.wait()
    fresh = jnp.dot(own_h[...], wkv_buf[...], preferred_element_type=jnp.float32) + bkv_ref[...].astype(jnp.float32).reshape(1, -1)
    fresh = fresh.astype(jnp.bfloat16).astype(jnp.float32)
    fk_ref[...] = jnp.zeros_like(fk_ref)
    fv_ref[...] = jnp.zeros_like(fv_ref)
    for s in range(n_steps):
        where = pl.ds(s, n_seqs, stride=FRESH_ROWS)
        fk_ref[where, :] = fresh[s * n_seqs:(s + 1) * n_seqs, :depth]
        fv_ref[where, :] = fresh[s * n_seqs:(s + 1) * n_seqs, depth:]

    def unpack(p):
        for d in range(1, n_dev):
            q_copy(p, d).wait_recv()
        for u in range(n_dev):
            for s in range(n_steps):
                for h in range(dev_heads):
                    first = ((u * n_steps + s) * dev_heads + h) * n_seqs + p * part_seqs
                    q_rows[first:first + part_seqs, :] = q_in[p, u, s, :, h * depth:(h + 1) * depth].astype(jnp.float32)

    shape = (rows, FRESH_ROWS)
    step_of_row = lax.broadcasted_iota(jnp.int32, shape, 0) // dev_heads % n_steps
    fresh_mask = lax.broadcasted_iota(jnp.int32, shape, 1) <= step_of_row

    def a_copy(p, d):
        return remote(a_src.at[p, chip_at(d)], a_buf.at[p, core, chip], a_send.at[p, d - 1], a_recv.at[p, d - 1], device(d))

    def a_forward(p, d):
        where = a_buf.at[p, core, chip_at(N_CHIPS - d)]
        return remote(a_src.at[p, chip] if d == 0 else where, where, f_send.at[p, d], f_recv.at[p, d], partner)

    low, high = pl.ds(0, quarter), pl.ds(quarter, quarter)

    def rs(p, s, i):
        def part(k, where):
            return p_buf.at[p, s, chip_at(k), :, where]
        src, dst, to = (
            (part(2, low), mid_buf.at[p, s, 0], right),
            (part(2, high), mid_buf.at[p, s, 1], left),
            (part(1, high), fin_buf.at[p, s, 0], right),
            (part(3, low), fin_buf.at[p, s, 1], left),
            (part(1, low), fin_buf.at[p, s, 2], right),
            (part(3, high), fin_buf.at[p, s, 3], left),
        )[i]
        return remote(src, dst, rs_send.at[p, s, i], rs_recv.at[p, s, i], to)

    def ag(p, s, i):
        k, begin, size, to = (
            (0, 0, half, right),
            (0, 0, half, left),
            (3, 0, quarter, right),
            (1, quarter, quarter, left),
            (0, 0, half, partner),
            (3, 0, half, partner),
            (1, 0, half, partner),
            (2, 0, quarter, partner),
            (2, quarter, quarter, partner),
        )[i]
        where = y_ref.at[s, chip_at(k), :, p, :, cols(core, begin, size)]
        return remote(where, where, ag_send.at[p, s, i], ag_recv.at[p, s, i], to)

    def pack(p):
        for t in range(N_CHIPS):
            for s in range(n_steps):
                pieces = []
                for h in range(chip_heads):
                    u = t * N_CORES + h // dev_heads
                    first = ((u * n_steps + s) * dev_heads + h % dev_heads) * n_seqs + p * part_seqs
                    pieces.append(head_buf[first:first + part_seqs, :])
                a_src[p, t, s] = jnp.concatenate(pieces, axis=1).astype(a_src.dtype)
        for d in (2, 1, 3):
            a_copy(p, d).start()
        a_forward(p, 0).start()
        a_buf[p, core, chip] = a_src[p, chip]

    def forward(p):
        for d in (1, 3, 2):
            a_copy(p, d).wait_recv()
            a_forward(p, d).start()

    def partial(p):
        for d in range(N_CHIPS):
            a_forward(p, d).wait_recv()
        if p == 0:
            wo_load.wait()
            wo_swap.wait_recv()
        for s in range(n_steps):
            for t in range(N_CHIPS):
                pair = jnp.concatenate([a_buf[p, c, t, s].astype(jnp.float32) for c in range(N_CORES)], axis=0)
                first = (s * N_CHIPS + t) * block
                lhs_buf[first:first + block, :] = pair.astype(lhs_buf.dtype)
        for n in range(0, half, 512):
            out = jnp.dot(lhs_buf[...], w_buf[:, n:n + 512], preferred_element_type=jnp.float32).astype(p_buf.dtype)
            for s in range(n_steps):
                for t in range(N_CHIPS):
                    first = (s * N_CHIPS + t) * block
                    p_buf[p, s, t, :, n:n + 512] = out[first:first + block]
        for pair in ((0, 1), (2, 3)):
            for s in range(n_steps):
                for i in pair:
                    rs(p, s, i).start()

    def add_into(target, other):
        target[...] = (target[...].astype(jnp.float32) + other[...].astype(jnp.float32)).astype(target.dtype)

    def middle(p, s):
        rs(p, s, 0).wait_recv()
        add_into(p_buf.at[p, s, chip_at(1), :, low], mid_buf.at[p, s, 0])
        rs(p, s, 4).start()
        rs(p, s, 1).wait_recv()
        add_into(p_buf.at[p, s, chip_at(3), :, high], mid_buf.at[p, s, 1])
        rs(p, s, 5).start()

    def finish(p, s):
        for i in (2, 3, 4, 5):
            rs(p, s, i).wait_recv()
        for begin, one, two in ((0, 1, 2), (quarter, 0, 3)):
            where = cols(core, begin, quarter)
            total = p_buf[p, s, chip, :, begin:begin + quarter].astype(jnp.float32)
            total = total + fin_buf[p, s, one].astype(jnp.float32)
            total = total + fin_buf[p, s, two].astype(jnp.float32)
            total = total + bo_buf[:, where]
            for c in range(N_CORES):
                x_part = x_buf[p, s, chip * N_CORES + c, :, where].astype(jnp.float32)
                y_ref[s, chip, c, p, :, where] = (x_part + total[c * part_seqs:(c + 1) * part_seqs]).astype(y_ref.dtype)
        for i in (0, 1, 4):
            ag(p, s, i).start()

    def relay(p, s):
        ag(p, s, 0).wait_recv()
        ag(p, s, 2).start()
        ag(p, s, 5).start()
        ag(p, s, 1).wait_recv()
        ag(p, s, 3).start()
        ag(p, s, 6).start()

    def last(p, s):
        ag(p, s, 2).wait_recv()
        ag(p, s, 7).start()
        ag(p, s, 3).wait_recv()
        ag(p, s, 8).start()

    def each(stage, p):
        for s in range(n_steps):
            stage(p, s)

    def query(b):
        return q_rows[pl.ds(b, rows, stride=n_seqs), :].astype(jnp.bfloat16)

    def attend(b, slot, after):
        new = pl.ds(pl.multiple_of(b * FRESH_ROWS, FRESH_ROWS), FRESH_ROWS)
        q_after = query(after)
        maxima = [None]

        def beside(start):
            maxima[0] = score_tile(q_after, k_buf.at[after], score_buf.at[1 - slot], start, len_ref[after], maxima[0])

        out = attend_one(query(b), v_buf.at[b], score_buf.at[slot], best_buf[slot],
                         fk_ref[new, :].astype(jnp.bfloat16), fv_ref[new, :].astype(jnp.bfloat16), fresh_mask, beside)
        best_buf[1 - slot] = maxima[0]
        head_buf[pl.ds(b, rows, stride=n_seqs), :] = out

    def wait_caches(b):
        for copy in kv_load(b):
            copy.wait()

    def attend_pair(i, carry):
        first = 2 * i
        after = jnp.minimum(first + 2, n_seqs - 1)
        wait_caches(first + 1)

        @pl.when(first + 2 < n_seqs)
        def _():
            wait_caches(after)

        attend(first, 0, first + 1)
        attend(first + 1, 1, after)

        @pl.when(i == part_seqs // 2 - 2)
        def _():
            unpack(1)

        @pl.when(i == part_seqs // 2 - 1)
        def _():
            pack(0)

        @pl.when(i == n_seqs // 2 - 2)
        def _():
            forward(0)

        return carry

    unpack(0)
    wait_caches(0)
    best = None
    for start in range(0, length, KEY_TILE):
        best = score_tile(query(0), k_buf.at[0], score_buf.at[0], start, len_ref[0], best)
    best_buf[0] = best
    lax.fori_loop(0, n_seqs // 2, attend_pair, 0)
    pack(1)
    partial(0)
    forward(1)
    each(middle, 0)
    partial(1)
    each(finish, 0)
    each(middle, 1)
    each(relay, 0)
    each(finish, 1)
    each(last, 0)
    each(relay, 1)
    each(last, 1)
    wo_swap.wait_send()
    for p in range(N_PARTS):
        for d in range(1, n_dev):
            q_copy(p, d).wait_send()
        for s in range(n_steps):
            for i in range(4, 9):
                ag(p, s, i).wait_recv()
            for i in range(9):
                ag(p, s, i).wait_send()
            for i in range(6):
                rs(p, s, i).wait_send()
        for d in (1, 2, 3):
            a_copy(p, d).wait_send()
        for d in range(N_CHIPS):
            a_forward(p, d).wait_send()


def store_kernel(n_steps, len_ref, fk_ref, fv_ref, y_ref, k_ref, v_ref, y_out, k_out, v_out, k_buf, v_buf, sems, y_sem):
    n_seqs, length, depth = k_buf.shape

    def store(b):
        return (pltpu.make_async_copy(k_buf.at[b], k_out.at[b], sems.at[0, b]),
                pltpu.make_async_copy(v_buf.at[b], v_out.at[b], sems.at[1, b]))

    def patch(b, buf, fresh):
        start = pl.multiple_of(jnp.minimum(len_ref[b] // 8 * 8, length - WINDOW), 8)
        offset = len_ref[b] - start
        row = lax.broadcasted_iota(jnp.int32, (WINDOW, depth), 0)
        window = buf[b, pl.ds(start, WINDOW), :].astype(jnp.float32)
        for s in range(n_steps):
            window = jnp.where(row == offset + s, fresh[b * FRESH_ROWS + s:b * FRESH_ROWS + s + 1, :], window)
        buf[b, pl.ds(start, WINDOW), :] = window.astype(buf.dtype)

    y_copy = pltpu.make_async_copy(y_ref, y_out, y_sem)
    y_copy.start()
    for b in range(n_seqs):
        patch(b, k_buf, fk_ref)
        patch(b, v_buf, fv_ref)
        for copy in store(b):
            copy.start()
    y_copy.wait()
    for b in range(n_seqs):
        for copy in store(b):
            copy.wait()


def solution(mesh):
    def local_block(x_steps, seq_lens, k_cache, v_cache, ln_gain, ln_bias, w_q, b_q, w_kv, b_kv, w_out, b_out):
        n_steps, _, width = x_steps.shape
        n_seqs, length, depth = k_cache.shape
        q_width = w_q.shape[1]
        n_dev = N_CHIPS * N_CORES
        part_seqs = n_seqs // N_PARTS
        rows = n_dev * n_steps * q_width // depth
        chip_width, half = N_CORES * q_width, width // 2
        block = N_CORES * part_seqs
        smem = pl.BlockSpec(memory_space=pltpu.SMEM)
        vmem = pl.BlockSpec(memory_space=pltpu.VMEM)
        hbm = pl.BlockSpec(memory_space=pl.ANY)
        dma = pltpu.SemaphoreType.DMA
        bf16, f32 = jnp.bfloat16, jnp.float32
        y_shape = (n_steps, N_CHIPS, N_CORES, N_PARTS, part_seqs, width)
        fresh_shape = (n_seqs * FRESH_ROWS, depth)
        y_vm, k_vm, v_vm, fresh_k, fresh_v = pl.pallas_call(
            block_kernel,
            out_shape=[pltpu.VMEM(y_shape, bf16), pltpu.VMEM(k_cache.shape, bf16), pltpu.VMEM(v_cache.shape, bf16), pltpu.VMEM(fresh_shape, f32), pltpu.VMEM(fresh_shape, f32)],
            in_specs=[hbm] * 12,
            out_specs=[vmem] * 5,
            scratch_shapes=[
                pltpu.SMEM(seq_lens.shape, jnp.int32),
                pltpu.VMEM(ln_gain.shape, bf16),
                pltpu.VMEM(ln_bias.shape, bf16),
                pltpu.VMEM(b_q.shape, bf16),
                pltpu.VMEM(b_kv.shape, bf16),
                pltpu.VMEM(b_out.shape, bf16),
                pltpu.VMEM((N_PARTS, n_steps, n_dev, part_seqs, width), bf16),
                pltpu.VMEM((n_steps, n_seqs, width), bf16),
                pltpu.VMEM((n_steps * n_seqs, width), bf16),
                pltpu.VMEM((N_PARTS, n_steps * n_dev * part_seqs, width), bf16),
                pltpu.VMEM((LN_ROWS, width), f32),
                pltpu.VMEM((LN_ROWS, width), f32),
                pltpu.VMEM((1, width), f32),
                pltpu.VMEM(w_q.shape, bf16),
                pltpu.VMEM(w_kv.shape, bf16),
                pltpu.VMEM((chip_width, half), bf16),
                pltpu.VMEM((q_width, half), bf16),
                pltpu.VMEM((N_PARTS, n_steps, n_dev, part_seqs, q_width), bf16),
                pltpu.VMEM((N_PARTS, n_dev, n_steps, part_seqs, q_width), bf16),
                pltpu.VMEM((rows * n_seqs, depth), f32),
                pltpu.VMEM((2, rows, length), f32),
                pltpu.VMEM((2, rows, LANES), f32),
                pltpu.VMEM((rows * n_seqs, depth), f32),
                pltpu.VMEM((N_PARTS, N_CHIPS, n_steps, part_seqs, chip_width), bf16),
                pltpu.VMEM((N_PARTS, N_CORES, N_CHIPS, n_steps, part_seqs, chip_width), bf16),
                pltpu.VMEM((n_steps * N_CHIPS * block, chip_width), bf16),
                pltpu.VMEM((N_PARTS, n_steps, N_CHIPS, block, half), bf16),
                pltpu.VMEM((N_PARTS, n_steps, 2, block, half // 2), bf16),
                pltpu.VMEM((N_PARTS, n_steps, 4, block, half // 2), bf16),
                dma((6,)), dma((2 * N_PARTS,)), dma((4,)), dma((2, n_seqs)), dma((2,)),
                dma((N_PARTS, n_dev - 1)), dma((N_PARTS, n_dev - 1)),
                dma((N_PARTS, 3)), dma((N_PARTS, 3)),
                dma((N_PARTS, N_CHIPS)), dma((N_PARTS, N_CHIPS)),
                dma((N_PARTS, n_steps, 6)), dma((N_PARTS, n_steps, 6)),
                dma((N_PARTS, n_steps, 9)), dma((N_PARTS, n_steps, 9)),
            ],
            compiler_params=pltpu.CompilerParams(vmem_limit_bytes=BLOCK_VMEM, collective_id=1, has_side_effects=True),
            cost_estimate=pl.CostEstimate(flops=4 * n_seqs * rows * length * depth, bytes_accessed=4 * n_seqs * length * depth, transcendentals=n_seqs * rows * length),
        )(seq_lens, ln_gain, ln_bias, b_q, b_kv, b_out,
          x_steps.reshape(n_steps, n_dev, N_PARTS, part_seqs, width), w_q, w_kv, w_out, k_cache, v_cache)
        y_steps, k_out, v_out, _, _ = pl.pallas_call(
            functools.partial(store_kernel, n_steps),
            out_shape=[jax.ShapeDtypeStruct(y_shape, bf16), jax.ShapeDtypeStruct(k_cache.shape, bf16), jax.ShapeDtypeStruct(v_cache.shape, bf16), pltpu.VMEM(k_cache.shape, bf16), pltpu.VMEM(v_cache.shape, bf16)],
            in_specs=[smem] + [vmem] * 5,
            out_specs=[hbm] * 3 + [vmem] * 2,
            scratch_shapes=[dma((2, n_seqs)), dma],
            input_output_aliases={4: 3, 5: 4},
            compiler_params=pltpu.CompilerParams(vmem_limit_bytes=2 * 1024 * 1024),
        )(seq_lens, fresh_k, fresh_v, y_vm, k_vm, v_vm)
        return y_steps.reshape(x_steps.shape), k_out, v_out

    row_spec = P(('dp', 'tp'), None, None)
    return jax.shard_map(
        local_block,
        mesh=mesh,
        in_specs=(P(None, 'dp', None), P(('dp', 'tp')), row_spec, row_spec, P(None), P(None), P(None, 'tp'), P('tp'), P(None, None), P(None), P('tp', None), P(None)),
        out_specs=(P(None, 'dp', None), row_spec, row_spec),
        check_vma=False,
    )
```

```python
import functools
import math

import jax
import jax.numpy as jnp
from jax import lax
from jax.experimental import pallas as pl
from jax.experimental.pallas import tpu as pltpu
from jax.sharding import PartitionSpec as P

LN_EPS = 1e-5
KEY_TILE = 256
LANES = 128
Q_TILE = 256
FRESH_ROWS = 16
WINDOW = 16
N_CHIPS = 4
N_CORES = 2
N_PARTS = 2
LN_ROWS = 16
MESH = pl.DeviceIdType.MESH
BLOCK_VMEM = 32 * 1024 * 1024


CONTRACT_LAST = (((1,), (1,)), ((), ()))


def score_tile(q_rows, k_ref, score_ref, start, seq_len, best):
    tile = lax.dot_general(q_rows, k_ref[start:start + KEY_TILE, :], CONTRACT_LAST, preferred_element_type=jnp.float32)
    lane = lax.broadcasted_iota(jnp.int32, tile.shape, 1)
    tile = jnp.where(lane < seq_len - start, tile, -jnp.inf)
    score_ref[:, start:start + KEY_TILE] = tile
    high = jnp.maximum(tile[:, :LANES], tile[:, LANES:])
    return high if best is None else jnp.maximum(best, high)


def attend_one(q_rows, v_ref, score_ref, best, fresh_k, fresh_v, fresh_mask, beside):
    length, depth = v_ref.shape
    to_log2 = depth ** -0.5 * math.log2(math.e)
    new_scores = lax.dot_general(q_rows, fresh_k, CONTRACT_LAST, preferred_element_type=jnp.float32)
    new_scores = jnp.where(fresh_mask, new_scores, -jnp.inf)
    top = jnp.maximum(jnp.max(best, axis=-1, keepdims=True), jnp.max(new_scores, axis=-1, keepdims=True))
    new_weights = jnp.exp2((new_scores - top) * to_log2)
    numerator = jnp.dot(new_weights.astype(jnp.bfloat16), fresh_v, preferred_element_type=jnp.float32)
    total, pieces = None, []
    for start in range(0, length, KEY_TILE):
        beside(start)
        weights = jnp.exp2((score_ref[:, start:start + KEY_TILE] - top) * to_log2)
        folded = weights[:, :LANES] + weights[:, LANES:]
        total = folded if total is None else total + folded
        pieces.append(weights.astype(jnp.bfloat16))
    numerator = numerator + jnp.dot(jnp.concatenate(pieces, axis=1), v_ref[...], preferred_element_type=jnp.float32)
    return numerator / (jnp.sum(total, axis=-1, keepdims=True) + jnp.sum(new_weights, axis=-1, keepdims=True))


def block_kernel(
        len_hbm, g_hbm, lb_hbm, bq_hbm, bkv_hbm, bo_hbm, x_hbm, wq_hbm, wkv_hbm, wo_hbm, k_hbm, v_hbm,
        y_ref, k_buf, v_buf, fk_ref, fv_ref,
        len_ref, g_ref, lb_ref, bq_ref, bkv_ref, bo_ref, x_buf, own_x, own_h, h_buf, gain_buf, bias_buf, bo_buf, wq_buf, wkv_buf, w_buf, swap_buf, q_buf, q_in, q_rows, score_buf, best_buf, head_buf, a_src, a_buf, lhs_buf, p_buf, mid_buf, fin_buf,
        vec_sems, x_sems, w_sems, kv_sems, swap_sems, q_send, q_recv, a_send, a_recv, f_send, f_recv, rs_send, rs_recv, ag_send, ag_recv):
    me = lax.axis_index('tp')
    n_dev = N_CHIPS * N_CORES
    chip, core = me // N_CORES, me % N_CORES
    n_steps, _, width = own_x.shape
    n_seqs, length, depth = k_buf.shape
    q_width = wq_buf.shape[1]
    dev_heads = q_width // depth
    chip_heads = N_CORES * dev_heads
    part_seqs = n_seqs // N_PARTS
    rows = n_dev * n_steps * dev_heads
    own_rows = wo_hbm.shape[0]
    half, quarter = width // 2, width // 4
    block = N_CORES * part_seqs

    def chip_at(k):
        return (chip + k) % N_CHIPS

    def device(k):
        return {'tp': chip_at(k) * N_CORES + core}

    def member(d):
        return (me + d) % n_dev

    right, left, partner = device(1), device(3), {'tp': chip * N_CORES + 1 - core}

    def remote(src, dst, send, recv, to):
        return pltpu.make_async_remote_copy(src_ref=src, dst_ref=dst, send_sem=send, recv_sem=recv, device_id=to, device_id_type=MESH)

    def cols(which, begin, size):
        return pl.ds(pl.multiple_of(which * half + begin, quarter), size)

    def x_load(p):
        return pltpu.make_async_copy(x_hbm.at[:, :, p], x_buf.at[p], x_sems.at[p])

    def kv_load(b):
        return (pltpu.make_async_copy(k_hbm.at[b], k_buf.at[b], kv_sems.at[0, b]),
                pltpu.make_async_copy(v_hbm.at[b], v_buf.at[b], kv_sems.at[1, b]))

    own_x_loads = [pltpu.make_async_copy(x_hbm.at[:, me, p], own_x.at[:, p * part_seqs:(p + 1) * part_seqs, :], x_sems.at[N_PARTS + p]) for p in range(N_PARTS)]
    own_w_rows = pl.ds(pl.multiple_of(core * own_rows, own_rows), own_rows)
    wq_load = pltpu.make_async_copy(wq_hbm, wq_buf, w_sems.at[0])
    wkv_load = pltpu.make_async_copy(wkv_hbm, wkv_buf, w_sems.at[1])
    wo_load = pltpu.make_async_copy(wo_hbm.at[:, cols(core, 0, half)], w_buf.at[own_w_rows, :], w_sems.at[2])
    swap_load = pltpu.make_async_copy(wo_hbm.at[:, cols(1 - core, 0, half)], swap_buf, w_sems.at[3])
    wo_swap = remote(swap_buf, w_buf.at[own_w_rows, :], swap_sems.at[0], swap_sems.at[1], partner)
    vector_loads = [pltpu.make_async_copy(src, dst, vec_sems.at[i]) for i, (src, dst) in enumerate(
        ((g_hbm, g_ref), (lb_hbm, lb_ref), (bq_hbm, bq_ref), (bkv_hbm, bkv_ref), (bo_hbm, bo_ref), (len_hbm, len_ref)))]
    for copy in vector_loads:
        copy.start()
    x_load(0).start()
    wq_load.start()

    barrier = pltpu.get_barrier_semaphore()
    for d in range(1, n_dev):
        pl.semaphore_signal(barrier, inc=1, device_id={'tp': member(d)}, device_id_type=MESH)

    for copy in vector_loads:
        copy.wait()

    bq_row = bq_ref[...].astype(jnp.float32).reshape(1, q_width)
    bo_buf[...] = bo_ref[...].astype(jnp.float32).reshape(1, width)
    gain_buf[...] = jnp.broadcast_to(g_ref[...].astype(jnp.float32).reshape(1, width), gain_buf.shape)
    bias_buf[...] = jnp.broadcast_to(lb_ref[...].astype(jnp.float32).reshape(1, width), bias_buf.shape)

    def norm(x_float):
        centered = x_float - jnp.mean(x_float, axis=-1, keepdims=True)
        row_var = jnp.mean(centered * centered, axis=-1, keepdims=True)
        scaled = centered * lax.rsqrt(row_var + LN_EPS)
        return (scaled * gain_buf[...] + bias_buf[...]).astype(h_buf.dtype)

    def q_copy(p, n, d):
        where = pl.ds(n * Q_TILE, Q_TILE)
        return remote(q_buf.at[p, :, member(d), :, where], q_in.at[p, me, :, :, where], q_send.at[p, n, d - 1], q_recv.at[p, n, d - 1], {'tp': member(d)})

    group = LN_ROWS // part_seqs
    for p in range(N_PARTS):
        x_load(p).wait()
        if p == 0:
            for later in range(1, N_PARTS):
                x_load(later).start()
            for copy in own_x_loads:
                copy.start()
            wkv_load.start()

        for s in range(n_steps):
            def norm_rows(i, carry):
                x_float = jnp.concatenate([x_buf[p, s, i * group + j].astype(jnp.float32) for j in range(group)], axis=0)
                where = pl.ds(pl.multiple_of((s * n_dev // group + i) * LN_ROWS, LN_ROWS), LN_ROWS)
                h_buf[p, where, :] = norm(x_float)
                return carry

            lax.fori_loop(0, n_dev // group, norm_rows, 0)
        if p == 0:
            wq_load.wait()
            swap_load.start()
            wo_load.start()
        for n in range(q_width // Q_TILE):
            where = slice(n * Q_TILE, (n + 1) * Q_TILE)
            part = jnp.dot(h_buf[p], wq_buf[:, where], preferred_element_type=jnp.float32) + bq_row[:, where]
            for s in range(n_steps):
                for u in range(n_dev):
                    first = (s * n_dev + u) * part_seqs
                    q_buf[p, s, u, :, where] = part[first:first + part_seqs].astype(q_buf.dtype)
            if p == 0 and n == 0:
                pl.semaphore_wait(barrier, n_dev - 1)
            for d in range(1, n_dev):
                q_copy(p, n, d).start()
        if p == 0:
            swap_load.wait()
            wo_swap.start()
        for b in range(p * part_seqs, (p + 1) * part_seqs):
            for copy in kv_load(b):
                copy.start()
        q_in[p, me] = q_buf[p, :, me]

    for copy in own_x_loads:
        copy.wait()
    for s in range(n_steps):
        own_h[s * n_seqs:(s + 1) * n_seqs, :] = norm(own_x[s].astype(jnp.float32))
    wkv_load.wait()
    fresh = jnp.dot(own_h[...], wkv_buf[...], preferred_element_type=jnp.float32) + bkv_ref[...].astype(jnp.float32).reshape(1, -1)
    fresh = fresh.astype(jnp.bfloat16).astype(jnp.float32)
    fk_ref[...] = jnp.zeros_like(fk_ref)
    fv_ref[...] = jnp.zeros_like(fv_ref)
    for s in range(n_steps):
        where = pl.ds(s, n_seqs, stride=FRESH_ROWS)
        fk_ref[where, :] = fresh[s * n_seqs:(s + 1) * n_seqs, :depth]
        fv_ref[where, :] = fresh[s * n_seqs:(s + 1) * n_seqs, depth:]

    def unpack(p):
        for n in range(q_width // Q_TILE):
            for d in range(1, n_dev):
                q_copy(p, n, d).wait_recv()
        for u in range(n_dev):
            for s in range(n_steps):
                for h in range(dev_heads):
                    first = ((u * n_steps + s) * dev_heads + h) * n_seqs + p * part_seqs
                    q_rows[first:first + part_seqs, :] = q_in[p, u, s, :, h * depth:(h + 1) * depth].astype(jnp.float32)

    shape = (rows, FRESH_ROWS)
    step_of_row = lax.broadcasted_iota(jnp.int32, shape, 0) // dev_heads % n_steps
    fresh_mask = lax.broadcasted_iota(jnp.int32, shape, 1) <= step_of_row

    def a_copy(p, d):
        return remote(a_src.at[p, chip_at(d)], a_buf.at[p, core, chip], a_send.at[p, d - 1], a_recv.at[p, d - 1], device(d))

    def a_forward(p, d):
        where = a_buf.at[p, core, chip_at(N_CHIPS - d)]
        return remote(a_src.at[p, chip] if d == 0 else where, where, f_send.at[p, d], f_recv.at[p, d], partner)

    low, high = pl.ds(0, quarter), pl.ds(quarter, quarter)

    def rs(p, s, i):
        def part(k, where):
            return p_buf.at[p, s, chip_at(k), :, where]
        src, dst, to = (
            (part(2, low), mid_buf.at[p, s, 0], right),
            (part(2, high), mid_buf.at[p, s, 1], left),
            (part(1, high), fin_buf.at[p, s, 0], right),
            (part(3, low), fin_buf.at[p, s, 1], left),
            (part(1, low), fin_buf.at[p, s, 2], right),
            (part(3, high), fin_buf.at[p, s, 3], left),
        )[i]
        return remote(src, dst, rs_send.at[p, s, i], rs_recv.at[p, s, i], to)

    def ag(p, s, i):
        k, begin, size, to = (
            (0, 0, half, right),
            (0, 0, half, left),
            (3, 0, quarter, right),
            (1, quarter, quarter, left),
            (0, 0, half, partner),
            (3, 0, half, partner),
            (1, 0, half, partner),
            (2, 0, quarter, partner),
            (2, quarter, quarter, partner),
        )[i]
        where = y_ref.at[s, chip_at(k), :, p, :, cols(core, begin, size)]
        return remote(where, where, ag_send.at[p, s, i], ag_recv.at[p, s, i], to)

    def pack(p):
        for t in range(N_CHIPS):
            for s in range(n_steps):
                pieces = []
                for h in range(chip_heads):
                    u = t * N_CORES + h // dev_heads
                    first = ((u * n_steps + s) * dev_heads + h % dev_heads) * n_seqs + p * part_seqs
                    pieces.append(head_buf[first:first + part_seqs, :])
                a_src[p, t, s] = jnp.concatenate(pieces, axis=1).astype(a_src.dtype)
        for d in (2, 1, 3):
            a_copy(p, d).start()
        a_forward(p, 0).start()
        a_buf[p, core, chip] = a_src[p, chip]

    def forward(p):
        for d in (1, 3, 2):
            a_copy(p, d).wait_recv()
            a_forward(p, d).start()

    def partial(p):
        for d in range(N_CHIPS):
            a_forward(p, d).wait_recv()
        if p == 0:
            wo_load.wait()
            wo_swap.wait_recv()
        for s in range(n_steps):
            for t in range(N_CHIPS):
                pair = jnp.concatenate([a_buf[p, c, t, s].astype(jnp.float32) for c in range(N_CORES)], axis=0)
                first = (s * N_CHIPS + t) * block
                lhs_buf[first:first + block, :] = pair.astype(lhs_buf.dtype)
        for n in range(0, half, 512):
            out = jnp.dot(lhs_buf[...], w_buf[:, n:n + 512], preferred_element_type=jnp.float32).astype(p_buf.dtype)
            for s in range(n_steps):
                for t in range(N_CHIPS):
                    first = (s * N_CHIPS + t) * block
                    p_buf[p, s, t, :, n:n + 512] = out[first:first + block]
        for pair in ((0, 1), (2, 3)):
            for s in range(n_steps):
                for i in pair:
                    rs(p, s, i).start()

    def add_into(target, other):
        target[...] = (target[...].astype(jnp.float32) + other[...].astype(jnp.float32)).astype(target.dtype)

    def middle(p, s):
        rs(p, s, 0).wait_recv()
        add_into(p_buf.at[p, s, chip_at(1), :, low], mid_buf.at[p, s, 0])
        rs(p, s, 4).start()
        rs(p, s, 1).wait_recv()
        add_into(p_buf.at[p, s, chip_at(3), :, high], mid_buf.at[p, s, 1])
        rs(p, s, 5).start()

    def finish(p, s):
        for i in (2, 3, 4, 5):
            rs(p, s, i).wait_recv()
        for begin, one, two in ((0, 1, 2), (quarter, 0, 3)):
            where = cols(core, begin, quarter)
            total = p_buf[p, s, chip, :, begin:begin + quarter].astype(jnp.float32)
            total = total + fin_buf[p, s, one].astype(jnp.float32)
            total = total + fin_buf[p, s, two].astype(jnp.float32)
            total = total + bo_buf[:, where]
            for c in range(N_CORES):
                x_part = x_buf[p, s, chip * N_CORES + c, :, where].astype(jnp.float32)
                y_ref[s, chip, c, p, :, where] = (x_part + total[c * part_seqs:(c + 1) * part_seqs]).astype(y_ref.dtype)
        for i in (0, 1, 4):
            ag(p, s, i).start()

    def relay(p, s):
        ag(p, s, 0).wait_recv()
        ag(p, s, 2).start()
        ag(p, s, 5).start()
        ag(p, s, 1).wait_recv()
        ag(p, s, 3).start()
        ag(p, s, 6).start()

    def last(p, s):
        ag(p, s, 2).wait_recv()
        ag(p, s, 7).start()
        ag(p, s, 3).wait_recv()
        ag(p, s, 8).start()

    def each(stage, p):
        for s in range(n_steps):
            stage(p, s)

    def query(b):
        return q_rows[pl.ds(b, rows, stride=n_seqs), :].astype(jnp.bfloat16)

    def attend(b, slot, after):
        new = pl.ds(pl.multiple_of(b * FRESH_ROWS, FRESH_ROWS), FRESH_ROWS)
        q_after = query(after)
        maxima = [None]

        def beside(start):
            maxima[0] = score_tile(q_after, k_buf.at[after], score_buf.at[1 - slot], start, len_ref[after], maxima[0])

        out = attend_one(query(b), v_buf.at[b], score_buf.at[slot], best_buf[slot],
                         fk_ref[new, :].astype(jnp.bfloat16), fv_ref[new, :].astype(jnp.bfloat16), fresh_mask, beside)
        best_buf[1 - slot] = maxima[0]
        head_buf[pl.ds(b, rows, stride=n_seqs), :] = out

    def wait_caches(b):
        for copy in kv_load(b):
            copy.wait()

    def attend_pair(i, carry):
        first = 2 * i
        after = jnp.minimum(first + 2, n_seqs - 1)
        wait_caches(first + 1)

        @pl.when(first + 2 < n_seqs)
        def _():
            wait_caches(after)

        attend(first, 0, first + 1)
        attend(first + 1, 1, after)

        @pl.when(i == part_seqs // 2 - 2)
        def _():
            unpack(1)

        @pl.when(i == part_seqs // 2 - 1)
        def _():
            pack(0)

        @pl.when(i == n_seqs // 2 - 2)
        def _():
            forward(0)

        return carry

    unpack(0)
    wait_caches(0)
    best = None
    for start in range(0, length, KEY_TILE):
        best = score_tile(query(0), k_buf.at[0], score_buf.at[0], start, len_ref[0], best)
    best_buf[0] = best
    lax.fori_loop(0, n_seqs // 2, attend_pair, 0)
    pack(1)
    partial(0)
    forward(1)
    each(middle, 0)
    partial(1)
    each(finish, 0)
    each(middle, 1)
    each(relay, 0)
    each(finish, 1)
    each(last, 0)
    each(relay, 1)
    each(last, 1)
    wo_swap.wait_send()
    for p in range(N_PARTS):
        for n in range(q_width // Q_TILE):
            for d in range(1, n_dev):
                q_copy(p, n, d).wait_send()
        for s in range(n_steps):
            for i in range(4, 9):
                ag(p, s, i).wait_recv()
            for i in range(9):
                ag(p, s, i).wait_send()
            for i in range(6):
                rs(p, s, i).wait_send()
        for d in (1, 2, 3):
            a_copy(p, d).wait_send()
        for d in range(N_CHIPS):
            a_forward(p, d).wait_send()


def store_kernel(n_steps, len_ref, fk_ref, fv_ref, y_ref, k_ref, v_ref, y_out, k_out, v_out, k_buf, v_buf, sems, y_sem):
    n_seqs, length, depth = k_buf.shape

    def store(b):
        return (pltpu.make_async_copy(k_buf.at[b], k_out.at[b], sems.at[0, b]),
                pltpu.make_async_copy(v_buf.at[b], v_out.at[b], sems.at[1, b]))

    def patch(b, buf, fresh):
        start = pl.multiple_of(jnp.minimum(len_ref[b] // 8 * 8, length - WINDOW), 8)
        offset = len_ref[b] - start
        row = lax.broadcasted_iota(jnp.int32, (WINDOW, depth), 0)
        window = buf[b, pl.ds(start, WINDOW), :].astype(jnp.float32)
        for s in range(n_steps):
            window = jnp.where(row == offset + s, fresh[b * FRESH_ROWS + s:b * FRESH_ROWS + s + 1, :], window)
        buf[b, pl.ds(start, WINDOW), :] = window.astype(buf.dtype)

    y_copy = pltpu.make_async_copy(y_ref, y_out, y_sem)
    y_copy.start()
    for b in range(n_seqs):
        patch(b, k_buf, fk_ref)
        patch(b, v_buf, fv_ref)
        for copy in store(b):
            copy.start()
    y_copy.wait()
    for b in range(n_seqs):
        for copy in store(b):
            copy.wait()


def solution(mesh):
    def local_block(x_steps, seq_lens, k_cache, v_cache, ln_gain, ln_bias, w_q, b_q, w_kv, b_kv, w_out, b_out):
        n_steps, _, width = x_steps.shape
        n_seqs, length, depth = k_cache.shape
        q_width = w_q.shape[1]
        n_dev = N_CHIPS * N_CORES
        part_seqs = n_seqs // N_PARTS
        rows = n_dev * n_steps * q_width // depth
        chip_width, half = N_CORES * q_width, width // 2
        block = N_CORES * part_seqs
        smem = pl.BlockSpec(memory_space=pltpu.SMEM)
        vmem = pl.BlockSpec(memory_space=pltpu.VMEM)
        hbm = pl.BlockSpec(memory_space=pl.ANY)
        dma = pltpu.SemaphoreType.DMA
        bf16, f32 = jnp.bfloat16, jnp.float32
        y_shape = (n_steps, N_CHIPS, N_CORES, N_PARTS, part_seqs, width)
        fresh_shape = (n_seqs * FRESH_ROWS, depth)
        y_vm, k_vm, v_vm, fresh_k, fresh_v = pl.pallas_call(
            block_kernel,
            out_shape=[pltpu.VMEM(y_shape, bf16), pltpu.VMEM(k_cache.shape, bf16), pltpu.VMEM(v_cache.shape, bf16), pltpu.VMEM(fresh_shape, f32), pltpu.VMEM(fresh_shape, f32)],
            in_specs=[hbm] * 12,
            out_specs=[vmem] * 5,
            scratch_shapes=[
                pltpu.SMEM(seq_lens.shape, jnp.int32),
                pltpu.VMEM(ln_gain.shape, bf16),
                pltpu.VMEM(ln_bias.shape, bf16),
                pltpu.VMEM(b_q.shape, bf16),
                pltpu.VMEM(b_kv.shape, bf16),
                pltpu.VMEM(b_out.shape, bf16),
                pltpu.VMEM((N_PARTS, n_steps, n_dev, part_seqs, width), bf16),
                pltpu.VMEM((n_steps, n_seqs, width), bf16),
                pltpu.VMEM((n_steps * n_seqs, width), bf16),
                pltpu.VMEM((N_PARTS, n_steps * n_dev * part_seqs, width), bf16),
                pltpu.VMEM((LN_ROWS, width), f32),
                pltpu.VMEM((LN_ROWS, width), f32),
                pltpu.VMEM((1, width), f32),
                pltpu.VMEM(w_q.shape, bf16),
                pltpu.VMEM(w_kv.shape, bf16),
                pltpu.VMEM((chip_width, half), bf16),
                pltpu.VMEM((q_width, half), bf16),
                pltpu.VMEM((N_PARTS, n_steps, n_dev, part_seqs, q_width), bf16),
                pltpu.VMEM((N_PARTS, n_dev, n_steps, part_seqs, q_width), bf16),
                pltpu.VMEM((rows * n_seqs, depth), f32),
                pltpu.VMEM((2, rows, length), f32),
                pltpu.VMEM((2, rows, LANES), f32),
                pltpu.VMEM((rows * n_seqs, depth), f32),
                pltpu.VMEM((N_PARTS, N_CHIPS, n_steps, part_seqs, chip_width), bf16),
                pltpu.VMEM((N_PARTS, N_CORES, N_CHIPS, n_steps, part_seqs, chip_width), bf16),
                pltpu.VMEM((n_steps * N_CHIPS * block, chip_width), bf16),
                pltpu.VMEM((N_PARTS, n_steps, N_CHIPS, block, half), bf16),
                pltpu.VMEM((N_PARTS, n_steps, 2, block, half // 2), bf16),
                pltpu.VMEM((N_PARTS, n_steps, 4, block, half // 2), bf16),
                dma((6,)), dma((2 * N_PARTS,)), dma((4,)), dma((2, n_seqs)), dma((2,)),
                dma((N_PARTS, q_width // Q_TILE, n_dev - 1)), dma((N_PARTS, q_width // Q_TILE, n_dev - 1)),
                dma((N_PARTS, 3)), dma((N_PARTS, 3)),
                dma((N_PARTS, N_CHIPS)), dma((N_PARTS, N_CHIPS)),
                dma((N_PARTS, n_steps, 6)), dma((N_PARTS, n_steps, 6)),
                dma((N_PARTS, n_steps, 9)), dma((N_PARTS, n_steps, 9)),
            ],
            compiler_params=pltpu.CompilerParams(vmem_limit_bytes=BLOCK_VMEM, collective_id=1, has_side_effects=True),
            cost_estimate=pl.CostEstimate(flops=4 * n_seqs * rows * length * depth, bytes_accessed=4 * n_seqs * length * depth, transcendentals=n_seqs * rows * length),
        )(seq_lens, ln_gain, ln_bias, b_q, b_kv, b_out,
          x_steps.reshape(n_steps, n_dev, N_PARTS, part_seqs, width), w_q, w_kv, w_out, k_cache, v_cache)
        y_steps, k_out, v_out, _, _ = pl.pallas_call(
            functools.partial(store_kernel, n_steps),
            out_shape=[jax.ShapeDtypeStruct(y_shape, bf16), jax.ShapeDtypeStruct(k_cache.shape, bf16), jax.ShapeDtypeStruct(v_cache.shape, bf16), pltpu.VMEM(k_cache.shape, bf16), pltpu.VMEM(v_cache.shape, bf16)],
            in_specs=[smem] + [vmem] * 5,
            out_specs=[hbm] * 3 + [vmem] * 2,
            scratch_shapes=[dma((2, n_seqs)), dma],
            input_output_aliases={4: 3, 5: 4},
            compiler_params=pltpu.CompilerParams(vmem_limit_bytes=2 * 1024 * 1024),
        )(seq_lens, fresh_k, fresh_v, y_vm, k_vm, v_vm)
        return y_steps.reshape(x_steps.shape), k_out, v_out

    row_spec = P(('dp', 'tp'), None, None)
    return jax.shard_map(
        local_block,
        mesh=mesh,
        in_specs=(P(None, 'dp', None), P(('dp', 'tp')), row_spec, row_spec, P(None), P(None), P(None, 'tp'), P('tp'), P(None, None), P(None), P('tp', None), P(None)),
        out_specs=(P(None, 'dp', None), row_spec, row_spec),
        check_vma=False,
    )
```

```python
import functools
import math

import jax
import jax.numpy as jnp
from jax import lax
from jax.experimental import pallas as pl
from jax.experimental.pallas import tpu as pltpu
from jax.sharding import PartitionSpec as P

LN_EPS = 1e-5
KEY_TILE = 256
LANES = 128
FRESH_ROWS = 16
WINDOW = 16
N_CHIPS = 4
N_CORES = 2
N_PARTS = 2
LN_ROWS = 16
MESH = pl.DeviceIdType.MESH
BLOCK_VMEM = 32 * 1024 * 1024


CONTRACT_LAST = (((1,), (1,)), ((), ()))


def score_tile(q_rows, k_ref, score_ref, start, seq_len, best):
    tile = lax.dot_general(q_rows, k_ref[start:start + KEY_TILE, :], CONTRACT_LAST, preferred_element_type=jnp.float32)
    lane = lax.broadcasted_iota(jnp.int32, tile.shape, 1)
    tile = jnp.where(lane < seq_len - start, tile, -jnp.inf)
    score_ref[:, start:start + KEY_TILE] = tile
    high = jnp.maximum(tile[:, :LANES], tile[:, LANES:])
    return high if best is None else jnp.maximum(best, high)


def attend_one(q_rows, v_ref, score_ref, best, fresh_k, fresh_v, fresh_mask, beside):
    length, depth = v_ref.shape
    to_log2 = depth ** -0.5 * math.log2(math.e)
    new_scores = lax.dot_general(q_rows, fresh_k, CONTRACT_LAST, preferred_element_type=jnp.float32)
    new_scores = jnp.where(fresh_mask, new_scores, -jnp.inf)
    top = jnp.maximum(jnp.max(best, axis=-1, keepdims=True), jnp.max(new_scores, axis=-1, keepdims=True))
    new_weights = jnp.exp2((new_scores - top) * to_log2)
    numerator = jnp.dot(new_weights.astype(jnp.bfloat16), fresh_v, preferred_element_type=jnp.float32)
    total, pieces = None, []
    for start in range(0, length, KEY_TILE):
        beside(start)
        weights = jnp.exp2((score_ref[:, start:start + KEY_TILE] - top) * to_log2)
        folded = weights[:, :LANES] + weights[:, LANES:]
        total = folded if total is None else total + folded
        pieces.append(weights.astype(jnp.bfloat16))
    numerator = numerator + jnp.dot(jnp.concatenate(pieces, axis=1), v_ref[...], preferred_element_type=jnp.float32)
    return numerator / (jnp.sum(total, axis=-1, keepdims=True) + jnp.sum(new_weights, axis=-1, keepdims=True))


def block_kernel(
        len_hbm, g_hbm, lb_hbm, bq_hbm, bkv_hbm, bo_hbm, x_hbm, wq_hbm, wkv_hbm, wo_hbm, k_hbm, v_hbm,
        y_ref, k_buf, v_buf, fk_ref, fv_ref,
        len_ref, g_ref, lb_ref, bq_ref, bkv_ref, bo_ref, x_buf, own_x, own_h, h_buf, gain_buf, bias_buf, bo_buf, wq_buf, wkv_buf, w_buf, swap_buf, q_buf, q_in, q_rows, score_buf, best_buf, head_buf, a_src, a_buf, lhs_buf, p_buf, mid_buf, fin_buf,
        vec_sems, x_sems, w_sems, kv_sems, swap_sems, q_send, q_recv, a_send, a_recv, f_send, f_recv, rs_send, rs_recv, ag_send, ag_recv):
    me = lax.axis_index('tp')
    n_dev = N_CHIPS * N_CORES
    chip, core = me // N_CORES, me % N_CORES
    n_steps, _, width = own_x.shape
    n_seqs, length, depth = k_buf.shape
    q_width = wq_buf.shape[1]
    dev_heads = q_width // depth
    chip_heads = N_CORES * dev_heads
    part_seqs = n_seqs // N_PARTS
    rows = n_dev * n_steps * dev_heads
    own_rows = wo_hbm.shape[0]
    half, quarter = width // 2, width // 4
    block = N_CORES * part_seqs

    def chip_at(k):
        return (chip + k) % N_CHIPS

    def device(k):
        return {'tp': chip_at(k) * N_CORES + core}

    def member(d):
        return (me + d) % n_dev

    right, left, partner = device(1), device(3), {'tp': chip * N_CORES + 1 - core}

    def remote(src, dst, send, recv, to):
        return pltpu.make_async_remote_copy(src_ref=src, dst_ref=dst, send_sem=send, recv_sem=recv, device_id=to, device_id_type=MESH)

    def cols(which, begin, size):
        return pl.ds(pl.multiple_of(which * half + begin, quarter), size)

    def x_load(p):
        return pltpu.make_async_copy(x_hbm.at[:, :, p], x_buf.at[p], x_sems.at[p])

    def kv_load(b):
        return (pltpu.make_async_copy(k_hbm.at[b], k_buf.at[b], kv_sems.at[0, b]),
                pltpu.make_async_copy(v_hbm.at[b], v_buf.at[b], kv_sems.at[1, b]))

    own_x_loads = [pltpu.make_async_copy(x_hbm.at[:, me, p], own_x.at[:, p * part_seqs:(p + 1) * part_seqs, :], x_sems.at[N_PARTS + p]) for p in range(N_PARTS)]
    own_w_rows = pl.ds(pl.multiple_of(core * own_rows, own_rows), own_rows)
    wq_load = pltpu.make_async_copy(wq_hbm, wq_buf, w_sems.at[0])
    wkv_load = pltpu.make_async_copy(wkv_hbm, wkv_buf, w_sems.at[1])
    wo_load = pltpu.make_async_copy(wo_hbm.at[:, cols(core, 0, half)], w_buf.at[own_w_rows, :], w_sems.at[2])
    swap_load = pltpu.make_async_copy(wo_hbm.at[:, cols(1 - core, 0, half)], swap_buf, w_sems.at[3])
    wo_swap = remote(swap_buf, w_buf.at[own_w_rows, :], swap_sems.at[0], swap_sems.at[1], partner)
    vector_loads = [pltpu.make_async_copy(src, dst, vec_sems.at[i]) for i, (src, dst) in enumerate(
        ((g_hbm, g_ref), (lb_hbm, lb_ref), (bq_hbm, bq_ref), (bkv_hbm, bkv_ref), (bo_hbm, bo_ref), (len_hbm, len_ref)))]
    for copy in vector_loads:
        copy.start()
    x_load(0).start()
    wq_load.start()

    barrier = pltpu.get_barrier_semaphore()
    for d in range(1, n_dev):
        pl.semaphore_signal(barrier, inc=1, device_id={'tp': member(d)}, device_id_type=MESH)

    for copy in vector_loads:
        copy.wait()

    bq_row = bq_ref[...].astype(jnp.float32).reshape(1, q_width)
    bo_buf[...] = bo_ref[...].astype(jnp.float32).reshape(1, width)
    gain_buf[...] = jnp.broadcast_to(g_ref[...].astype(jnp.float32).reshape(1, width), gain_buf.shape)
    bias_buf[...] = jnp.broadcast_to(lb_ref[...].astype(jnp.float32).reshape(1, width), bias_buf.shape)

    def norm(x_float):
        centered = x_float - jnp.mean(x_float, axis=-1, keepdims=True)
        row_var = jnp.mean(centered * centered, axis=-1, keepdims=True)
        scaled = centered * lax.rsqrt(row_var + LN_EPS)
        return (scaled * gain_buf[...] + bias_buf[...]).astype(h_buf.dtype)

    def q_copy(p, d):
        return remote(q_buf.at[p, :, member(d)], q_in.at[p, me], q_send.at[p, d - 1], q_recv.at[p, d - 1], {'tp': member(d)})

    group = LN_ROWS // part_seqs
    for p in range(N_PARTS):
        x_load(p).wait()
        if p == 0:
            for later in range(1, N_PARTS):
                x_load(later).start()
            for copy in own_x_loads:
                copy.start()
            wkv_load.start()

        for s in range(n_steps):
            def norm_rows(i, carry):
                x_float = jnp.concatenate([x_buf[p, s, i * group + j].astype(jnp.float32) for j in range(group)], axis=0)
                where = pl.ds(pl.multiple_of((s * n_dev // group + i) * LN_ROWS, LN_ROWS), LN_ROWS)
                h_buf[p, where, :] = norm(x_float)
                return carry

            lax.fori_loop(0, n_dev // group, norm_rows, 0)
        if p == 0:
            wq_load.wait()
            swap_load.start()
            wo_load.start()
        for n in range(0, q_width, 256):
            part = jnp.dot(h_buf[p], wq_buf[:, n:n + 256], preferred_element_type=jnp.float32) + bq_row[:, n:n + 256]
            for s in range(n_steps):
                for u in range(n_dev):
                    first = (s * n_dev + u) * part_seqs
                    q_buf[p, s, u, :, n:n + 256] = part[first:first + part_seqs].astype(q_buf.dtype)
        if p == 0:
            pl.semaphore_wait(barrier, n_dev - 1)
        for d in range(1, n_dev):
            q_copy(p, d).start()
        if p == 0:
            swap_load.wait()
            wo_swap.start()
        for b in range(p * part_seqs, (p + 1) * part_seqs):
            for copy in kv_load(b):
                copy.start()
        q_in[p, me] = q_buf[p, :, me]

    for copy in own_x_loads:
        copy.wait()
    for s in range(n_steps):
        own_h[s * n_seqs:(s + 1) * n_seqs, :] = norm(own_x[s].astype(jnp.float32))
    wkv_load.wait()
    fresh = jnp.dot(own_h[...], wkv_buf[...], preferred_element_type=jnp.float32) + bkv_ref[...].astype(jnp.float32).reshape(1, -1)
    fresh = fresh.astype(jnp.bfloat16).astype(jnp.float32)
    fk_ref[...] = jnp.zeros_like(fk_ref)
    fv_ref[...] = jnp.zeros_like(fv_ref)
    for s in range(n_steps):
        where = pl.ds(s, n_seqs, stride=FRESH_ROWS)
        fk_ref[where, :] = fresh[s * n_seqs:(s + 1) * n_seqs, :depth]
        fv_ref[where, :] = fresh[s * n_seqs:(s + 1) * n_seqs, depth:]

    def unpack(p):
        for d in range(1, n_dev):
            q_copy(p, d).wait_recv()
        for u in range(n_dev):
            for s in range(n_steps):
                for h in range(dev_heads):
                    first = ((u * n_steps + s) * dev_heads + h) * n_seqs + p * part_seqs
                    q_rows[first:first + part_seqs, :] = q_in[p, u, s, :, h * depth:(h + 1) * depth].astype(jnp.float32)

    shape = (rows, FRESH_ROWS)
    step_of_row = lax.broadcasted_iota(jnp.int32, shape, 0) // dev_heads % n_steps
    fresh_mask = lax.broadcasted_iota(jnp.int32, shape, 1) <= step_of_row

    def a_copy(p, d):
        return remote(a_src.at[p, chip_at(d)], a_buf.at[p, core, chip], a_send.at[p, d - 1], a_recv.at[p, d - 1], device(d))

    def a_forward(p, d):
        where = a_buf.at[p, core, chip_at(N_CHIPS - d)]
        return remote(a_src.at[p, chip] if d == 0 else where, where, f_send.at[p, d], f_recv.at[p, d], partner)

    low, high = pl.ds(0, quarter), pl.ds(quarter, quarter)

    def rs(p, s, i):
        def part(k, where):
            return p_buf.at[p, s, chip_at(k), :, where]
        src, dst, to = (
            (part(2, low), mid_buf.at[p, s, 0], right),
            (part(2, high), mid_buf.at[p, s, 1], left),
            (part(1, high), fin_buf.at[p, s, 0], right),
            (part(3, low), fin_buf.at[p, s, 1], left),
            (part(1, low), fin_buf.at[p, s, 2], right),
            (part(3, high), fin_buf.at[p, s, 3], left),
        )[i]
        return remote(src, dst, rs_send.at[p, s, i], rs_recv.at[p, s, i], to)

    def ag(p, s, i):
        k, begin, size, to = (
            (0, 0, half, right),
            (0, 0, half, left),
            (3, 0, quarter, right),
            (1, quarter, quarter, left),
            (0, 0, half, partner),
            (3, 0, half, partner),
            (1, 0, half, partner),
            (2, 0, quarter, partner),
            (2, quarter, quarter, partner),
        )[i]
        where = y_ref.at[s, chip_at(k), :, p, :, cols(core, begin, size)]
        return remote(where, where, ag_send.at[p, s, i], ag_recv.at[p, s, i], to)

    def pack(p):
        for t in range(N_CHIPS):
            for s in range(n_steps):
                pieces = []
                for h in range(chip_heads):
                    u = t * N_CORES + h // dev_heads
                    first = ((u * n_steps + s) * dev_heads + h % dev_heads) * n_seqs + p * part_seqs
                    pieces.append(head_buf[first:first + part_seqs, :])
                a_src[p, t, s] = jnp.concatenate(pieces, axis=1).astype(a_src.dtype)
        for d in (2, 1, 3):
            a_copy(p, d).start()
        a_forward(p, 0).start()
        a_buf[p, core, chip] = a_src[p, chip]

    def forward(p):
        for d in (1, 3, 2):
            a_copy(p, d).wait_recv()
            a_forward(p, d).start()

    def partial(p):
        for d in range(N_CHIPS):
            a_forward(p, d).wait_recv()
        if p == 0:
            wo_load.wait()
            wo_swap.wait_recv()
        for s in range(n_steps):
            for t in range(N_CHIPS):
                pair = jnp.concatenate([a_buf[p, c, t, s].astype(jnp.float32) for c in range(N_CORES)], axis=0)
                first = (s * N_CHIPS + t) * block
                lhs_buf[first:first + block, :] = pair.astype(lhs_buf.dtype)
        for n in range(0, half, 512):
            out = jnp.dot(lhs_buf[...], w_buf[:, n:n + 512], preferred_element_type=jnp.float32).astype(p_buf.dtype)
            for s in range(n_steps):
                for t in range(N_CHIPS):
                    first = (s * N_CHIPS + t) * block
                    p_buf[p, s, t, :, n:n + 512] = out[first:first + block]
        for pair in ((0, 1), (2, 3)):
            for s in range(n_steps):
                for i in pair:
                    rs(p, s, i).start()

    def add_into(target, other):
        target[...] = (target[...].astype(jnp.float32) + other[...].astype(jnp.float32)).astype(target.dtype)

    def middle(p, s):
        rs(p, s, 0).wait_recv()
        add_into(p_buf.at[p, s, chip_at(1), :, low], mid_buf.at[p, s, 0])
        rs(p, s, 4).start()
        rs(p, s, 1).wait_recv()
        add_into(p_buf.at[p, s, chip_at(3), :, high], mid_buf.at[p, s, 1])
        rs(p, s, 5).start()

    def finish(p, s):
        for i in (2, 3, 4, 5):
            rs(p, s, i).wait_recv()
        for begin, one, two in ((0, 1, 2), (quarter, 0, 3)):
            where = cols(core, begin, quarter)
            total = p_buf[p, s, chip, :, begin:begin + quarter].astype(jnp.float32)
            total = total + fin_buf[p, s, one].astype(jnp.float32)
            total = total + fin_buf[p, s, two].astype(jnp.float32)
            total = total + bo_buf[:, where]
            for c in range(N_CORES):
                x_part = x_buf[p, s, chip * N_CORES + c, :, where].astype(jnp.float32)
                y_ref[s, chip, c, p, :, where] = (x_part + total[c * part_seqs:(c + 1) * part_seqs]).astype(y_ref.dtype)
        for i in (0, 1, 4):
            ag(p, s, i).start()

    def relay(p, s):
        ag(p, s, 0).wait_recv()
        ag(p, s, 2).start()
        ag(p, s, 5).start()
        ag(p, s, 1).wait_recv()
        ag(p, s, 3).start()
        ag(p, s, 6).start()

    def last(p, s):
        ag(p, s, 2).wait_recv()
        ag(p, s, 7).start()
        ag(p, s, 3).wait_recv()
        ag(p, s, 8).start()

    def each(stage, p):
        for s in range(n_steps):
            stage(p, s)

    def query(b):
        return q_rows[pl.ds(b, rows, stride=n_seqs), :].astype(jnp.bfloat16)

    def attend(b, slot, after):
        new = pl.ds(pl.multiple_of(b * FRESH_ROWS, FRESH_ROWS), FRESH_ROWS)
        q_after = query(after)
        maxima = [None]

        def beside(start):
            maxima[0] = score_tile(q_after, k_buf.at[after], score_buf.at[1 - slot], start, len_ref[after], maxima[0])

        out = attend_one(query(b), v_buf.at[b], score_buf.at[slot], best_buf[slot],
                         fk_ref[new, :].astype(jnp.bfloat16), fv_ref[new, :].astype(jnp.bfloat16), fresh_mask, beside)
        best_buf[1 - slot] = maxima[0]
        head_buf[pl.ds(b, rows, stride=n_seqs), :] = out

    def wait_caches(b):
        for copy in kv_load(b):
            copy.wait()

    def attend_pair(i, carry):
        first = 2 * i
        after = jnp.minimum(first + 2, n_seqs - 1)
        wait_caches(first + 1)

        @pl.when(first + 2 < n_seqs)
        def _():
            wait_caches(after)

        attend(first, 0, first + 1)
        attend(first + 1, 1, after)

        @pl.when(i == part_seqs // 2 - 2)
        def _():
            unpack(1)

        @pl.when(i == part_seqs // 2 - 1)
        def _():
            pack(0)

        @pl.when(i == n_seqs // 2 - 2)
        def _():
            forward(0)

        return carry

    unpack(0)
    wait_caches(0)
    best = None
    for start in range(0, length, KEY_TILE):
        best = score_tile(query(0), k_buf.at[0], score_buf.at[0], start, len_ref[0], best)
    best_buf[0] = best
    lax.fori_loop(0, n_seqs // 2, attend_pair, 0)
    pack(1)
    partial(0)
    forward(1)
    each(middle, 0)
    partial(1)
    each(middle, 1)
    each(finish, 0)
    each(finish, 1)
    each(relay, 0)
    each(relay, 1)
    each(last, 0)
    each(last, 1)
    wo_swap.wait_send()
    for p in range(N_PARTS):
        for d in range(1, n_dev):
            q_copy(p, d).wait_send()
        for s in range(n_steps):
            for i in range(4, 9):
                ag(p, s, i).wait_recv()
            for i in range(9):
                ag(p, s, i).wait_send()
            for i in range(6):
                rs(p, s, i).wait_send()
        for d in (1, 2, 3):
            a_copy(p, d).wait_send()
        for d in range(N_CHIPS):
            a_forward(p, d).wait_send()


def store_kernel(n_steps, len_ref, fk_ref, fv_ref, y_ref, k_ref, v_ref, y_out, k_out, v_out, k_buf, v_buf, sems, y_sem):
    n_seqs, length, depth = k_buf.shape

    def store(b):
        return (pltpu.make_async_copy(k_buf.at[b], k_out.at[b], sems.at[0, b]),
                pltpu.make_async_copy(v_buf.at[b], v_out.at[b], sems.at[1, b]))

    def patch(b, buf, fresh):
        start = pl.multiple_of(jnp.minimum(len_ref[b] // 8 * 8, length - WINDOW), 8)
        offset = len_ref[b] - start
        row = lax.broadcasted_iota(jnp.int32, (WINDOW, depth), 0)
        window = buf[b, pl.ds(start, WINDOW), :].astype(jnp.float32)
        for s in range(n_steps):
            window = jnp.where(row == offset + s, fresh[b * FRESH_ROWS + s:b * FRESH_ROWS + s + 1, :], window)
        buf[b, pl.ds(start, WINDOW), :] = window.astype(buf.dtype)

    y_copy = pltpu.make_async_copy(y_ref, y_out, y_sem)
    y_copy.start()
    for b in range(n_seqs):
        patch(b, k_buf, fk_ref)
        patch(b, v_buf, fv_ref)
        for copy in store(b):
            copy.start()
    y_copy.wait()
    for b in range(n_seqs):
        for copy in store(b):
            copy.wait()


def solution(mesh):
    def local_block(x_steps, seq_lens, k_cache, v_cache, ln_gain, ln_bias, w_q, b_q, w_kv, b_kv, w_out, b_out):
        n_steps, _, width = x_steps.shape
        n_seqs, length, depth = k_cache.shape
        q_width = w_q.shape[1]
        n_dev = N_CHIPS * N_CORES
        part_seqs = n_seqs // N_PARTS
        rows = n_dev * n_steps * q_width // depth
        chip_width, half = N_CORES * q_width, width // 2
        block = N_CORES * part_seqs
        smem = pl.BlockSpec(memory_space=pltpu.SMEM)
        vmem = pl.BlockSpec(memory_space=pltpu.VMEM)
        hbm = pl.BlockSpec(memory_space=pl.ANY)
        dma = pltpu.SemaphoreType.DMA
        bf16, f32 = jnp.bfloat16, jnp.float32
        y_shape = (n_steps, N_CHIPS, N_CORES, N_PARTS, part_seqs, width)
        fresh_shape = (n_seqs * FRESH_ROWS, depth)
        y_vm, k_vm, v_vm, fresh_k, fresh_v = pl.pallas_call(
            block_kernel,
            out_shape=[pltpu.VMEM(y_shape, bf16), pltpu.VMEM(k_cache.shape, bf16), pltpu.VMEM(v_cache.shape, bf16), pltpu.VMEM(fresh_shape, f32), pltpu.VMEM(fresh_shape, f32)],
            in_specs=[hbm] * 12,
            out_specs=[vmem] * 5,
            scratch_shapes=[
                pltpu.SMEM(seq_lens.shape, jnp.int32),
                pltpu.VMEM(ln_gain.shape, bf16),
                pltpu.VMEM(ln_bias.shape, bf16),
                pltpu.VMEM(b_q.shape, bf16),
                pltpu.VMEM(b_kv.shape, bf16),
                pltpu.VMEM(b_out.shape, bf16),
                pltpu.VMEM((N_PARTS, n_steps, n_dev, part_seqs, width), bf16),
                pltpu.VMEM((n_steps, n_seqs, width), bf16),
                pltpu.VMEM((n_steps * n_seqs, width), bf16),
                pltpu.VMEM((N_PARTS, n_steps * n_dev * part_seqs, width), bf16),
                pltpu.VMEM((LN_ROWS, width), f32),
                pltpu.VMEM((LN_ROWS, width), f32),
                pltpu.VMEM((1, width), f32),
                pltpu.VMEM(w_q.shape, bf16),
                pltpu.VMEM(w_kv.shape, bf16),
                pltpu.VMEM((chip_width, half), bf16),
                pltpu.VMEM((q_width, half), bf16),
                pltpu.VMEM((N_PARTS, n_steps, n_dev, part_seqs, q_width), bf16),
                pltpu.VMEM((N_PARTS, n_dev, n_steps, part_seqs, q_width), bf16),
                pltpu.VMEM((rows * n_seqs, depth), f32),
                pltpu.VMEM((2, rows, length), f32),
                pltpu.VMEM((2, rows, LANES), f32),
                pltpu.VMEM((rows * n_seqs, depth), f32),
                pltpu.VMEM((N_PARTS, N_CHIPS, n_steps, part_seqs, chip_width), bf16),
                pltpu.VMEM((N_PARTS, N_CORES, N_CHIPS, n_steps, part_seqs, chip_width), bf16),
                pltpu.VMEM((n_steps * N_CHIPS * block, chip_width), bf16),
                pltpu.VMEM((N_PARTS, n_steps, N_CHIPS, block, half), bf16),
                pltpu.VMEM((N_PARTS, n_steps, 2, block, half // 2), bf16),
                pltpu.VMEM((N_PARTS, n_steps, 4, block, half // 2), bf16),
                dma((6,)), dma((2 * N_PARTS,)), dma((4,)), dma((2, n_seqs)), dma((2,)),
                dma((N_PARTS, n_dev - 1)), dma((N_PARTS, n_dev - 1)),
                dma((N_PARTS, 3)), dma((N_PARTS, 3)),
                dma((N_PARTS, N_CHIPS)), dma((N_PARTS, N_CHIPS)),
                dma((N_PARTS, n_steps, 6)), dma((N_PARTS, n_steps, 6)),
                dma((N_PARTS, n_steps, 9)), dma((N_PARTS, n_steps, 9)),
            ],
            compiler_params=pltpu.CompilerParams(vmem_limit_bytes=BLOCK_VMEM, collective_id=1, has_side_effects=True),
            cost_estimate=pl.CostEstimate(flops=4 * n_seqs * rows * length * depth, bytes_accessed=4 * n_seqs * length * depth, transcendentals=n_seqs * rows * length),
        )(seq_lens, ln_gain, ln_bias, b_q, b_kv, b_out,
          x_steps.reshape(n_steps, n_dev, N_PARTS, part_seqs, width), w_q, w_kv, w_out, k_cache, v_cache)
        y_steps, k_out, v_out, _, _ = pl.pallas_call(
            functools.partial(store_kernel, n_steps),
            out_shape=[jax.ShapeDtypeStruct(y_shape, bf16), jax.ShapeDtypeStruct(k_cache.shape, bf16), jax.ShapeDtypeStruct(v_cache.shape, bf16), pltpu.VMEM(k_cache.shape, bf16), pltpu.VMEM(v_cache.shape, bf16)],
            in_specs=[smem] + [vmem] * 5,
            out_specs=[hbm] * 3 + [vmem] * 2,
            scratch_shapes=[dma((2, n_seqs)), dma],
            input_output_aliases={4: 3, 5: 4},
            compiler_params=pltpu.CompilerParams(vmem_limit_bytes=2 * 1024 * 1024),
        )(seq_lens, fresh_k, fresh_v, y_vm, k_vm, v_vm)
        return y_steps.reshape(x_steps.shape), k_out, v_out

    row_spec = P(('dp', 'tp'), None, None)
    return jax.shard_map(
        local_block,
        mesh=mesh,
        in_specs=(P(None, 'dp', None), P(('dp', 'tp')), row_spec, row_spec, P(None), P(None), P(None, 'tp'), P('tp'), P(None, None), P(None), P('tp', None), P(None)),
        out_specs=(P(None, 'dp', None), row_spec, row_spec),
        check_vma=False,
    )
```

```python
import functools
import math

import jax
import jax.numpy as jnp
from jax import lax
from jax.experimental import pallas as pl
from jax.experimental.pallas import tpu as pltpu
from jax.sharding import PartitionSpec as P

LN_EPS = 1e-5
KEY_TILE = 512
LANES = 128
FRESH_ROWS = 16
WINDOW = 16
N_CHIPS = 4
N_CORES = 2
N_PARTS = 2
LN_ROWS = 16
MESH = pl.DeviceIdType.MESH
BLOCK_VMEM = 32 * 1024 * 1024


CONTRACT_LAST = (((1,), (1,)), ((), ()))


def score_tile(q_rows, k_ref, score_ref, start, seq_len, best):
    tile = lax.dot_general(q_rows, k_ref[start:start + KEY_TILE, :], CONTRACT_LAST, preferred_element_type=jnp.float32)
    lane = lax.broadcasted_iota(jnp.int32, tile.shape, 1)
    tile = jnp.where(lane < seq_len - start, tile, -jnp.inf)
    score_ref[:, start:start + KEY_TILE] = tile
    high = functools.reduce(jnp.maximum, [tile[:, i:i + LANES] for i in range(0, KEY_TILE, LANES)])
    return high if best is None else jnp.maximum(best, high)


def attend_one(q_rows, v_ref, score_ref, best, fresh_k, fresh_v, fresh_mask, beside):
    length, depth = v_ref.shape
    to_log2 = depth ** -0.5 * math.log2(math.e)
    new_scores = lax.dot_general(q_rows, fresh_k, CONTRACT_LAST, preferred_element_type=jnp.float32)
    new_scores = jnp.where(fresh_mask, new_scores, -jnp.inf)
    top = jnp.maximum(jnp.max(best, axis=-1, keepdims=True), jnp.max(new_scores, axis=-1, keepdims=True))
    new_weights = jnp.exp2((new_scores - top) * to_log2)
    numerator = jnp.dot(new_weights.astype(jnp.bfloat16), fresh_v, preferred_element_type=jnp.float32)
    total, pieces = None, []
    for start in range(0, length, KEY_TILE):
        beside(start)
        weights = jnp.exp2((score_ref[:, start:start + KEY_TILE] - top) * to_log2)
        folded = functools.reduce(jnp.add, [weights[:, i:i + LANES] for i in range(0, KEY_TILE, LANES)])
        total = folded if total is None else total + folded
        pieces.append(weights.astype(jnp.bfloat16))
    numerator = numerator + jnp.dot(jnp.concatenate(pieces, axis=1), v_ref[...], preferred_element_type=jnp.float32)
    return numerator / (jnp.sum(total, axis=-1, keepdims=True) + jnp.sum(new_weights, axis=-1, keepdims=True))


def block_kernel(
        len_hbm, g_hbm, lb_hbm, bq_hbm, bkv_hbm, bo_hbm, x_hbm, wq_hbm, wkv_hbm, wo_hbm, k_hbm, v_hbm,
        y_ref, k_buf, v_buf, fk_ref, fv_ref,
        len_ref, g_ref, lb_ref, bq_ref, bkv_ref, bo_ref, x_buf, own_x, own_h, h_buf, gain_buf, bias_buf, bo_buf, wq_buf, wkv_buf, w_buf, swap_buf, q_buf, q_in, q_rows, score_buf, best_buf, head_buf, a_src, a_buf, lhs_buf, p_buf, mid_buf, fin_buf,
        vec_sems, x_sems, w_sems, kv_sems, swap_sems, q_send, q_recv, a_send, a_recv, f_send, f_recv, rs_send, rs_recv, ag_send, ag_recv):
    me = lax.axis_index('tp')
    n_dev = N_CHIPS * N_CORES
    chip, core = me // N_CORES, me % N_CORES
    n_steps, _, width = own_x.shape
    n_seqs, length, depth = k_buf.shape
    q_width = wq_buf.shape[1]
    dev_heads = q_width // depth
    chip_heads = N_CORES * dev_heads
    part_seqs = n_seqs // N_PARTS
    rows = n_dev * n_steps * dev_heads
    own_rows = wo_hbm.shape[0]
    half, quarter = width // 2, width // 4
    block = N_CORES * part_seqs

    def chip_at(k):
        return (chip + k) % N_CHIPS

    def device(k):
        return {'tp': chip_at(k) * N_CORES + core}

    def member(d):
        return (me + d) % n_dev

    right, left, partner = device(1), device(3), {'tp': chip * N_CORES + 1 - core}

    def remote(src, dst, send, recv, to):
        return pltpu.make_async_remote_copy(src_ref=src, dst_ref=dst, send_sem=send, recv_sem=recv, device_id=to, device_id_type=MESH)

    def cols(which, begin, size):
        return pl.ds(pl.multiple_of(which * half + begin, quarter), size)

    def x_load(p):
        return pltpu.make_async_copy(x_hbm.at[:, :, p], x_buf.at[p], x_sems.at[p])

    def kv_load(b):
        return (pltpu.make_async_copy(k_hbm.at[b], k_buf.at[b], kv_sems.at[0, b]),
                pltpu.make_async_copy(v_hbm.at[b], v_buf.at[b], kv_sems.at[1, b]))

    own_x_loads = [pltpu.make_async_copy(x_hbm.at[:, me, p], own_x.at[:, p * part_seqs:(p + 1) * part_seqs, :], x_sems.at[N_PARTS + p]) for p in range(N_PARTS)]
    own_w_rows = pl.ds(pl.multiple_of(core * own_rows, own_rows), own_rows)
    wq_load = pltpu.make_async_copy(wq_hbm, wq_buf, w_sems.at[0])
    wkv_load = pltpu.make_async_copy(wkv_hbm, wkv_buf, w_sems.at[1])
    wo_load = pltpu.make_async_copy(wo_hbm.at[:, cols(core, 0, half)], w_buf.at[own_w_rows, :], w_sems.at[2])
    swap_load = pltpu.make_async_copy(wo_hbm.at[:, cols(1 - core, 0, half)], swap_buf, w_sems.at[3])
    wo_swap = remote(swap_buf, w_buf.at[own_w_rows, :], swap_sems.at[0], swap_sems.at[1], partner)
    vector_loads = [pltpu.make_async_copy(src, dst, vec_sems.at[i]) for i, (src, dst) in enumerate(
        ((g_hbm, g_ref), (lb_hbm, lb_ref), (bq_hbm, bq_ref), (bkv_hbm, bkv_ref), (bo_hbm, bo_ref), (len_hbm, len_ref)))]
    for copy in vector_loads:
        copy.start()
    x_load(0).start()
    wq_load.start()

    barrier = pltpu.get_barrier_semaphore()
    for d in range(1, n_dev):
        pl.semaphore_signal(barrier, inc=1, device_id={'tp': member(d)}, device_id_type=MESH)

    for copy in vector_loads:
        copy.wait()

    bq_row = bq_ref[...].astype(jnp.float32).reshape(1, q_width)
    bo_buf[...] = bo_ref[...].astype(jnp.float32).reshape(1, width)
    gain_buf[...] = jnp.broadcast_to(g_ref[...].astype(jnp.float32).reshape(1, width), gain_buf.shape)
    bias_buf[...] = jnp.broadcast_to(lb_ref[...].astype(jnp.float32).reshape(1, width), bias_buf.shape)

    def norm(x_float):
        centered = x_float - jnp.mean(x_float, axis=-1, keepdims=True)
        row_var = jnp.mean(centered * centered, axis=-1, keepdims=True)
        scaled = centered * lax.rsqrt(row_var + LN_EPS)
        return (scaled * gain_buf[...] + bias_buf[...]).astype(h_buf.dtype)

    def q_copy(p, d):
        return remote(q_buf.at[p, :, member(d)], q_in.at[p, me], q_send.at[p, d - 1], q_recv.at[p, d - 1], {'tp': member(d)})

    group = LN_ROWS // part_seqs
    for p in range(N_PARTS):
        x_load(p).wait()
        if p == 0:
            for later in range(1, N_PARTS):
                x_load(later).start()
            for copy in own_x_loads:
                copy.start()
            wkv_load.start()

        for s in range(n_steps):
            def norm_rows(i, carry):
                x_float = jnp.concatenate([x_buf[p, s, i * group + j].astype(jnp.float32) for j in range(group)], axis=0)
                where = pl.ds(pl.multiple_of((s * n_dev // group + i) * LN_ROWS, LN_ROWS), LN_ROWS)
                h_buf[p, where, :] = norm(x_float)
                return carry

            lax.fori_loop(0, n_dev // group, norm_rows, 0)
        if p == 0:
            wq_load.wait()
            swap_load.start()
            wo_load.start()
        for n in range(0, q_width, 256):
            part = jnp.dot(h_buf[p], wq_buf[:, n:n + 256], preferred_element_type=jnp.float32) + bq_row[:, n:n + 256]
            for s in range(n_steps):
                for u in range(n_dev):
                    first = (s * n_dev + u) * part_seqs
                    q_buf[p, s, u, :, n:n + 256] = part[first:first + part_seqs].astype(q_buf.dtype)
        if p == 0:
            pl.semaphore_wait(barrier, n_dev - 1)
        for d in range(1, n_dev):
            q_copy(p, d).start()
        if p == 0:
            swap_load.wait()
            wo_swap.start()
        for b in range(p * part_seqs, (p + 1) * part_seqs):
            for copy in kv_load(b):
                copy.start()
        q_in[p, me] = q_buf[p, :, me]

    for copy in own_x_loads:
        copy.wait()
    for s in range(n_steps):
        own_h[s * n_seqs:(s + 1) * n_seqs, :] = norm(own_x[s].astype(jnp.float32))
    wkv_load.wait()
    fresh = jnp.dot(own_h[...], wkv_buf[...], preferred_element_type=jnp.float32) + bkv_ref[...].astype(jnp.float32).reshape(1, -1)
    fresh = fresh.astype(jnp.bfloat16).astype(jnp.float32)
    fk_ref[...] = jnp.zeros_like(fk_ref)
    fv_ref[...] = jnp.zeros_like(fv_ref)
    for s in range(n_steps):
        where = pl.ds(s, n_seqs, stride=FRESH_ROWS)
        fk_ref[where, :] = fresh[s * n_seqs:(s + 1) * n_seqs, :depth]
        fv_ref[where, :] = fresh[s * n_seqs:(s + 1) * n_seqs, depth:]

    def unpack(p):
        for d in range(1, n_dev):
            q_copy(p, d).wait_recv()
        for u in range(n_dev):
            for s in range(n_steps):
                for h in range(dev_heads):
                    first = ((u * n_steps + s) * dev_heads + h) * n_seqs + p * part_seqs
                    q_rows[first:first + part_seqs, :] = q_in[p, u, s, :, h * depth:(h + 1) * depth].astype(jnp.float32)

    shape = (rows, FRESH_ROWS)
    step_of_row = lax.broadcasted_iota(jnp.int32, shape, 0) // dev_heads % n_steps
    fresh_mask = lax.broadcasted_iota(jnp.int32, shape, 1) <= step_of_row

    def a_copy(p, d):
        return remote(a_src.at[p, chip_at(d)], a_buf.at[p, core, chip], a_send.at[p, d - 1], a_recv.at[p, d - 1], device(d))

    def a_forward(p, d):
        where = a_buf.at[p, core, chip_at(N_CHIPS - d)]
        return remote(a_src.at[p, chip] if d == 0 else where, where, f_send.at[p, d], f_recv.at[p, d], partner)

    low, high = pl.ds(0, quarter), pl.ds(quarter, quarter)

    def rs(p, s, i):
        def part(k, where):
            return p_buf.at[p, s, chip_at(k), :, where]
        src, dst, to = (
            (part(2, low), mid_buf.at[p, s, 0], right),
            (part(2, high), mid_buf.at[p, s, 1], left),
            (part(1, high), fin_buf.at[p, s, 0], right),
            (part(3, low), fin_buf.at[p, s, 1], left),
            (part(1, low), fin_buf.at[p, s, 2], right),
            (part(3, high), fin_buf.at[p, s, 3], left),
        )[i]
        return remote(src, dst, rs_send.at[p, s, i], rs_recv.at[p, s, i], to)

    def ag(p, s, i):
        k, begin, size, to = (
            (0, 0, half, right),
            (0, 0, half, left),
            (3, 0, quarter, right),
            (1, quarter, quarter, left),
            (0, 0, half, partner),
            (3, 0, half, partner),
            (1, 0, half, partner),
            (2, 0, quarter, partner),
            (2, quarter, quarter, partner),
        )[i]
        where = y_ref.at[s, chip_at(k), :, p, :, cols(core, begin, size)]
        return remote(where, where, ag_send.at[p, s, i], ag_recv.at[p, s, i], to)

    def pack(p):
        for t in range(N_CHIPS):
            for s in range(n_steps):
                pieces = []
                for h in range(chip_heads):
                    u = t * N_CORES + h // dev_heads
                    first = ((u * n_steps + s) * dev_heads + h % dev_heads) * n_seqs + p * part_seqs
                    pieces.append(head_buf[first:first + part_seqs, :])
                a_src[p, t, s] = jnp.concatenate(pieces, axis=1).astype(a_src.dtype)
        for d in (2, 1, 3):
            a_copy(p, d).start()
        a_forward(p, 0).start()
        a_buf[p, core, chip] = a_src[p, chip]

    def forward(p):
        for d in (1, 3, 2):
            a_copy(p, d).wait_recv()
            a_forward(p, d).start()

    def partial(p):
        for d in range(N_CHIPS):
            a_forward(p, d).wait_recv()
        if p == 0:
            wo_load.wait()
            wo_swap.wait_recv()
        for s in range(n_steps):
            for t in range(N_CHIPS):
                pair = jnp.concatenate([a_buf[p, c, t, s].astype(jnp.float32) for c in range(N_CORES)], axis=0)
                first = (s * N_CHIPS + t) * block
                lhs_buf[first:first + block, :] = pair.astype(lhs_buf.dtype)
        for n in range(0, half, 512):
            out = jnp.dot(lhs_buf[...], w_buf[:, n:n + 512], preferred_element_type=jnp.float32).astype(p_buf.dtype)
            for s in range(n_steps):
                for t in range(N_CHIPS):
                    first = (s * N_CHIPS + t) * block
                    p_buf[p, s, t, :, n:n + 512] = out[first:first + block]
        for pair in ((0, 1), (2, 3)):
            for s in range(n_steps):
                for i in pair:
                    rs(p, s, i).start()

    def add_into(target, other):
        target[...] = (target[...].astype(jnp.float32) + other[...].astype(jnp.float32)).astype(target.dtype)

    def middle(p, s):
        rs(p, s, 0).wait_recv()
        add_into(p_buf.at[p, s, chip_at(1), :, low], mid_buf.at[p, s, 0])
        rs(p, s, 4).start()
        rs(p, s, 1).wait_recv()
        add_into(p_buf.at[p, s, chip_at(3), :, high], mid_buf.at[p, s, 1])
        rs(p, s, 5).start()

    def finish(p, s):
        for i in (2, 3, 4, 5):
            rs(p, s, i).wait_recv()
        for begin, one, two in ((0, 1, 2), (quarter, 0, 3)):
            where = cols(core, begin, quarter)
            total = p_buf[p, s, chip, :, begin:begin + quarter].astype(jnp.float32)
            total = total + fin_buf[p, s, one].astype(jnp.float32)
            total = total + fin_buf[p, s, two].astype(jnp.float32)
            total = total + bo_buf[:, where]
            for c in range(N_CORES):
                x_part = x_buf[p, s, chip * N_CORES + c, :, where].astype(jnp.float32)
                y_ref[s, chip, c, p, :, where] = (x_part + total[c * part_seqs:(c + 1) * part_seqs]).astype(y_ref.dtype)
        for i in (0, 1, 4):
            ag(p, s, i).start()

    def relay(p, s):
        ag(p, s, 0).wait_recv()
        ag(p, s, 2).start()
        ag(p, s, 5).start()
        ag(p, s, 1).wait_recv()
        ag(p, s, 3).start()
        ag(p, s, 6).start()

    def last(p, s):
        ag(p, s, 2).wait_recv()
        ag(p, s, 7).start()
        ag(p, s, 3).wait_recv()
        ag(p, s, 8).start()

    def each(stage, p):
        for s in range(n_steps):
            stage(p, s)

    def query(b):
        return q_rows[pl.ds(b, rows, stride=n_seqs), :].astype(jnp.bfloat16)

    def attend(b, slot, after):
        new = pl.ds(pl.multiple_of(b * FRESH_ROWS, FRESH_ROWS), FRESH_ROWS)
        q_after = query(after)
        maxima = [None]

        def beside(start):
            maxima[0] = score_tile(q_after, k_buf.at[after], score_buf.at[1 - slot], start, len_ref[after], maxima[0])

        out = attend_one(query(b), v_buf.at[b], score_buf.at[slot], best_buf[slot],
                         fk_ref[new, :].astype(jnp.bfloat16), fv_ref[new, :].astype(jnp.bfloat16), fresh_mask, beside)
        best_buf[1 - slot] = maxima[0]
        head_buf[pl.ds(b, rows, stride=n_seqs), :] = out

    def wait_caches(b):
        for copy in kv_load(b):
            copy.wait()

    def attend_pair(i, carry):
        first = 2 * i
        after = jnp.minimum(first + 2, n_seqs - 1)
        wait_caches(first + 1)

        @pl.when(first + 2 < n_seqs)
        def _():
            wait_caches(after)

        attend(first, 0, first + 1)
        attend(first + 1, 1, after)

        @pl.when(i == part_seqs // 2 - 2)
        def _():
            unpack(1)

        @pl.when(i == part_seqs // 2 - 1)
        def _():
            pack(0)

        @pl.when(i == n_seqs // 2 - 2)
        def _():
            forward(0)

        return carry

    unpack(0)
    wait_caches(0)
    best = None
    for start in range(0, length, KEY_TILE):
        best = score_tile(query(0), k_buf.at[0], score_buf.at[0], start, len_ref[0], best)
    best_buf[0] = best
    lax.fori_loop(0, n_seqs // 2, attend_pair, 0)
    pack(1)
    partial(0)
    forward(1)
    each(middle, 0)
    partial(1)
    each(middle, 1)
    each(finish, 0)
    each(finish, 1)
    each(relay, 0)
    each(relay, 1)
    each(last, 0)
    each(last, 1)
    wo_swap.wait_send()
    for p in range(N_PARTS):
        for d in range(1, n_dev):
            q_copy(p, d).wait_send()
        for s in range(n_steps):
            for i in range(4, 9):
                ag(p, s, i).wait_recv()
            for i in range(9):
                ag(p, s, i).wait_send()
            for i in range(6):
                rs(p, s, i).wait_send()
        for d in (1, 2, 3):
            a_copy(p, d).wait_send()
        for d in range(N_CHIPS):
            a_forward(p, d).wait_send()


def store_kernel(n_steps, len_ref, fk_ref, fv_ref, y_ref, k_ref, v_ref, y_out, k_out, v_out, k_buf, v_buf, sems, y_sem):
    n_seqs, length, depth = k_buf.shape

    def store(b):
        return (pltpu.make_async_copy(k_buf.at[b], k_out.at[b], sems.at[0, b]),
                pltpu.make_async_copy(v_buf.at[b], v_out.at[b], sems.at[1, b]))

    def patch(b, buf, fresh):
        start = pl.multiple_of(jnp.minimum(len_ref[b] // 8 * 8, length - WINDOW), 8)
        offset = len_ref[b] - start
        row = lax.broadcasted_iota(jnp.int32, (WINDOW, depth), 0)
        window = buf[b, pl.ds(start, WINDOW), :].astype(jnp.float32)
        for s in range(n_steps):
            window = jnp.where(row == offset + s, fresh[b * FRESH_ROWS + s:b * FRESH_ROWS + s + 1, :], window)
        buf[b, pl.ds(start, WINDOW), :] = window.astype(buf.dtype)

    y_copy = pltpu.make_async_copy(y_ref, y_out, y_sem)
    y_copy.start()
    for b in range(n_seqs):
        patch(b, k_buf, fk_ref)
        patch(b, v_buf, fv_ref)
        for copy in store(b):
            copy.start()
    y_copy.wait()
    for b in range(n_seqs):
        for copy in store(b):
            copy.wait()


def solution(mesh):
    def local_block(x_steps, seq_lens, k_cache, v_cache, ln_gain, ln_bias, w_q, b_q, w_kv, b_kv, w_out, b_out):
        n_steps, _, width = x_steps.shape
        n_seqs, length, depth = k_cache.shape
        q_width = w_q.shape[1]
        n_dev = N_CHIPS * N_CORES
        part_seqs = n_seqs // N_PARTS
        rows = n_dev * n_steps * q_width // depth
        chip_width, half = N_CORES * q_width, width // 2
        block = N_CORES * part_seqs
        smem = pl.BlockSpec(memory_space=pltpu.SMEM)
        vmem = pl.BlockSpec(memory_space=pltpu.VMEM)
        hbm = pl.BlockSpec(memory_space=pl.ANY)
        dma = pltpu.SemaphoreType.DMA
        bf16, f32 = jnp.bfloat16, jnp.float32
        y_shape = (n_steps, N_CHIPS, N_CORES, N_PARTS, part_seqs, width)
        fresh_shape = (n_seqs * FRESH_ROWS, depth)
        y_vm, k_vm, v_vm, fresh_k, fresh_v = pl.pallas_call(
            block_kernel,
            out_shape=[pltpu.VMEM(y_shape, bf16), pltpu.VMEM(k_cache.shape, bf16), pltpu.VMEM(v_cache.shape, bf16), pltpu.VMEM(fresh_shape, f32), pltpu.VMEM(fresh_shape, f32)],
            in_specs=[hbm] * 12,
            out_specs=[vmem] * 5,
            scratch_shapes=[
                pltpu.SMEM(seq_lens.shape, jnp.int32),
                pltpu.VMEM(ln_gain.shape, bf16),
                pltpu.VMEM(ln_bias.shape, bf16),
                pltpu.VMEM(b_q.shape, bf16),
                pltpu.VMEM(b_kv.shape, bf16),
                pltpu.VMEM(b_out.shape, bf16),
                pltpu.VMEM((N_PARTS, n_steps, n_dev, part_seqs, width), bf16),
                pltpu.VMEM((n_steps, n_seqs, width), bf16),
                pltpu.VMEM((n_steps * n_seqs, width), bf16),
                pltpu.VMEM((N_PARTS, n_steps * n_dev * part_seqs, width), bf16),
                pltpu.VMEM((LN_ROWS, width), f32),
                pltpu.VMEM((LN_ROWS, width), f32),
                pltpu.VMEM((1, width), f32),
                pltpu.VMEM(w_q.shape, bf16),
                pltpu.VMEM(w_kv.shape, bf16),
                pltpu.VMEM((chip_width, half), bf16),
                pltpu.VMEM((q_width, half), bf16),
                pltpu.VMEM((N_PARTS, n_steps, n_dev, part_seqs, q_width), bf16),
                pltpu.VMEM((N_PARTS, n_dev, n_steps, part_seqs, q_width), bf16),
                pltpu.VMEM((rows * n_seqs, depth), f32),
                pltpu.VMEM((2, rows, length), f32),
                pltpu.VMEM((2, rows, LANES), f32),
                pltpu.VMEM((rows * n_seqs, depth), f32),
                pltpu.VMEM((N_PARTS, N_CHIPS, n_steps, part_seqs, chip_width), bf16),
                pltpu.VMEM((N_PARTS, N_CORES, N_CHIPS, n_steps, part_seqs, chip_width), bf16),
                pltpu.VMEM((n_steps * N_CHIPS * block, chip_width), bf16),
                pltpu.VMEM((N_PARTS, n_steps, N_CHIPS, block, half), bf16),
                pltpu.VMEM((N_PARTS, n_steps, 2, block, half // 2), bf16),
                pltpu.VMEM((N_PARTS, n_steps, 4, block, half // 2), bf16),
                dma((6,)), dma((2 * N_PARTS,)), dma((4,)), dma((2, n_seqs)), dma((2,)),
                dma((N_PARTS, n_dev - 1)), dma((N_PARTS, n_dev - 1)),
                dma((N_PARTS, 3)), dma((N_PARTS, 3)),
                dma((N_PARTS, N_CHIPS)), dma((N_PARTS, N_CHIPS)),
                dma((N_PARTS, n_steps, 6)), dma((N_PARTS, n_steps, 6)),
                dma((N_PARTS, n_steps, 9)), dma((N_PARTS, n_steps, 9)),
            ],
            compiler_params=pltpu.CompilerParams(vmem_limit_bytes=BLOCK_VMEM, collective_id=1, has_side_effects=True),
            cost_estimate=pl.CostEstimate(flops=4 * n_seqs * rows * length * depth, bytes_accessed=4 * n_seqs * length * depth, transcendentals=n_seqs * rows * length),
        )(seq_lens, ln_gain, ln_bias, b_q, b_kv, b_out,
          x_steps.reshape(n_steps, n_dev, N_PARTS, part_seqs, width), w_q, w_kv, w_out, k_cache, v_cache)
        y_steps, k_out, v_out, _, _ = pl.pallas_call(
            functools.partial(store_kernel, n_steps),
            out_shape=[jax.ShapeDtypeStruct(y_shape, bf16), jax.ShapeDtypeStruct(k_cache.shape, bf16), jax.ShapeDtypeStruct(v_cache.shape, bf16), pltpu.VMEM(k_cache.shape, bf16), pltpu.VMEM(v_cache.shape, bf16)],
            in_specs=[smem] + [vmem] * 5,
            out_specs=[hbm] * 3 + [vmem] * 2,
            scratch_shapes=[dma((2, n_seqs)), dma],
            input_output_aliases={4: 3, 5: 4},
            compiler_params=pltpu.CompilerParams(vmem_limit_bytes=2 * 1024 * 1024),
        )(seq_lens, fresh_k, fresh_v, y_vm, k_vm, v_vm)
        return y_steps.reshape(x_steps.shape), k_out, v_out

    row_spec = P(('dp', 'tp'), None, None)
    return jax.shard_map(
        local_block,
        mesh=mesh,
        in_specs=(P(None, 'dp', None), P(('dp', 'tp')), row_spec, row_spec, P(None), P(None), P(None, 'tp'), P('tp'), P(None, None), P(None), P('tp', None), P(None)),
        out_specs=(P(None, 'dp', None), row_spec, row_spec),
        check_vma=False,
    )
```
